32 devices in a mesh: dp: 8 (over z, core), tensor: 4 (over y, x).
Axes of the slice: x: 2, y: 2, z: 4, core: 2. Of those that a mesh axis runs over, the one named last changes fastest.
Arguments:
- block_input_rows: bfloat16 [2, 8, 2048, 1024], P(None, 'dp', 'tensor'), may hold values from -6 to 6
- output_gradient: bfloat16 [2, 8, 2048, 1024], P(None, 'dp', 'tensor'), may hold values from -6 to 6
- segment_numbers: int32 [2, 8, 2048], P(None, 'dp'), may hold values from 0 to 4, never falling along the last dimension, each value on 1 to 1024 neighbouring positions
- token_keep_mask: int32 [2, 8, 2048], P(None, 'dp'), may hold values 0 or 1
- layer_norm_gain: float32 [2, 1024], replicated, may hold values from 0.1 to 1.9
- layer_norm_bias: float32 [2, 1024], replicated, may hold values from -3 to 3
- projection_weight: bfloat16 [3, 1024, 1024], P(None, None, 'tensor'), may hold values from -0.1875 to 0.1875
- output_weight: bfloat16 [1024, 1024], P('tensor'), may hold values from -0.75 to 0.75
- up_weight: bfloat16 [1024, 4096], P(None, 'tensor'), may hold values from -0.1875 to 0.1875
- down_weight: bfloat16 [4096, 1024], P('tensor'), may hold values from -0.09375 to 0.09375
- adapter_first_input: bfloat16 [4, 1024, 128], P(None, None, 'tensor'), may hold values from -0.1875 to 0.1875
- adapter_second_projections: bfloat16 [3, 128, 1024], P(None, None, 'tensor'), may hold values from -0.5 to 0.5
- adapter_second_upward: bfloat16 [128, 4096], P(None, 'tensor'), may hold values from -0.5 to 0.5
- adapter_first_output: bfloat16 [1024, 128], P('tensor'), may hold values from -0.75 to 0.75
- adapter_first_down: bfloat16 [4096, 128], P('tensor'), may hold values from -0.09375 to 0.09375
- adapter_second_output: bfloat16 [2, 128, 1024], P(None, 'tensor'), may hold values from -0.5 to 0.5
Outputs:
- block_output: bfloat16 [2, 8, 2048, 1024], P(None, 'dp', 'tensor')
- grad_in: bfloat16 [2, 8, 2048, 1024], P(None, 'dp', 'tensor')
- grad_norm_gain: float32 [2, 1024], replicated
- grad_norm_bias: float32 [2, 1024], replicated
- grad_lora_a_in: float32 [4, 1024, 128], P(None, None, 'tensor')
- grad_lora_b_qkv: float32 [3, 128, 1024], P(None, None, 'tensor')
- grad_lora_b_up: float32 [128, 4096], P(None, 'tensor')
- grad_lora_a_o: float32 [1024, 128], P('tensor')
- grad_lora_a_down: float32 [4096, 128], P('tensor')
- grad_lora_b_out: float32 [2, 128, 1024], P(None, 'tensor')
The draws below stay inside these ranges and needn't reach their ends.
Inputs may be any that keep to these rules, and one draw needn't show every extreme that they name: `segment_numbers`: in each group the 2048 tokens hold 5 whole documents one after another, numbered from 0 upward; each has 1 to 1024 tokens and one has exactly 1024.
All inputs are finite; a program needn't handle non-finite values. No bound on the sum of `token_keep_mask` on one device may be relied on, other than what follows from the above.
Results may differ from the reference program's by a relative error of at most 0.012.
The reference program's roundings to bfloat16 on the way count: a program that leaves them out, or rounds other values in their place, can miss the bound.
Values may be sent and summed in bfloat16 or wider, within the bound.
A program may use at most 192 MiB of HBM per device.

```python
import math
import jax
import jax.numpy as jnp
import numpy as np
from jax import lax

MODEL_WIDTH = 1024
ATTENTION_HEADS = 16
HEAD_SIZE = 64
HIDDEN_UNITS = 4096
ROT = 16
ADAPTER_RANK = 128
BLOCK = 512
TOK_DEV = 2048
MICRO = 2
SEQ_MAX = 1024
N_DOCS = 5
N_DP = 8


def place_ends(values, stream_key, smallest, largest):
    longest = values.shape.index(max(values.shape))
    spots = []
    for shift in (0, 1):
        where = [jax.random.randint(jax.random.fold_in(stream_key, axis), (), 0, length) for axis, length in enumerate(values.shape)]
        where[longest] = (where[longest] + shift) % values.shape[longest]
        spots.append(tuple(where))
    return values.at[spots[0]].set(smallest).at[spots[1]].set(largest)


def block_scale(own_key, shape, cuts, smallest, top_value):
    gain, own = 1.0, jax.random.fold_in(own_key, 6)
    for axis_at, shards_of in cuts:
        steps = jnp.exp(jax.random.uniform(jax.random.fold_in(own, axis_at), (shards_of,), jnp.float32, smallest / len(cuts), top_value / len(cuts)))
        gain = gain * jnp.repeat(steps, shape[axis_at] // shards_of).reshape([-1 if axis == axis_at else 1 for axis in range(len(shape))])
    return gain


def split_up(number_of, total, reach, skew):
    loads = [(1 << 20) // math.isqrt(grade ** skew) + 1 for grade in range(2, number_of + 1)]
    spare, counts = total - reach - (number_of - 1), [1] * (number_of - 1)
    while spare > 0:
        candidates = [i for i in range(number_of - 1) if counts[i] < reach]
        pool, left = sum([loads[i] for i in candidates]), spare
        for i in candidates:
            extra = min(reach - counts[i], max(1, left * loads[i] // pool), spare)
            counts[i] = counts[i] + extra
            spare = spare - extra
    return np.array([reach] + counts)


def ragged_sizes(key, count, total, limit, skew):
    if count == 2:
        one = jax.random.randint(key, (), max(1, total - limit), min(limit, total - 1) + 1)
        return jnp.stack([one, total - one])
    lengths = jnp.asarray(split_up(count, total, limit, skew), jnp.int32)
    twos = (count - 1) // 2
    source_of, taker = lengths[1:1 + 2 * twos:2], lengths[2:2 + 2 * twos:2]
    slack = jnp.minimum(source_of - 1, limit - taker)
    shifted = jax.random.randint(jax.random.fold_in(key, 1), (twos,), 0, 1 << 20) % (slack + 1)
    lengths = lengths.at[1:1 + 2 * twos:2].set(source_of - shifted).at[2:2 + 2 * twos:2].set(taker + shifted)
    return lengths[jax.random.permutation(jax.random.fold_in(key, 2), count)]


def centred(key, dims, width, limit, split=(), held_as=jnp.bfloat16):
    drawn = width * jax.random.normal(key, dims, jnp.float32)
    if split:
        drawn = drawn * block_scale(key, dims, split, -0.22, 0.18)
    return jnp.clip(drawn, -limit, limit).astype(held_as)


def setup_inputs(seed: int = 0) -> dict:
    keys = jax.random.split(jax.random.key(seed), 17)
    block_input_rows = centred(keys[0], (MICRO, N_DP, TOK_DEV, MODEL_WIDTH), 1.0, 6.0, ((1, 8), (2, 4)))
    output_gradient = centred(keys[1], (MICRO, N_DP, TOK_DEV, MODEL_WIDTH), 1.0, 6.0, ((1, 8), (2, 4)))
    segment_numbers = jax.vmap(lambda own: jnp.searchsorted(jnp.cumsum(ragged_sizes(own, N_DOCS, TOK_DEV, SEQ_MAX, 2)), jnp.arange(TOK_DEV), side="right"))(jax.random.split(keys[2], MICRO * N_DP)).reshape((MICRO, N_DP, TOK_DEV)).astype(jnp.int32)
    token_keep_mask = place_ends((jax.random.randint(keys[3], (MICRO, N_DP, TOK_DEV), 0, 8) < 7).astype(jnp.int32), jax.random.fold_in(keys[3], 1), 0, 1)
    layer_norm_gain = jnp.clip(1.0 + 0.18 * jax.random.normal(keys[4], (2, MODEL_WIDTH), jnp.float32), 0.1, 1.9)
    layer_norm_bias = centred(keys[5], (2, MODEL_WIDTH), 0.5, 3.0, (), jnp.float32)
    projection_weight = centred(keys[6], (3, MODEL_WIDTH, ATTENTION_HEADS * HEAD_SIZE), MODEL_WIDTH ** -0.5, 0.1875, ((2, 4),))
    output_weight = centred(keys[7], (ATTENTION_HEADS * HEAD_SIZE, MODEL_WIDTH), HEAD_SIZE ** -0.5, 0.75, ((0, 4),))
    up_weight = centred(keys[8], (MODEL_WIDTH, HIDDEN_UNITS), MODEL_WIDTH ** -0.5, 0.1875, ((1, 4),))
    down_weight = centred(keys[9], (HIDDEN_UNITS, MODEL_WIDTH), HIDDEN_UNITS ** -0.5, 0.09375, ((0, 4),))
    adapter_first_input = centred(keys[10], (4, MODEL_WIDTH, ADAPTER_RANK), MODEL_WIDTH ** -0.5, 0.1875, ((2, 4),))
    adapter_second_projections = centred(keys[11], (3, ADAPTER_RANK, ATTENTION_HEADS * HEAD_SIZE), ADAPTER_RANK ** -0.5, 0.5, ((2, 4),))
    adapter_second_upward = centred(keys[12], (ADAPTER_RANK, HIDDEN_UNITS), ADAPTER_RANK ** -0.5, 0.5, ((1, 4),))
    adapter_first_output = centred(keys[13], (ATTENTION_HEADS * HEAD_SIZE, ADAPTER_RANK), HEAD_SIZE ** -0.5, 0.75, ((0, 4),))
    adapter_first_down = centred(keys[14], (HIDDEN_UNITS, ADAPTER_RANK), HIDDEN_UNITS ** -0.5, 0.09375, ((0, 4),))
    adapter_second_output = centred(keys[15], (2, ADAPTER_RANK, MODEL_WIDTH), ADAPTER_RANK ** -0.5, 0.5, ((1, 4),))
    return dict(block_input_rows=block_input_rows, output_gradient=output_gradient, segment_numbers=segment_numbers, token_keep_mask=token_keep_mask, layer_norm_gain=layer_norm_gain, layer_norm_bias=layer_norm_bias, projection_weight=projection_weight, output_weight=output_weight, up_weight=up_weight, down_weight=down_weight, adapter_first_input=adapter_first_input, adapter_second_projections=adapter_second_projections, adapter_second_upward=adapter_second_upward, adapter_first_output=adapter_first_output, adapter_first_down=adapter_first_down, adapter_second_output=adapter_second_output)


@jax.custom_vjp
def low(v):
    return lax.optimization_barrier(v.astype(jnp.bfloat16)).astype(jnp.float32)

@jax.custom_vjp
def reduced_backward(v):
    return v

def low_keep(v):
    return (low(v), None)

def low_pass(kept, grad):
    return (grad,)

def back_keep(v):
    return (v, None)

def back_low(kept, grad):
    return (low(grad),)
low.defvjp(low_keep, low_pass)
reduced_backward.defvjp(back_keep, back_low)
EPSILON = 1e-05
ADAPTER_SCALE = 0.25
NEG_LARGE = -1e+30
HIGHEST = lax.Precision.HIGHEST

def rounded_operands(value):
    return low(reduced_backward(value))

def matrix_product(left_operand, right_operand):
    return jnp.dot(left_operand, right_operand, precision=HIGHEST)

def normalized(values):
    average = lax.optimization_barrier(jnp.mean(values, axis=-1, keepdims=True))
    centered = values - average
    variance = lax.optimization_barrier(jnp.mean(centered * centered, axis=-1, keepdims=True))
    return centered * lax.rsqrt(variance + EPSILON)

def positions(segment):
    sequence_length = segment.shape[0]
    indices = jnp.arange(sequence_length, dtype=jnp.int32)
    previous = jnp.concatenate([segment[:1] - 1, segment[:-1]])
    starting = jnp.where(segment != previous, indices, jnp.zeros_like(indices))
    return indices - lax.cummax(starting, axis=0)

def rotary_tables(segment):
    half_rot = ROT // 2
    exponent = 2.0 * jnp.arange(half_rot, dtype=jnp.float32) / ROT
    frequency = jnp.exp(-math.log(10000.0) * exponent)
    angles = positions(segment).astype(jnp.float32)[:, None] * frequency[None, :]
    return (jnp.cos(angles), jnp.sin(angles))

def rotate(values, cos_table, sin_table):
    half_rot = cos_table.shape[1]
    first_half = values[..., :half_rot]
    second_half = values[..., half_rot:2 * half_rot]
    cosine = cos_table[:, None, :]
    sine_wide = sin_table[:, None, :]
    return jnp.concatenate([first_half * cosine - second_half * sine_wide, second_half * cosine + first_half * sine_wide, values[..., 2 * half_rot:]], axis=-1)

def allowed_pairs(segment, seg_pad, keep_pad, start):
    query_pos = start + jnp.arange(BLOCK, dtype=jnp.int32)
    key_pos = start - 2 * BLOCK + jnp.arange(3 * BLOCK, dtype=jnp.int32)
    query_seg = lax.dynamic_slice_in_dim(segment, start, BLOCK)
    key_seg = lax.dynamic_slice_in_dim(seg_pad, start, 3 * BLOCK)
    key_keep = lax.dynamic_slice_in_dim(keep_pad, start, 3 * BLOCK)
    same_doc = query_seg[:, None] == key_seg[None, :]
    causal = key_pos[None, :] <= query_pos[:, None]
    usable = (key_keep[None, :] == 1) | (key_pos[None, :] == query_pos[:, None])
    return same_doc & causal & usable

def padded_keys(keys_all, values_all, segment, token_keep_mask):
    pad_rows = 2 * BLOCK
    blank = jnp.zeros((pad_rows,) + keys_all.shape[1:], keys_all.dtype)
    key_pad = jnp.concatenate([blank, keys_all], axis=0)
    value_pad = jnp.concatenate([blank, values_all], axis=0)
    seg_pad = jnp.concatenate([jnp.full((pad_rows,), -1, jnp.int32), segment.astype(jnp.int32)])
    keep_pad = jnp.concatenate([jnp.zeros((pad_rows,), jnp.int32), token_keep_mask.astype(jnp.int32)])
    return (key_pad, value_pad, seg_pad, keep_pad)

def attention(queries, keys_all, values_all, segment, token_keep_mask):
    sequence_length = queries.shape[0]
    key_pad, value_pad, seg_pad, keep_pad = padded_keys(keys_all, values_all, segment, token_keep_mask)
    scale = 1.0 / math.sqrt(HEAD_SIZE)

    def one_block(block_id):
        start = block_id * BLOCK
        query_block = lax.dynamic_slice_in_dim(queries, start, BLOCK, 0)
        key_block = lax.dynamic_slice_in_dim(key_pad, start, 3 * BLOCK, 0)
        value_block = lax.dynamic_slice_in_dim(value_pad, start, 3 * BLOCK, 0)
        allowed = allowed_pairs(segment, seg_pad, keep_pad, start)
        scores = reduced_backward(jnp.einsum('qhd,khd->hqk', query_block, key_block, precision=HIGHEST) * scale)
        scores = jnp.where(allowed[None], scores, NEG_LARGE)
        weights = low(jax.nn.softmax(scores, axis=-1))
        return jnp.einsum('hqk,khd->qhd', weights, value_block, precision=HIGHEST)
    blocks = lax.map(jax.checkpoint(one_block), jnp.arange(sequence_length // BLOCK, dtype=jnp.int32))
    return blocks.reshape(sequence_length, ATTENTION_HEADS, HEAD_SIZE)

def block_forward(inputs, parameters, frozen, segment, token_keep_mask):
    layer_norm_gain, layer_norm_bias, adapter_first_input, adapter_second_projections, adapter_second_upward, adapter_first_output, adapter_first_down, adapter_second_output = parameters
    projection_weight, output_weight, up_weight, down_weight = frozen
    sequence_length = inputs.shape[0]
    standard = normalized(inputs)
    first_normed_rows = low(standard * layer_norm_gain[0] + layer_norm_bias[0])
    second_normed_rows = low(standard * layer_norm_gain[1] + layer_norm_bias[1])
    reduced_input = [rounded_operands(matrix_product(first_normed_rows, adapter_first_input[item_number])) for item_number in range(3)]
    reduced_input.append(rounded_operands(matrix_product(second_normed_rows, adapter_first_input[3])))
    linear_output = [reduced_backward(matrix_product(first_normed_rows, projection_weight[item_number]) + ADAPTER_SCALE * matrix_product(reduced_input[item_number], adapter_second_projections[item_number])).reshape(sequence_length, ATTENTION_HEADS, HEAD_SIZE) for item_number in range(3)]
    cos_table, sin_table = rotary_tables(segment)
    queries = low(rotate(linear_output[0], cos_table, sin_table))
    keys_all = low(rotate(linear_output[1], cos_table, sin_table))
    values_all = low(linear_output[2])
    attended_context = rounded_operands(attention(queries, keys_all, values_all, segment, token_keep_mask).reshape(sequence_length, ATTENTION_HEADS * HEAD_SIZE))
    preactivation = reduced_backward(matrix_product(second_normed_rows, up_weight) + ADAPTER_SCALE * matrix_product(reduced_input[3], adapter_second_upward))
    hidden_rows = low(jax.nn.gelu(preactivation, approximate=False))
    reduced_attention = rounded_operands(matrix_product(attended_context, adapter_first_output))
    reduced_feedforward = rounded_operands(matrix_product(hidden_rows, adapter_first_down))
    side_branch = matrix_product(attended_context, output_weight) + matrix_product(hidden_rows, down_weight)
    side_branch = side_branch + ADAPTER_SCALE * (matrix_product(reduced_attention, adapter_second_output[0]) + matrix_product(reduced_feedforward, adapter_second_output[1]))
    return inputs + side_branch

def reference(block_input_rows, output_gradient, segment_numbers, token_keep_mask, layer_norm_gain, layer_norm_bias, projection_weight, output_weight, up_weight, down_weight, adapter_first_input, adapter_second_projections, adapter_second_upward, adapter_first_output, adapter_first_down, adapter_second_output):
    frozen = (projection_weight.astype(jnp.float32), output_weight.astype(jnp.float32), up_weight.astype(jnp.float32), down_weight.astype(jnp.float32))
    trainable_parameters = (layer_norm_gain.astype(jnp.float32), layer_norm_bias.astype(jnp.float32), adapter_first_input.astype(jnp.float32), adapter_second_projections.astype(jnp.float32), adapter_second_upward.astype(jnp.float32), adapter_first_output.astype(jnp.float32), adapter_first_down.astype(jnp.float32), adapter_second_output.astype(jnp.float32))
    group_rows = block_input_rows.reshape(-1, TOK_DEV, MODEL_WIDTH)
    group_grad = output_gradient.reshape(-1, TOK_DEV, MODEL_WIDTH)
    group_seg = segment_numbers.reshape(-1, TOK_DEV).astype(jnp.int32)
    group_keep = token_keep_mask.reshape(-1, TOK_DEV).astype(jnp.int32)

    def group_step(totals, item):
        rows_input, rows_grad, segment, keep_row = item

        def forward(inputs, parameters):
            return block_forward(inputs, parameters, frozen, segment, keep_row)
        result, pullback = jax.vjp(forward, rows_input.astype(jnp.float32), trainable_parameters)
        grad_rows, grad_params = pullback(rows_grad.astype(jnp.float32))
        totals = jax.tree.map(lambda left_operand, right_operand: left_operand + right_operand, totals, grad_params)
        return (totals, (result.astype(jnp.bfloat16), grad_rows.astype(jnp.bfloat16)))
    initial = jax.tree.map(jnp.zeros_like, trainable_parameters)
    totals, (results, grad_rows) = lax.scan(group_step, initial, (group_rows, group_grad, group_seg, group_keep))
    return (results.reshape(block_input_rows.shape), grad_rows.reshape(block_input_rows.shape), totals[0], totals[1], totals[2], totals[3], totals[4], totals[5], totals[6], totals[7])
```

```python
import functools
import math

import jax
import jax.numpy as jnp
from jax import lax
from jax.experimental import pallas as pl
from jax.experimental.pallas import tpu as pltpu
from jax.sharding import PartitionSpec as P

HEAD = 64
HALF = 8
N_DOCS = 5
TILE = 256
SLOTS = 5
EPSILON = 1e-05
SCALE = 0.25
F32 = jnp.float32
BF = jnp.bfloat16


def dot(a, b, ca, cb):
    return lax.dot_general(a, b, (((ca,), (cb,)), ((), ())), preferred_element_type=F32)


def attention_kernel(heads, lo_ref, lin_ref, g_ref, cos_ref, sin_ref, segq_ref, segk_ref,
                     ctx_ref, dlin_ref, qt, kt, vt, kn, vn, qz, acc, s_scr, e_scr):
    width = heads * HEAD
    length = lin_ref.shape[1]
    blocks = length // TILE

    def rotate(z, cos, sin):
        a, b = z[:HALF], z[HALF:2 * HALF]
        return jnp.concatenate([a * cos - b * sin, b * cos + a * sin, z[2 * HALF:]], axis=0)

    def prepare(c, carry):
        cols = pl.ds(pl.multiple_of(c * TILE, TILE), TILE)
        cos, sin = cos_ref[:, cols], sin_ref[:, cols]
        for h in range(heads):
            rows = pl.ds(h * HEAD, HEAD)
            q = rotate(lin_ref[pl.ds(h * HEAD, HEAD), cols], cos, sin).astype(BF).astype(F32) * 0.125
            k = rotate(lin_ref[pl.ds(width + h * HEAD, HEAD), cols], cos, sin)
            v = lin_ref[pl.ds(2 * width + h * HEAD, HEAD), cols]
            qt[rows, cols] = q.astype(BF)
            kt[rows, cols] = k.astype(BF)
            vt[rows, cols] = v.astype(BF)
            kn[h, cols, :] = jnp.transpose(k).astype(BF)
            vn[h, cols, :] = jnp.transpose(v).astype(BF)
            qn = jnp.transpose(q)
            qz[h, cols, :] = jnp.concatenate([jnp.zeros_like(qn), qn], axis=1).astype(BF)
            acc[h, cols, :] = jnp.zeros((TILE, 2 * HEAD), F32)
        return carry

    lax.fori_loop(0, blocks, prepare, 0)

    def query_block(qb, carry):
        lo = lo_ref[qb]
        qcols = pl.ds(pl.multiple_of(qb * TILE, TILE), TILE)
        segq = segq_ref[:, qcols]

        def scores(kb, tops):
            krows = pl.ds(pl.multiple_of(kb * TILE, TILE), TILE)
            kpos = kb * TILE + lax.broadcasted_iota(jnp.int32, (TILE, TILE), 0)
            qpos = qb * TILE + lax.broadcasted_iota(jnp.int32, (TILE, TILE), 1)
            allowed = ((segk_ref[krows, :] == segq) & (kpos <= qpos)) | (kpos == qpos)
            out = []
            for h in range(heads):
                s = dot(kn[h, krows, :], qt[pl.ds(h * HEAD, HEAD), qcols], 1, 0)
                s = jnp.where(allowed, s, -1e30)
                s_scr[h, kb - lo] = s
                out.append(jnp.maximum(tops[h], jnp.max(s, axis=0, keepdims=True)))
            return tuple(out)

        tops = lax.fori_loop(lo, qb + 1, scores,
                             tuple(jnp.full((1, TILE), -1e30, F32) for _ in range(heads)))

        def weights(kb, sums):
            kcols = pl.ds(pl.multiple_of(kb * TILE, TILE), TILE)
            out = []
            for h in range(heads):
                e = jnp.exp(s_scr[h, kb - lo] - tops[h])
                low = e.astype(BF)
                e_scr[h, kb - lo] = low
                total, ctx = sums[h]
                out.append((total + jnp.sum(e, axis=0, keepdims=True),
                            ctx + dot(vt[pl.ds(h * HEAD, HEAD), kcols], low, 1, 0)))
            return tuple(out)

        sums = lax.fori_loop(lo, qb + 1, weights,
                             tuple((jnp.zeros((1, TILE), F32), jnp.zeros((HEAD, TILE), F32))
                                   for _ in range(heads)))
        gts, gzs, terms = [], [], []
        for h in range(heads):
            rows = pl.ds(h * HEAD, HEAD)
            inverse = 1.0 / sums[h][0]
            ctx = sums[h][1] * inverse
            ctx_ref[rows, qcols] = ctx.astype(BF)
            g = g_ref[rows, qcols].astype(F32)
            terms.append(jnp.sum(g * ctx, axis=0, keepdims=True) * inverse)
            g = g * inverse
            gts.append(g.astype(BF))
            gn = jnp.transpose(g)
            gzs.append(jnp.concatenate([gn, jnp.zeros_like(gn)], axis=1).astype(BF))

        def backward(kb, dqs):
            krows = pl.ds(pl.multiple_of(kb * TILE, TILE), TILE)
            out = []
            for h in range(heads):
                low = e_scr[h, kb - lo]
                dp = dot(vn[h, krows, :], gts[h], 1, 0)
                ds = (low.astype(F32) * (dp - terms[h])).astype(BF)
                acc[h, krows, :] += dot(low, gzs[h], 1, 0) + dot(ds, qz[h, qcols, :], 1, 0)
                out.append(dqs[h] + dot(kt[pl.ds(h * HEAD, HEAD), krows], ds, 1, 0))
            return tuple(out)

        dqs = lax.fori_loop(lo, qb + 1, backward,
                            tuple(jnp.zeros((HEAD, TILE), F32) for _ in range(heads)))
        cos, sin = cos_ref[:, qcols], sin_ref[:, qcols]
        for h in range(heads):
            dlin_ref[pl.ds(h * HEAD, HEAD), qcols] = rotate(dqs[h] * 0.125, cos, -sin).astype(BF)
        return carry

    lax.fori_loop(0, blocks, query_block, 0)

    def finish(c, carry):
        cols = pl.ds(pl.multiple_of(c * TILE, TILE), TILE)
        cos, sin = cos_ref[:, cols], sin_ref[:, cols]
        for h in range(heads):
            both = jnp.transpose(acc[h, cols, :])
            dlin_ref[pl.ds(width + h * HEAD, HEAD), cols] = rotate(both[HEAD:], cos, -sin).astype(BF)
            dlin_ref[pl.ds(2 * width + h * HEAD, HEAD), cols] = both[:HEAD].astype(BF)
        return carry

    lax.fori_loop(0, blocks, finish, 0)


def attention(lin, g, cos, sin, segment, keep):
    width, length = g.shape
    heads = width // HEAD
    starts = jnp.sum(segment[None, :] < jnp.arange(N_DOCS, dtype=jnp.int32)[:, None], axis=1)
    firsts = segment[::TILE]
    lo = jnp.sum(jnp.where(firsts[:, None] == jnp.arange(N_DOCS)[None, :], starts[None, :], 0), axis=1)
    lo = (lo // TILE).astype(jnp.int32)
    segk = jnp.where(keep == 1, segment, -1)[:, None]
    vmem = pl.BlockSpec(memory_space=pltpu.VMEM)
    return pl.pallas_call(
        functools.partial(attention_kernel, heads),
        grid_spec=pltpu.PrefetchScalarGridSpec(
            num_scalar_prefetch=1,
            in_specs=[vmem] * 6,
            out_specs=[vmem] * 2,
            scratch_shapes=[
                pltpu.VMEM((width, length), BF),
                pltpu.VMEM((width, length), BF),
                pltpu.VMEM((width, length), BF),
                pltpu.VMEM((heads, length, HEAD), BF),
                pltpu.VMEM((heads, length, HEAD), BF),
                pltpu.VMEM((heads, length, 2 * HEAD), BF),
                pltpu.VMEM((heads, length, 2 * HEAD), F32),
                pltpu.VMEM((heads, SLOTS, TILE, TILE), F32),
                pltpu.VMEM((heads, SLOTS, TILE, TILE), BF),
            ]),
        out_shape=[jax.ShapeDtypeStruct((width, length), BF), jax.ShapeDtypeStruct((3 * width, length), BF)],
        compiler_params=pltpu.CompilerParams(vmem_limit_bytes=60 << 20),
        name="attention",
        cost_estimate=pl.CostEstimate(flops=20 * heads * length * 768 * 64, transcendentals=heads * length * 768,
                                      bytes_accessed=13 * width * length * 2),
    )(lo, lin, g, cos, sin, segment[None, :], segk)


def rotary_tables(segment):
    length = segment.shape[0]
    starts = jnp.sum(segment[None, :] < jnp.arange(N_DOCS, dtype=jnp.int32)[:, None], axis=1)
    begin = jnp.sum(jnp.where(segment[None, :] == jnp.arange(N_DOCS)[:, None], starts[:, None], 0), axis=0)
    position = (jnp.arange(length, dtype=jnp.int32) - begin).astype(F32)
    exponent = jnp.arange(HALF, dtype=F32) / HALF
    frequency = jnp.exp(-math.log(10000.0) * exponent)
    angles = frequency[:, None] * position[None, :]
    return jnp.cos(angles), jnp.sin(angles)


def normalized(values):
    average = jnp.mean(values, axis=-1, keepdims=True)
    centered = values - average
    variance = jnp.mean(centered * centered, axis=-1, keepdims=True)
    inverse = lax.rsqrt(variance + EPSILON)
    return centered * inverse, inverse


def on_device(x, gy, segment, keep, gain, bias, w_qkv, w_out, w_up, w_down,
              a_in, b_qkv, b_up, a_out, a_down, b_out):
    width = w_qkv.shape[2]
    micro = x.shape[0]
    a_full = lax.all_gather(a_in, "tensor", axis=2, tiled=True)
    b_full = lax.all_gather(b_out, "tensor", axis=1, tiled=True)

    m_qkv = jnp.concatenate([
        (w_qkv[i].astype(F32) + SCALE * dot(a_full[i], b_qkv[i], 1, 0)).astype(BF) for i in range(3)
    ], axis=1)
    m_up = (w_up.astype(F32) + SCALE * dot(a_full[3], b_up, 1, 0)).astype(BF)
    m_out = (w_out.astype(F32) + SCALE * dot(a_out, b_full[0], 1, 0)).astype(BF)
    m_down = (w_down.astype(F32) + SCALE * dot(a_down, b_full[1], 1, 0)).astype(BF)
    a_three = jnp.concatenate([a_full[0], a_full[1], a_full[2]], axis=1)
    b_both = jnp.concatenate([b_full[0], b_full[1]], axis=0)

    outs, grads, sums = [], [], None
    for m in range(micro):
        rows, seg = x[m, 0], segment[m, 0]
        xg = lax.all_gather(rows, "tensor", axis=0, tiled=True)
        gg = lax.all_gather(gy[m, 0], "tensor", axis=0, tiled=True)
        standard, _ = normalized(xg.astype(F32))
        n1 = (standard * gain[0] + bias[0]).astype(BF)
        n2 = (standard * gain[1] + bias[1]).astype(BF)
        lin = dot(m_qkv, n1, 0, 1)
        low3 = dot(n1, a_three, 1, 0).astype(BF)
        low1 = dot(n2, a_full[3], 1, 0).astype(BF)
        g_ctx = dot(m_out, gg, 1, 1).astype(BF)
        low_grad = (SCALE * dot(gg, b_both, 1, 1)).astype(BF)
        cos, sin = rotary_tables(seg)
        ctx, d_lin = attention(lin, g_ctx, cos, sin, seg, keep[m, 0])

        pre = dot(n2, m_up, 1, 0)
        cdf = 0.5 * (1.0 + lax.erf(pre * math.sqrt(0.5)))
        hidden = (pre * cdf).astype(BF)
        slope = cdf + pre * (math.sqrt(0.5 / math.pi) * jnp.exp(-0.5 * pre * pre))
        d_pre = (dot(gg, m_down, 1, 1) * slope).astype(BF)

        part = dot(ctx, m_out, 0, 0) + dot(hidden, m_down, 1, 0)
        branch = lax.psum_scatter(part.astype(BF), "tensor", scatter_dimension=0, tiled=True)
        outs.append((rows.astype(F32) + branch.astype(F32)).astype(BF))

        one = dot(d_lin, m_qkv, 0, 1)
        two = dot(d_pre, m_up, 1, 1)
        total = (gain[0] * one + gain[1] * two).astype(BF)
        total = lax.psum_scatter(total, "tensor", scatter_dimension=0, tiled=True).astype(F32)
        own, inverse = normalized(rows.astype(F32))
        grad = total - jnp.mean(total, axis=-1, keepdims=True)
        grad = grad - own * jnp.mean(total * own, axis=-1, keepdims=True)
        grads.append((gy[m, 0].astype(F32) + grad * inverse).astype(BF))

        norms = jnp.stack([jnp.sum(one * standard, axis=0), jnp.sum(two * standard, axis=0),
                           jnp.sum(one, axis=0), jnp.sum(two, axis=0)])
        lo_ctx = dot(ctx, a_out, 0, 0).astype(BF)
        lo_hid = dot(hidden, a_down, 1, 0).astype(BF)
        d_b_out = SCALE * jnp.stack([dot(lo_ctx, gg, 0, 0), dot(lo_hid, gg, 0, 0)], axis=1)
        d_a_out = dot(ctx, low_grad[:, :128], 1, 0)
        d_a_down = dot(hidden, low_grad[:, 128:], 0, 0)
        d_b_qkv = SCALE * jnp.stack([
            dot(low3[:, 128 * i:128 * (i + 1)], d_lin[width * i:width * (i + 1)], 0, 1) for i in range(3)])
        d_b_up = SCALE * dot(low1, d_pre, 0, 0)
        back = [(SCALE * dot(d_lin[width * i:width * (i + 1)], b_qkv[i], 0, 1)).astype(BF) for i in range(3)]
        back.append((SCALE * dot(d_pre, b_up, 1, 1)).astype(BF))
        d_a_in = jnp.stack([dot(back[i], n1 if i < 3 else n2, 0, 0) for i in range(4)], axis=1)
        terms = (d_a_in, d_b_qkv, d_b_up, d_a_out, d_a_down, d_b_out, norms)
        sums = terms if sums is None else tuple(p + q for p, q in zip(sums, terms))

    d_a_in, d_b_qkv, d_b_up, d_a_out, d_a_down, d_b_out, norms = sums
    d_a_in = lax.psum_scatter(d_a_in, "tensor", scatter_dimension=0, tiled=True)
    d_b_out = lax.psum_scatter(d_b_out, "tensor", scatter_dimension=0, tiled=True)
    d_a_in, d_b_qkv, d_b_up, d_a_out, d_a_down, d_b_out = lax.psum(
        (d_a_in, d_b_qkv, d_b_up, d_a_out, d_a_down, d_b_out), "dp")
    norms = lax.psum(norms, ("dp", "tensor"))
    return (jnp.stack(outs)[:, None], jnp.stack(grads)[:, None], norms[:2], norms[2:],
            jnp.transpose(d_a_in, (1, 2, 0)), d_b_qkv, d_b_up, d_a_out, d_a_down,
            jnp.transpose(d_b_out, (1, 0, 2)))


def solution(mesh):
    in_specs = (
        P(None, "dp", "tensor", None),
        P(None, "dp", "tensor", None),
        P(None, "dp", None),
        P(None, "dp", None),
        P(),
        P(),
        P(None, None, "tensor"),
        P("tensor", None),
        P(None, "tensor"),
        P("tensor", None),
        P(None, None, "tensor"),
        P(None, None, "tensor"),
        P(None, "tensor"),
        P("tensor", None),
        P("tensor", None),
        P(None, "tensor", None),
    )
    out_specs = (
        P(None, "dp", "tensor", None),
        P(None, "dp", "tensor", None),
        P(),
        P(),
        P(None, None, "tensor"),
        P(None, None, "tensor"),
        P(None, "tensor"),
        P("tensor", None),
        P("tensor", None),
        P(None, "tensor", None),
    )
    return jax.shard_map(
        on_device, mesh=mesh, in_specs=in_specs, out_specs=out_specs, check_vma=False
    )
```

```python
import functools
import math

import jax
import jax.numpy as jnp
from jax import lax
from jax.experimental import pallas as pl
from jax.experimental.pallas import tpu as pltpu
from jax.sharding import PartitionSpec as P

HEAD = 64
HALF = 8
N_DOCS = 5
TILE = 256
SLOTS = 5
EPSILON = 1e-05
SCALE = 0.25
F32 = jnp.float32
BF = jnp.bfloat16


def dot(a, b, ca, cb):
    return lax.dot_general(a, b, (((ca,), (cb,)), ((), ())), preferred_element_type=F32)


def attention_kernel(heads, lo_ref, lin_ref, g_ref, cos_ref, sin_ref, segq_ref, segk_ref,
                     ctx_ref, dlin_ref, qt, kt, vt, kn, vn, qz, acc, s_scr, e_scr):
    length = lin_ref.shape[2]
    blocks = length // TILE

    def rotate(z, cos, sin):
        a, b = z[:HALF], z[HALF:2 * HALF]
        return jnp.concatenate([a * cos - b * sin, b * cos + a * sin, z[2 * HALF:]], axis=0)

    def prepare(c, carry):
        cols = pl.ds(pl.multiple_of(c * TILE, TILE), TILE)
        cos, sin = cos_ref[:, cols], sin_ref[:, cols]
        for h in range(heads):
            rows = pl.ds(h * HEAD, HEAD)
            q = rotate(lin_ref[0, pl.ds(h * HEAD, HEAD), cols], cos, sin).astype(BF).astype(F32) * 0.125
            k = rotate(lin_ref[1, pl.ds(h * HEAD, HEAD), cols], cos, sin)
            v = lin_ref[2, pl.ds(h * HEAD, HEAD), cols]
            qt[rows, cols] = q.astype(BF)
            kt[rows, cols] = k.astype(BF)
            vt[rows, cols] = v.astype(BF)
            kn[h, cols, :] = jnp.transpose(k).astype(BF)
            vn[h, cols, :] = jnp.transpose(v).astype(BF)
            qn = jnp.transpose(q)
            qz[h, cols, :] = jnp.concatenate([jnp.zeros_like(qn), qn], axis=1).astype(BF)
            acc[h, cols, :] = jnp.zeros((TILE, 2 * HEAD), F32)
        return carry

    lax.fori_loop(0, blocks, prepare, 0)

    def query_block(qb, carry):
        lo = lo_ref[qb]
        qcols = pl.ds(pl.multiple_of(qb * TILE, TILE), TILE)
        segq = segq_ref[:, qcols]

        def scores(kb, tops):
            krows = pl.ds(pl.multiple_of(kb * TILE, TILE), TILE)
            kpos = kb * TILE + lax.broadcasted_iota(jnp.int32, (TILE, TILE), 0)
            qpos = qb * TILE + lax.broadcasted_iota(jnp.int32, (TILE, TILE), 1)
            allowed = ((segk_ref[krows, :] == segq) & (kpos <= qpos)) | (kpos == qpos)
            out = []
            for h in range(heads):
                s = dot(kn[h, krows, :], qt[pl.ds(h * HEAD, HEAD), qcols], 1, 0)
                s = jnp.where(allowed, s, -1e30)
                s_scr[h, kb - lo] = s
                out.append(jnp.maximum(tops[h], jnp.max(s, axis=0, keepdims=True)))
            return tuple(out)

        tops = lax.fori_loop(lo, qb + 1, scores,
                             tuple(jnp.full((1, TILE), -1e30, F32) for _ in range(heads)))

        def weights(kb, sums):
            kcols = pl.ds(pl.multiple_of(kb * TILE, TILE), TILE)
            out = []
            for h in range(heads):
                e = jnp.exp(s_scr[h, kb - lo] - tops[h])
                low = e.astype(BF)
                e_scr[h, kb - lo] = low
                total, ctx = sums[h]
                out.append((total + jnp.sum(e, axis=0, keepdims=True),
                            ctx + dot(vt[pl.ds(h * HEAD, HEAD), kcols], low, 1, 0)))
            return tuple(out)

        sums = lax.fori_loop(lo, qb + 1, weights,
                             tuple((jnp.zeros((1, TILE), F32), jnp.zeros((HEAD, TILE), F32))
                                   for _ in range(heads)))
        gts, gzs, terms = [], [], []
        for h in range(heads):
            rows = pl.ds(h * HEAD, HEAD)
            inverse = 1.0 / sums[h][0]
            ctx = sums[h][1] * inverse
            ctx_ref[rows, qcols] = ctx.astype(BF)
            g = g_ref[rows, qcols].astype(F32)
            terms.append(jnp.sum(g * ctx, axis=0, keepdims=True) * inverse)
            g = g * inverse
            gts.append(g.astype(BF))
            gn = jnp.transpose(g)
            gzs.append(jnp.concatenate([gn, jnp.zeros_like(gn)], axis=1).astype(BF))

        def backward(kb, dqs):
            krows = pl.ds(pl.multiple_of(kb * TILE, TILE), TILE)
            out = []
            for h in range(heads):
                low = e_scr[h, kb - lo]
                dp = dot(vn[h, krows, :], gts[h], 1, 0)
                ds = (low.astype(F32) * (dp - terms[h])).astype(BF)
                acc[h, krows, :] += dot(low, gzs[h], 1, 0) + dot(ds, qz[h, qcols, :], 1, 0)
                out.append(dqs[h] + dot(kt[pl.ds(h * HEAD, HEAD), krows], ds, 1, 0))
            return tuple(out)

        dqs = lax.fori_loop(lo, qb + 1, backward,
                            tuple(jnp.zeros((HEAD, TILE), F32) for _ in range(heads)))
        cos, sin = cos_ref[:, qcols], sin_ref[:, qcols]
        for h in range(heads):
            dlin_ref[0, pl.ds(h * HEAD, HEAD), qcols] = rotate(dqs[h] * 0.125, cos, -sin).astype(BF)
        return carry

    lax.fori_loop(0, blocks, query_block, 0)

    def finish(c, carry):
        cols = pl.ds(pl.multiple_of(c * TILE, TILE), TILE)
        cos, sin = cos_ref[:, cols], sin_ref[:, cols]
        for h in range(heads):
            both = jnp.transpose(acc[h, cols, :])
            dlin_ref[1, pl.ds(h * HEAD, HEAD), cols] = rotate(both[HEAD:], cos, -sin).astype(BF)
            dlin_ref[2, pl.ds(h * HEAD, HEAD), cols] = both[:HEAD].astype(BF)
        return carry

    lax.fori_loop(0, blocks, finish, 0)


def attention(lin, g, cos, sin, segment, keep):
    width, length = g.shape
    heads = min(4, width // HEAD)
    wide = heads * HEAD
    starts = jnp.sum(segment[None, :] < jnp.arange(N_DOCS, dtype=jnp.int32)[:, None], axis=1)
    firsts = segment[::TILE]
    lo = jnp.sum(jnp.where(firsts[:, None] == jnp.arange(N_DOCS)[None, :], starts[None, :], 0), axis=1)
    lo = (lo // TILE).astype(jnp.int32)
    segk = jnp.where(keep == 1, segment, -1)[:, None]
    vmem = pl.BlockSpec(memory_space=pltpu.VMEM)
    three = pl.BlockSpec((3, wide, length), lambda i, lo: (0, i, 0))
    single = pl.BlockSpec((wide, length), lambda i, lo: (i, 0))
    return pl.pallas_call(
        functools.partial(attention_kernel, heads),
        grid_spec=pltpu.PrefetchScalarGridSpec(
            num_scalar_prefetch=1,
            grid=(width // wide,),
            in_specs=[three, single] + [vmem] * 4,
            out_specs=[single, three],
            scratch_shapes=[
                pltpu.VMEM((wide, length), BF),
                pltpu.VMEM((wide, length), BF),
                pltpu.VMEM((wide, length), BF),
                pltpu.VMEM((heads, length, HEAD), BF),
                pltpu.VMEM((heads, length, HEAD), BF),
                pltpu.VMEM((heads, length, 2 * HEAD), BF),
                pltpu.VMEM((heads, length, 2 * HEAD), F32),
                pltpu.VMEM((heads, SLOTS, TILE, TILE), F32),
                pltpu.VMEM((heads, SLOTS, TILE, TILE), BF),
            ]),
        out_shape=[jax.ShapeDtypeStruct((width, length), BF), jax.ShapeDtypeStruct((3, width, length), BF)],
        compiler_params=pltpu.CompilerParams(vmem_limit_bytes=60 << 20),
        name="attention",
        cost_estimate=pl.CostEstimate(flops=10 * width * length * 768, transcendentals=width * length * 12,
                                      bytes_accessed=26 * width * length),
    )(lo, lin, g, cos, sin, segment[None, :], segk)


def rotary_tables(segment):
    length = segment.shape[0]
    starts = jnp.sum(segment[None, :] < jnp.arange(N_DOCS, dtype=jnp.int32)[:, None], axis=1)
    begin = jnp.sum(jnp.where(segment[None, :] == jnp.arange(N_DOCS)[:, None], starts[:, None], 0), axis=0)
    position = (jnp.arange(length, dtype=jnp.int32) - begin).astype(F32)
    exponent = jnp.arange(HALF, dtype=F32) / HALF
    frequency = jnp.exp(-math.log(10000.0) * exponent)
    angles = frequency[:, None] * position[None, :]
    return jnp.cos(angles), jnp.sin(angles)


def normalized(values):
    average = jnp.mean(values, axis=-1, keepdims=True)
    centered = values - average
    variance = jnp.mean(centered * centered, axis=-1, keepdims=True)
    inverse = lax.rsqrt(variance + EPSILON)
    return centered * inverse, inverse


def by_features(x, gy, segment, keep, gain, bias, w_qkv, w_out, w_up, w_down,
              a_in, b_qkv, b_up, a_out, a_down, b_out):
    width = w_qkv.shape[2]
    micro = x.shape[0]
    a_full = lax.all_gather(a_in, "tensor", axis=2, tiled=True)
    b_full = lax.all_gather(b_out, "tensor", axis=1, tiled=True)

    m_qkv = jnp.concatenate([
        (w_qkv[i].astype(F32) + SCALE * dot(a_full[i], b_qkv[i], 1, 0)).astype(BF) for i in range(3)
    ], axis=1)
    m_up = (w_up.astype(F32) + SCALE * dot(a_full[3], b_up, 1, 0)).astype(BF)
    m_out = (w_out.astype(F32) + SCALE * dot(a_out, b_full[0], 1, 0)).astype(BF)
    m_down = (w_down.astype(F32) + SCALE * dot(a_down, b_full[1], 1, 0)).astype(BF)
    a_three = jnp.concatenate([a_full[0], a_full[1], a_full[2]], axis=1)
    b_both = jnp.concatenate([b_full[0], b_full[1]], axis=0)

    outs, grads, sums = [], [], None
    for m in range(micro):
        rows, seg = x[m, 0], segment[m, 0]
        xg = lax.all_gather(rows, "tensor", axis=0, tiled=True)
        gg = lax.all_gather(gy[m, 0], "tensor", axis=0, tiled=True)
        standard, _ = normalized(xg.astype(F32))
        n1 = (standard * gain[0] + bias[0]).astype(BF)
        n2 = (standard * gain[1] + bias[1]).astype(BF)
        lin = dot(m_qkv, n1, 0, 1)
        low3 = dot(n1, a_three, 1, 0).astype(BF)
        low1 = dot(n2, a_full[3], 1, 0).astype(BF)
        g_ctx = dot(m_out, gg, 1, 1).astype(BF)
        low_grad = (SCALE * dot(gg, b_both, 1, 1)).astype(BF)
        cos, sin = rotary_tables(seg)
        ctx, d_lin = attention(lin.reshape(3, width, -1), g_ctx, cos, sin, seg, keep[m, 0])
        d_lin = d_lin.reshape(3 * width, -1)

        pre = dot(n2, m_up, 1, 0)
        cdf = 0.5 * (1.0 + lax.erf(pre * math.sqrt(0.5)))
        hidden = (pre * cdf).astype(BF)
        slope = cdf + pre * (math.sqrt(0.5 / math.pi) * jnp.exp(-0.5 * pre * pre))
        d_pre = (dot(gg, m_down, 1, 1) * slope).astype(BF)

        part = dot(ctx, m_out, 0, 0) + dot(hidden, m_down, 1, 0)
        branch = lax.psum_scatter(part.astype(BF), "tensor", scatter_dimension=0, tiled=True)
        outs.append((rows.astype(F32) + branch.astype(F32)).astype(BF))

        one = dot(d_lin, m_qkv, 0, 1)
        two = dot(d_pre, m_up, 1, 1)
        total = (gain[0] * one + gain[1] * two).astype(BF)
        total = lax.psum_scatter(total, "tensor", scatter_dimension=0, tiled=True).astype(F32)
        own, inverse = normalized(rows.astype(F32))
        grad = total - jnp.mean(total, axis=-1, keepdims=True)
        grad = grad - own * jnp.mean(total * own, axis=-1, keepdims=True)
        grads.append((gy[m, 0].astype(F32) + grad * inverse).astype(BF))

        norms = jnp.stack([jnp.sum(one * standard, axis=0), jnp.sum(two * standard, axis=0),
                           jnp.sum(one, axis=0), jnp.sum(two, axis=0)])
        lo_ctx = dot(ctx, a_out, 0, 0).astype(BF)
        lo_hid = dot(hidden, a_down, 1, 0).astype(BF)
        d_b_out = SCALE * jnp.stack([dot(lo_ctx, gg, 0, 0), dot(lo_hid, gg, 0, 0)], axis=1)
        d_a_out = dot(ctx, low_grad[:, :128], 1, 0)
        d_a_down = dot(hidden, low_grad[:, 128:], 0, 0)
        d_b_qkv = SCALE * jnp.stack([
            dot(low3[:, 128 * i:128 * (i + 1)], d_lin[width * i:width * (i + 1)], 0, 1) for i in range(3)])
        d_b_up = SCALE * dot(low1, d_pre, 0, 0)
        back = [(SCALE * dot(d_lin[width * i:width * (i + 1)], b_qkv[i], 0, 1)).astype(BF) for i in range(3)]
        back.append((SCALE * dot(d_pre, b_up, 1, 1)).astype(BF))
        d_a_in = jnp.stack([dot(back[i], n1 if i < 3 else n2, 0, 0) for i in range(4)], axis=1)
        terms = (d_a_in, d_b_qkv, d_b_up, d_a_out, d_a_down, d_b_out, norms)
        sums = terms if sums is None else tuple(p + q for p, q in zip(sums, terms))

    d_a_in, d_b_qkv, d_b_up, d_a_out, d_a_down, d_b_out, norms = sums
    d_a_in = lax.psum_scatter(d_a_in, "tensor", scatter_dimension=0, tiled=True)
    d_b_out = lax.psum_scatter(d_b_out, "tensor", scatter_dimension=0, tiled=True)
    d_a_in, d_b_qkv, d_b_up, d_a_out, d_a_down, d_b_out = lax.psum(
        (d_a_in, d_b_qkv, d_b_up, d_a_out, d_a_down, d_b_out), "dp")
    norms = lax.psum(norms, ("dp", "tensor"))
    return (jnp.stack(outs)[:, None], jnp.stack(grads)[:, None], norms[:2], norms[2:],
            jnp.transpose(d_a_in, (1, 2, 0)), d_b_qkv, d_b_up, d_a_out, d_a_down,
            jnp.transpose(d_b_out, (1, 0, 2)))


RANK = 128


def send(v, k):
    return lax.ppermute(v, "tensor", [(i, i ^ k) for i in range(4)])


def swap(v, k=1):
    return lax.ppermute(v, "dp", [(i, i ^ k) for i in range(lax.axis_size("dp"))])


def after(v, *others):
    return lax.optimization_barrier((v,) + others)[0]


def gather(v):
    half = v.shape[0] // 2
    one, two = send(v, 1), send(v, 2)
    far = jnp.concatenate([send(two[:half], 1), send(one[half:], 2)], axis=0)
    return [v, one, two, far]


def ordered(parts, t):
    low, high = t % 2 == 1, t // 2 == 1
    parts = [jnp.where(low, parts[k ^ 1], parts[k]) for k in range(4)]
    return [jnp.where(high, parts[k ^ 2], parts[k]) for k in range(4)]


def pick(v, axis, index, size):
    return lax.dynamic_slice_in_dim(v, index * size, size, axis)


def to_group(v, c):
    parts = v.reshape(2, 2, 256, -1)
    mine = pick(parts, 1, c, 1)[:, 0]
    got = swap(pick(parts, 1, 1 - c, 1)[:, 0])
    groups = jnp.where(c == 0, jnp.stack([mine, got], 1), jnp.stack([got, mine], 1)).reshape(4, 256, -1)
    own = lax.all_to_all(groups, "tensor", 0, 0, tiled=True)
    other = swap(own)
    return jnp.where(c == 0, jnp.stack([own, other], 1), jnp.stack([other, own], 1)).reshape(2048, -1)


def half_rows(v, c):
    return pick(v.reshape(4, 2, 256, -1), 1, c, 1)[:, 0]


def from_group(own, c):
    got = lax.all_to_all(own, "tensor", 0, 0, tiled=True).reshape(2, 2, 256, -1)
    mine = pick(got, 1, c, 1)[:, 0]
    other = swap(pick(got, 1, 1 - c, 1)[:, 0])
    return jnp.where(c == 0, jnp.stack([mine, other], 1), jnp.stack([other, mine], 1)).reshape(2, 512, -1)


def reduced(parts, z):
    total = parts[0]
    for k in (1, 2, 3):
        total = total + send(parts[k].astype(BF), k).astype(F32)
    rows = total.shape[0] // 4
    own = pick(total, 0, z, rows)
    for k in (1, 2, 3):
        own = own + swap(pick(total, 0, z ^ k, rows).astype(BF), 2 * k).astype(F32)
    whole = jnp.zeros((4, rows, 128), F32)
    whole = lax.dynamic_update_slice_in_dim(whole, own[None], z, 0)
    low = own.astype(BF)
    for k in (1, 2, 3):
        whole = lax.dynamic_update_slice_in_dim(whole, swap(low, 2 * k).astype(F32)[None], z ^ k, 0)
    return whole.reshape(4 * rows, 128)


def by_groups(x, gy, segment, keep, gain, bias, w_qkv, w_out, w_up, w_down,
              a_in, b_qkv, b_up, a_out, a_down, b_out):
    d = lax.axis_index("dp")
    c, z, t = d % 2, d // 2, lax.axis_index("tensor")
    tables = jnp.stack([segment[:, 0], keep[:, 0]], 1)
    others = swap(tables)
    same = t % 2 == c
    pair = jnp.where(same, tables, others)
    seg, kept = jnp.where(t // 2 == 0, pair[0], pair[1])

    x_full = to_group(x[:, 0], c)
    small = jnp.concatenate([
        pick(b_qkv, 2, c, 128).reshape(384, 128),
        pick(a_out, 0, c, 128),
        pick(a_down, 0, c, 512),
        jnp.concatenate([pick(b_up, 1, c, 512)[:, 128 * i:128 * (i + 1)] for i in range(4)], axis=0),
        jnp.concatenate([a_in[i] for i in range(4)], axis=1),
        jnp.concatenate([b_out.reshape(64, 1024)[:, 128 * i:128 * (i + 1)] for i in range(8)], axis=0),
    ], axis=0)
    small = gather(small)
    qkv = gather(pick(w_qkv, 2, c, 128).reshape(3 * 1024, 128))
    g_full = to_group(after(gy[:, 0], x_full), c)
    out = gather(after(pick(w_out, 0, c, 128), x_full))
    up = gather(after(pick(w_up, 1, c, 512), x_full, qkv[3]))
    down = gather(after(pick(w_down, 0, c, 512), x_full, up[3]))

    a_ranks = ordered([p[1536:2560] for p in small], t)
    a_full = [jnp.concatenate([p[:, 32 * i:32 * (i + 1)] for p in a_ranks], axis=1) for i in range(4)]
    b_ranks = ordered([jnp.concatenate([p[2560 + 64 * i:2560 + 64 * (i + 1)] for i in range(8)], axis=1)
                       for p in small], t)
    b_full = [jnp.concatenate([p[32 * i:32 * (i + 1)] for p in b_ranks], axis=0) for i in range(2)]
    b_qkv_all = [jnp.concatenate([p[128 * i:128 * (i + 1)] for p in small], axis=1) for i in range(3)]
    a_out_all = jnp.concatenate([p[384:512] for p in small], axis=0)
    a_down_all = jnp.concatenate([p[512:1024] for p in small], axis=0)
    b_up_all = jnp.concatenate([p[1024 + 128 * i:1152 + 128 * i] for p in small for i in range(4)], axis=1)

    m_qkv = jnp.concatenate([
        (jnp.concatenate([p[1024 * i:1024 * (i + 1)] for p in qkv], axis=1).astype(F32)
         + SCALE * dot(a_full[i], b_qkv_all[i], 1, 0)).astype(BF) for i in range(3)], axis=1)
    m_up = (jnp.concatenate(up, axis=1).astype(F32) + SCALE * dot(a_full[3], b_up_all, 1, 0)).astype(BF)
    m_out = (jnp.concatenate(out, axis=0).astype(F32) + SCALE * dot(a_out_all, b_full[0], 1, 0)).astype(BF)
    m_down = (jnp.concatenate(down, axis=0).astype(F32) + SCALE * dot(a_down_all, b_full[1], 1, 0)).astype(BF)
    a_three = jnp.concatenate(a_full[:3], axis=1)
    b_both = jnp.concatenate(b_full, axis=0)

    standard, inverse = normalized(x_full.astype(F32))
    n1 = (standard * gain[0] + bias[0]).astype(BF)
    n2 = (standard * gain[1] + bias[1]).astype(BF)
    lin = dot(m_qkv, n1, 0, 1).reshape(3, 512, 2048)
    low3 = dot(n1, a_three, 1, 0).astype(BF)
    low1 = dot(n2, a_full[3], 1, 0).astype(BF)
    g_ctx = dot(m_out, g_full, 1, 1).astype(BF)
    low_grad = (SCALE * dot(g_full, b_both, 1, 1)).astype(BF)
    cos, sin = rotary_tables(seg)
    ctx, d_lin = attention(lin, g_ctx, cos, sin, seg, kept)

    pre = dot(n2, m_up, 1, 0)
    cdf = 0.5 * (1.0 + lax.erf(pre * math.sqrt(0.5)))
    hidden = (pre * cdf).astype(BF)
    slope = cdf + pre * (math.sqrt(0.5 / math.pi) * jnp.exp(-0.5 * pre * pre))
    d_pre = (dot(g_full, m_down, 1, 1) * slope).astype(BF)

    part = dot(ctx, m_out, 0, 0) + dot(hidden, m_down, 1, 0)
    theirs = swap(half_rows(part, 1 - c).astype(BF))
    y = half_rows(x_full, c).astype(F32) + half_rows(part, c) + theirs.astype(F32)
    y = from_group(y.astype(BF), c)

    d_rows = d_lin.reshape(1536, 2048)
    one = dot(d_rows, m_qkv, 0, 1)
    two = dot(d_pre, m_up, 1, 1)
    total = gain[0] * one + gain[1] * two
    theirs = swap(half_rows(total, 1 - c).astype(BF))
    total = half_rows(total, c) + theirs.astype(F32)
    own = half_rows(standard, c)
    grad = total - jnp.mean(total, axis=-1, keepdims=True)
    grad = grad - own * jnp.mean(total * own, axis=-1, keepdims=True)
    grad = half_rows(g_full, c).astype(F32) + grad * half_rows(inverse, c)
    grad = from_group(grad.astype(BF), c)

    norms = jnp.stack([jnp.sum(one * standard, axis=0), jnp.sum(two * standard, axis=0),
                       jnp.sum(one, axis=0), jnp.sum(two, axis=0)])
    lo_ctx = dot(ctx, a_out_all, 0, 0).astype(BF)
    lo_hid = dot(hidden, a_down_all, 1, 0).astype(BF)
    d_b_out = SCALE * jnp.stack([dot(lo_ctx, g_full, 0, 0), dot(lo_hid, g_full, 0, 0)])
    d_a_out = dot(ctx, low_grad[:, :RANK], 1, 0)
    d_a_down = dot(hidden, low_grad[:, RANK:], 0, 0)
    d_b_qkv = [SCALE * dot(low3[:, RANK * i:RANK * (i + 1)], d_lin[i], 0, 1) for i in range(3)]
    d_b_up = SCALE * dot(low1, d_pre, 0, 0)
    back = [(SCALE * dot(d_lin[i], b_qkv_all[i], 0, 1)).astype(BF) for i in range(3)]
    back.append((SCALE * dot(d_pre, b_up_all, 1, 1)).astype(BF))
    d_a_in = jnp.stack([dot(back[i], n1 if i < 3 else n2, 0, 0) for i in range(4)])

    shared = jnp.concatenate([d_a_in.reshape(4, 4, 32, 1024), d_b_out.reshape(2, 4, 32, 1024)], axis=0)
    shared = jnp.concatenate([jnp.swapaxes(shared, 0, 1).reshape(4, 192, 1024), norms.reshape(4, 1, 1024),
                              jnp.zeros((4, 7, 1024), F32)], axis=1)
    shared = pick(shared, 2, c, 512) + swap(pick(shared, 2, 1 - c, 512).astype(BF)).astype(F32)
    shared = jnp.concatenate([shared[:, :, 128 * i:128 * (i + 1)] for i in range(4)], axis=1)
    shared = ordered([shared[i] for i in range(4)], t)
    parts = []
    for k in range(4):
        parts.append(jnp.concatenate(
            [d_b_qkv[i][:, 128 * k:128 * (k + 1)] for i in range(3)]
            + [d_b_up[:, 512 * k + 128 * i:512 * k + 128 * (i + 1)] for i in range(4)]
            + [d_a_out[128 * k:128 * (k + 1)], d_a_down[512 * k:512 * (k + 1)], shared[k]], axis=0))
    mine = reduced(parts, z)
    other = swap(mine)
    first, second = jnp.where(c == 0, mine, other), jnp.where(c == 0, other, mine)
    r_b_qkv = jnp.stack([jnp.concatenate([v[128 * i:128 * (i + 1)] for v in (first, second)], 1) for i in range(3)])
    r_b_up = jnp.concatenate([v[384 + 128 * i:512 + 128 * i] for v in (first, second) for i in range(4)], axis=1)
    r_a_out = jnp.concatenate([v[896:1024] for v in (first, second)], axis=0)
    r_a_down = jnp.concatenate([v[1024:1536] for v in (first, second)], axis=0)
    rest = jnp.concatenate([v[1536 + 200 * i:1736 + 200 * i] for v in (first, second) for i in range(4)], axis=1)
    r_a_in = jnp.transpose(rest[:128].reshape(4, 32, 1024), (0, 2, 1))
    r_b_out = rest[128:192].reshape(2, 32, 1024)
    row = rest[192:200]
    rows = ordered([row] + [send(row, k) for k in (1, 2, 3)], t)
    norms = jnp.stack([r[0] for r in rows])
    return (y[:, None], grad[:, None], norms[:2], norms[2:], r_a_in, r_b_qkv, r_b_up, r_a_out, r_a_down, r_b_out)


def solution(mesh):
    in_specs = (
        P(None, "dp", "tensor", None),
        P(None, "dp", "tensor", None),
        P(None, "dp", None),
        P(None, "dp", None),
        P(),
        P(),
        P(None, None, "tensor"),
        P("tensor", None),
        P(None, "tensor"),
        P("tensor", None),
        P(None, None, "tensor"),
        P(None, None, "tensor"),
        P(None, "tensor"),
        P("tensor", None),
        P("tensor", None),
        P(None, "tensor", None),
    )
    out_specs = (
        P(None, "dp", "tensor", None),
        P(None, "dp", "tensor", None),
        P(),
        P(),
        P(None, None, "tensor"),
        P(None, None, "tensor"),
        P(None, "tensor"),
        P("tensor", None),
        P("tensor", None),
        P(None, "tensor", None),
    )
    small = mesh.shape["tensor"] == 4 and mesh.shape["dp"] == 8
    return jax.shard_map(
        by_groups if small else by_features, mesh=mesh, in_specs=in_specs, out_specs=out_specs, check_vma=False
    )
```

```python
import functools
import math

import jax
import jax.numpy as jnp
from jax import lax
from jax.experimental import pallas as pl
from jax.experimental.pallas import tpu as pltpu
from jax.sharding import PartitionSpec as P

HEAD = 64
HALF = 8
N_DOCS = 5
TILE = 256
SLOTS = 5
EPSILON = 1e-05
SCALE = 0.25
F32 = jnp.float32
BF = jnp.bfloat16


def dot(a, b, ca, cb):
    return lax.dot_general(a, b, (((ca,), (cb,)), ((), ())), preferred_element_type=F32)


def attention_kernel(heads, lo_ref, lin_ref, g_ref, cos_ref, sin_ref, segq_ref, segk_ref,
                     ctx_ref, dlin_ref, qt, kt, vt, kn, vn, qz, acc, s_scr, e_scr):
    length = lin_ref.shape[2]
    blocks = length // TILE

    def rotate(z, cos, sin):
        a, b = z[:HALF], z[HALF:2 * HALF]
        return jnp.concatenate([a * cos - b * sin, b * cos + a * sin, z[2 * HALF:]], axis=0)

    def prepare(c, carry):
        cols = pl.ds(pl.multiple_of(c * TILE, TILE), TILE)
        cos, sin = cos_ref[:, cols], sin_ref[:, cols]
        for h in range(heads):
            rows = pl.ds(h * HEAD, HEAD)
            q = rotate(lin_ref[0, pl.ds(h * HEAD, HEAD), cols], cos, sin).astype(BF).astype(F32) * 0.125
            k = rotate(lin_ref[1, pl.ds(h * HEAD, HEAD), cols], cos, sin)
            v = lin_ref[2, pl.ds(h * HEAD, HEAD), cols]
            qt[rows, cols] = q.astype(BF)
            kt[rows, cols] = k.astype(BF)
            vt[rows, cols] = v.astype(BF)
            kn[h, cols, :] = jnp.transpose(k).astype(BF)
            vn[h, cols, :] = jnp.transpose(v).astype(BF)
            qn = jnp.transpose(q)
            qz[h, cols, :] = jnp.concatenate([jnp.zeros_like(qn), qn], axis=1).astype(BF)
            acc[h, cols, :] = jnp.zeros((TILE, 2 * HEAD), F32)
        return carry

    lax.fori_loop(0, blocks, prepare, 0)

    def query_block(qb, carry):
        lo = lo_ref[qb]
        qcols = pl.ds(pl.multiple_of(qb * TILE, TILE), TILE)
        segq = segq_ref[:, qcols]

        def scores(kb, tops):
            krows = pl.ds(pl.multiple_of(kb * TILE, TILE), TILE)
            kpos = kb * TILE + lax.broadcasted_iota(jnp.int32, (TILE, TILE), 0)
            qpos = qb * TILE + lax.broadcasted_iota(jnp.int32, (TILE, TILE), 1)
            allowed = ((segk_ref[krows, :] == segq) & (kpos <= qpos)) | (kpos == qpos)
            out = []
            for h in range(heads):
                s = dot(kn[h, krows, :], qt[pl.ds(h * HEAD, HEAD), qcols], 1, 0)
                s = jnp.where(allowed, s, -1e30)
                s_scr[h, kb - lo] = s
                out.append(jnp.maximum(tops[h], jnp.max(s, axis=0, keepdims=True)))
            return tuple(out)

        tops = lax.fori_loop(lo, qb + 1, scores,
                             tuple(jnp.full((1, TILE), -1e30, F32) for _ in range(heads)))

        def weights(kb, sums):
            kcols = pl.ds(pl.multiple_of(kb * TILE, TILE), TILE)
            out = []
            for h in range(heads):
                e = jnp.exp(s_scr[h, kb - lo] - tops[h])
                low = e.astype(BF)
                e_scr[h, kb - lo] = low
                total, ctx = sums[h]
                out.append((total + jnp.sum(e, axis=0, keepdims=True),
                            ctx + dot(vt[pl.ds(h * HEAD, HEAD), kcols], low, 1, 0)))
            return tuple(out)

        sums = lax.fori_loop(lo, qb + 1, weights,
                             tuple((jnp.zeros((1, TILE), F32), jnp.zeros((HEAD, TILE), F32))
                                   for _ in range(heads)))
        gts, gzs, terms = [], [], []
        for h in range(heads):
            rows = pl.ds(h * HEAD, HEAD)
            inverse = 1.0 / sums[h][0]
            ctx = sums[h][1] * inverse
            ctx_ref[rows, qcols] = ctx.astype(BF)
            g = g_ref[rows, qcols].astype(F32)
            terms.append(jnp.sum(g * ctx, axis=0, keepdims=True) * inverse)
            g = g * inverse
            gts.append(g.astype(BF))
            gn = jnp.transpose(g)
            gzs.append(jnp.concatenate([gn, jnp.zeros_like(gn)], axis=1).astype(BF))

        def backward(kb, dqs):
            krows = pl.ds(pl.multiple_of(kb * TILE, TILE), TILE)
            out = []
            for h in range(heads):
                low = e_scr[h, kb - lo]
                dp = dot(vn[h, krows, :], gts[h], 1, 0)
                ds = (low.astype(F32) * (dp - terms[h])).astype(BF)
                acc[h, krows, :] += dot(low, gzs[h], 1, 0) + dot(ds, qz[h, qcols, :], 1, 0)
                out.append(dqs[h] + dot(kt[pl.ds(h * HEAD, HEAD), krows], ds, 1, 0))
            return tuple(out)

        dqs = lax.fori_loop(lo, qb + 1, backward,
                            tuple(jnp.zeros((HEAD, TILE), F32) for _ in range(heads)))
        cos, sin = cos_ref[:, qcols], sin_ref[:, qcols]
        for h in range(heads):
            dlin_ref[0, pl.ds(h * HEAD, HEAD), qcols] = rotate(dqs[h] * 0.125, cos, -sin).astype(BF)
        return carry

    lax.fori_loop(0, blocks, query_block, 0)

    def finish(c, carry):
        cols = pl.ds(pl.multiple_of(c * TILE, TILE), TILE)
        cos, sin = cos_ref[:, cols], sin_ref[:, cols]
        for h in range(heads):
            both = jnp.transpose(acc[h, cols, :])
            dlin_ref[1, pl.ds(h * HEAD, HEAD), cols] = rotate(both[HEAD:], cos, -sin).astype(BF)
            dlin_ref[2, pl.ds(h * HEAD, HEAD), cols] = both[:HEAD].astype(BF)
        return carry

    lax.fori_loop(0, blocks, finish, 0)


def attention(lin, g, cos, sin, segment, keep):
    width, length = g.shape
    heads = min(4, width // HEAD)
    wide = heads * HEAD
    starts = jnp.sum(segment[None, :] < jnp.arange(N_DOCS, dtype=jnp.int32)[:, None], axis=1)
    firsts = segment[::TILE]
    lo = jnp.sum(jnp.where(firsts[:, None] == jnp.arange(N_DOCS)[None, :], starts[None, :], 0), axis=1)
    lo = (lo // TILE).astype(jnp.int32)
    segk = jnp.where(keep == 1, segment, -1)[:, None]
    vmem = pl.BlockSpec(memory_space=pltpu.VMEM)
    three = pl.BlockSpec((3, wide, length), lambda i, lo: (0, i, 0))
    single = pl.BlockSpec((wide, length), lambda i, lo: (i, 0))
    return pl.pallas_call(
        functools.partial(attention_kernel, heads),
        grid_spec=pltpu.PrefetchScalarGridSpec(
            num_scalar_prefetch=1,
            grid=(width // wide,),
            in_specs=[three, single] + [vmem] * 4,
            out_specs=[single, three],
            scratch_shapes=[
                pltpu.VMEM((wide, length), BF),
                pltpu.VMEM((wide, length), BF),
                pltpu.VMEM((wide, length), BF),
                pltpu.VMEM((heads, length, HEAD), BF),
                pltpu.VMEM((heads, length, HEAD), BF),
                pltpu.VMEM((heads, length, 2 * HEAD), BF),
                pltpu.VMEM((heads, length, 2 * HEAD), F32),
                pltpu.VMEM((heads, SLOTS, TILE, TILE), F32),
                pltpu.VMEM((heads, SLOTS, TILE, TILE), BF),
            ]),
        out_shape=[jax.ShapeDtypeStruct((width, length), BF), jax.ShapeDtypeStruct((3, width, length), BF)],
        compiler_params=pltpu.CompilerParams(vmem_limit_bytes=60 << 20),
        name="attention",
        cost_estimate=pl.CostEstimate(flops=10 * width * length * 768, transcendentals=width * length * 12,
                                      bytes_accessed=26 * width * length),
    )(lo, lin, g, cos, sin, segment[None, :], segk)


def rotary_tables(segment):
    length = segment.shape[0]
    starts = jnp.sum(segment[None, :] < jnp.arange(N_DOCS, dtype=jnp.int32)[:, None], axis=1)
    begin = jnp.sum(jnp.where(segment[None, :] == jnp.arange(N_DOCS)[:, None], starts[:, None], 0), axis=0)
    position = (jnp.arange(length, dtype=jnp.int32) - begin).astype(F32)
    exponent = jnp.arange(HALF, dtype=F32) / HALF
    frequency = jnp.exp(-math.log(10000.0) * exponent)
    angles = frequency[:, None] * position[None, :]
    return jnp.cos(angles), jnp.sin(angles)


def normalized(values):
    average = jnp.mean(values, axis=-1, keepdims=True)
    centered = values - average
    variance = jnp.mean(centered * centered, axis=-1, keepdims=True)
    inverse = lax.rsqrt(variance + EPSILON)
    return centered * inverse, inverse


def by_features(x, gy, segment, keep, gain, bias, w_qkv, w_out, w_up, w_down,
              a_in, b_qkv, b_up, a_out, a_down, b_out):
    width = w_qkv.shape[2]
    micro = x.shape[0]
    a_full = lax.all_gather(a_in, "tensor", axis=2, tiled=True)
    b_full = lax.all_gather(b_out, "tensor", axis=1, tiled=True)

    m_qkv = jnp.concatenate([
        (w_qkv[i].astype(F32) + SCALE * dot(a_full[i], b_qkv[i], 1, 0)).astype(BF) for i in range(3)
    ], axis=1)
    m_up = (w_up.astype(F32) + SCALE * dot(a_full[3], b_up, 1, 0)).astype(BF)
    m_out = (w_out.astype(F32) + SCALE * dot(a_out, b_full[0], 1, 0)).astype(BF)
    m_down = (w_down.astype(F32) + SCALE * dot(a_down, b_full[1], 1, 0)).astype(BF)
    a_three = jnp.concatenate([a_full[0], a_full[1], a_full[2]], axis=1)
    b_both = jnp.concatenate([b_full[0], b_full[1]], axis=0)

    outs, grads, sums = [], [], None
    for m in range(micro):
        rows, seg = x[m, 0], segment[m, 0]
        xg = lax.all_gather(rows, "tensor", axis=0, tiled=True)
        gg = lax.all_gather(gy[m, 0], "tensor", axis=0, tiled=True)
        standard, _ = normalized(xg.astype(F32))
        n1 = (standard * gain[0] + bias[0]).astype(BF)
        n2 = (standard * gain[1] + bias[1]).astype(BF)
        lin = dot(m_qkv, n1, 0, 1)
        low3 = dot(n1, a_three, 1, 0).astype(BF)
        low1 = dot(n2, a_full[3], 1, 0).astype(BF)
        g_ctx = dot(m_out, gg, 1, 1).astype(BF)
        low_grad = (SCALE * dot(gg, b_both, 1, 1)).astype(BF)
        cos, sin = rotary_tables(seg)
        ctx, d_lin = attention(lin.reshape(3, width, -1), g_ctx, cos, sin, seg, keep[m, 0])
        d_lin = d_lin.reshape(3 * width, -1)

        pre = dot(n2, m_up, 1, 0)
        cdf = 0.5 * (1.0 + lax.erf(pre * math.sqrt(0.5)))
        hidden = (pre * cdf).astype(BF)
        slope = cdf + pre * (math.sqrt(0.5 / math.pi) * jnp.exp(-0.5 * pre * pre))
        d_pre = (dot(gg, m_down, 1, 1) * slope).astype(BF)

        part = dot(ctx, m_out, 0, 0) + dot(hidden, m_down, 1, 0)
        branch = lax.psum_scatter(part.astype(BF), "tensor", scatter_dimension=0, tiled=True)
        outs.append((rows.astype(F32) + branch.astype(F32)).astype(BF))

        one = dot(d_lin, m_qkv, 0, 1)
        two = dot(d_pre, m_up, 1, 1)
        total = (gain[0] * one + gain[1] * two).astype(BF)
        total = lax.psum_scatter(total, "tensor", scatter_dimension=0, tiled=True).astype(F32)
        own, inverse = normalized(rows.astype(F32))
        grad = total - jnp.mean(total, axis=-1, keepdims=True)
        grad = grad - own * jnp.mean(total * own, axis=-1, keepdims=True)
        grads.append((gy[m, 0].astype(F32) + grad * inverse).astype(BF))

        norms = jnp.stack([jnp.sum(one * standard, axis=0), jnp.sum(two * standard, axis=0),
                           jnp.sum(one, axis=0), jnp.sum(two, axis=0)])
        lo_ctx = dot(ctx, a_out, 0, 0).astype(BF)
        lo_hid = dot(hidden, a_down, 1, 0).astype(BF)
        d_b_out = SCALE * jnp.stack([dot(lo_ctx, gg, 0, 0), dot(lo_hid, gg, 0, 0)], axis=1)
        d_a_out = dot(ctx, low_grad[:, :128], 1, 0)
        d_a_down = dot(hidden, low_grad[:, 128:], 0, 0)
        d_b_qkv = SCALE * jnp.stack([
            dot(low3[:, 128 * i:128 * (i + 1)], d_lin[width * i:width * (i + 1)], 0, 1) for i in range(3)])
        d_b_up = SCALE * dot(low1, d_pre, 0, 0)
        back = [(SCALE * dot(d_lin[width * i:width * (i + 1)], b_qkv[i], 0, 1)).astype(BF) for i in range(3)]
        back.append((SCALE * dot(d_pre, b_up, 1, 1)).astype(BF))
        d_a_in = jnp.stack([dot(back[i], n1 if i < 3 else n2, 0, 0) for i in range(4)], axis=1)
        terms = (d_a_in, d_b_qkv, d_b_up, d_a_out, d_a_down, d_b_out, norms)
        sums = terms if sums is None else tuple(p + q for p, q in zip(sums, terms))

    d_a_in, d_b_qkv, d_b_up, d_a_out, d_a_down, d_b_out, norms = sums
    d_a_in = lax.psum_scatter(d_a_in, "tensor", scatter_dimension=0, tiled=True)
    d_b_out = lax.psum_scatter(d_b_out, "tensor", scatter_dimension=0, tiled=True)
    d_a_in, d_b_qkv, d_b_up, d_a_out, d_a_down, d_b_out = lax.psum(
        (d_a_in, d_b_qkv, d_b_up, d_a_out, d_a_down, d_b_out), "dp")
    norms = lax.psum(norms, ("dp", "tensor"))
    return (jnp.stack(outs)[:, None], jnp.stack(grads)[:, None], norms[:2], norms[2:],
            jnp.transpose(d_a_in, (1, 2, 0)), d_b_qkv, d_b_up, d_a_out, d_a_down,
            jnp.transpose(d_b_out, (1, 0, 2)))


RANK = 128


MESH = pl.DeviceIdType.MESH


def place():
    d = lax.axis_index("dp")
    return d // 2, d % 2, lax.axis_index("tensor")


def meet(z, c, t):
    barrier = pltpu.get_barrier_semaphore()
    for h in (0, 1):
        for k in range(4):
            if h or k:
                pl.semaphore_signal(barrier, 1, device_id=(2 * z + (c ^ h), t ^ k), device_id_type=MESH)
    pl.semaphore_wait(barrier, 7)


def remote(src, dst, send_sem, recv_sem, device):
    return pltpu.make_async_remote_copy(src_ref=src, dst_ref=dst, send_sem=send_sem, recv_sem=recv_sem,
                                        device_id=device, device_id_type=MESH)


class Rows:
    def __init__(self, v, full, sems, stage, local, z, c, t):
        self.v, self.full, self.sems, self.stage, self.local = v, full, sems, stage, local
        self.z, self.c, self.t = z, c, t

    def rows(self, s, h):
        return self.full.at[pl.ds(pl.multiple_of(s * 512 + h * 256, 256), 256)]

    def block(self, m, h):
        return self.v.at[m, pl.ds(pl.multiple_of(h * 256, 256), 256)]

    def copy(self, m, other):
        h = self.c ^ other
        return remote(self.block(m, h), self.rows(self.t, h), self.sems.at[2 * m + other], self.sems.at[4 + self.t],
                      (2 * self.z + h, 2 * m + self.c))

    def forward(self, s):
        part = self.rows(s, self.c)
        return remote(part, part, self.sems.at[8 + s], self.sems.at[12 + s], (2 * self.z + (self.c ^ 1), self.t))

    def start(self):
        for m in (0, 1):
            away = 2 * m + self.c != self.t

            @pl.when(away)
            def _():
                self.copy(m, 0).start()

            self.copy(m, 1).start()

            @pl.when(jnp.logical_not(away))
            def _():
                pltpu.make_async_copy(self.block(m, self.c), self.stage, self.local.at[0]).start()

    def relay(self):
        mine = self.t % 2 == self.c

        @pl.when(mine)
        def _():
            pltpu.make_async_copy(self.block(0, self.c), self.stage, self.local.at[0]).wait()
            pltpu.make_async_copy(self.stage, self.rows(self.t, self.c), self.sems.at[4 + self.t]).start()

        for k in (0, 1, 2, 3):
            s = self.t ^ k
            pltpu.make_async_copy(self.stage, self.rows(s, self.c), self.sems.at[4 + s]).wait()
            self.forward(s).start()

    def finish(self):
        for s in range(4):
            part = self.rows(s, self.c ^ 1)
            remote(part, part, self.sems.at[8 + s], self.sems.at[12 + s], (2 * self.z + (self.c ^ 1), self.t)).wait_recv()
            self.forward(s).wait_send()
        for m in (0, 1):
            @pl.when(2 * m + self.c != self.t)
            def _():
                self.copy(m, 0).wait_send()

            self.copy(m, 1).wait_send()


class Blocks:
    def __init__(self, own, where, sems, stage, local, halves, z, c, t):
        self.own, self.where, self.sems, self.stage, self.local = own, where, sems, stage, local
        self.halves, self.t, self.d = halves, t, 2 * z + c

    def first(self, k):
        return remote(self.own, self.where(self.t), self.sems.at[k - 1], self.sems.at[3 + k - 1], (self.d, self.t ^ k))

    def arrival(self, k):
        spot = self.where(self.t ^ k)
        return remote(spot, spot, self.sems.at[k - 1], self.sems.at[3 + k - 1], (self.d, self.t ^ k))

    def second(self, k):
        part = self.halves(self.where(self.t ^ (3 - k)), k - 1)
        return remote(part, part, self.sems.at[6 + k - 1], self.sems.at[8 + k - 1], (self.d, self.t ^ k))

    def start(self):
        for k in ((1, 2) if self.halves else (1, 2, 3)):
            self.first(k).start()
        pltpu.make_async_copy(self.own, self.stage, self.local.at[0]).start()

    def store(self):
        pltpu.make_async_copy(self.own, self.stage, self.local.at[0]).wait()
        pltpu.make_async_copy(self.stage, self.where(self.t), self.local.at[1]).start()

    def relay(self):
        if self.halves:
            for k in (1, 2):
                self.arrival(3 - k).wait_recv()
                self.second(k).start()

    def finish(self):
        pltpu.make_async_copy(self.stage, self.where(self.t), self.local.at[1]).wait()
        if self.halves:
            for k in (1, 2):
                part = self.halves(self.where(self.t ^ 3), k - 1)
                remote(part, part, self.sems.at[6 + k - 1], self.sems.at[8 + k - 1], (self.d, self.t ^ k)).wait_recv()
                self.first(k).wait_send()
                self.second(k).wait_send()
        else:
            for k in (1, 2, 3):
                self.arrival(k).wait_recv()
                self.first(k).wait_send()


def aligned(i, n):
    return pl.ds(pl.multiple_of(i * n, n), n)


def front_kernel(x, g, wq, wo, ain, bq, ao, bo,
                 xf, gf, wqf, wof, ainf, bqf, aof, bof,
                 row_sems, sems, local, xs, gs, wqs, wos, ains, bqs, aos, bos):
    z, c, t = place()
    meet(z, c, t)
    at = dict(z=z, c=c, t=t)
    x_rows = Rows(x, xf, row_sems.at[0], xs, local.at[0], **at)
    g_rows = Rows(g, gf, row_sems.at[1], gs, local.at[1], **at)
    qkv = Blocks(wq.at[:, :, aligned(c, 128)], lambda i: wqf.at[:, :, aligned(i, 128)], sems.at[0], wqs, local.at[2],
                 lambda v, h: v.at[:, pl.ds(h * 512, 512)], **at)
    into = Blocks(ain, lambda i: ainf.at[:, aligned(i, 32)], sems.at[1], ains, local.at[3], None, **at)
    second = Blocks(bq.at[:, :, aligned(c, 128)], lambda i: bqf.at[:, :, aligned(i, 128)], sems.at[2], bqs, local.at[4],
                    None, **at)
    out = Blocks(wo.at[aligned(c, 128)], lambda i: wof.at[aligned(i, 128)], sems.at[3], wos, local.at[5],
                 lambda v, h: v.at[pl.ds(h * 64, 64)], **at)
    a_out = Blocks(ao.at[aligned(c, 128)], lambda i: aof.at[aligned(i, 128)], sems.at[4], aos, local.at[6], None, **at)
    b_out = Blocks(bo, lambda i: bof.at[:, aligned(i, 32)], sems.at[5], bos, local.at[7], None, **at)
    x_rows.start()
    into.start()
    second.start()
    qkv.start()
    x_rows.relay()
    for v in (into, second, qkv):
        v.store()
    g_rows.start()
    qkv.relay()
    for v in (b_out, a_out, out):
        v.start()
    g_rows.relay()
    for v in (b_out, a_out, out):
        v.store()
    out.relay()
    for v in (x_rows, into, second, qkv, g_rows, b_out, a_out, out):
        v.finish()


def front(x, g, wq, wo, ain, bq, ao, bo):
    shapes = [(2048, 1024), (2048, 1024), (3, 1024, 512), (512, 1024), (4, 128, 1024), (3, 128, 512), (512, 128),
              (2, 128, 1024)]
    anywhere = pl.BlockSpec(memory_space=pl.ANY)
    return pl.pallas_call(
        front_kernel,
        in_specs=[anywhere] * 8,
        out_specs=[anywhere] * 8,
        out_shape=[jax.ShapeDtypeStruct(s, BF) for s in shapes],
        scratch_shapes=[
            pltpu.SemaphoreType.DMA((2, 16)),
            pltpu.SemaphoreType.DMA((6, 10)),
            pltpu.SemaphoreType.DMA((8, 2)),
            pltpu.VMEM((256, 1024), BF),
            pltpu.VMEM((256, 1024), BF),
            pltpu.VMEM((3, 1024, 128), BF),
            pltpu.VMEM((128, 1024), BF),
            pltpu.VMEM((4, 32, 1024), BF),
            pltpu.VMEM((3, 128, 128), BF),
            pltpu.VMEM((128, 128), BF),
            pltpu.VMEM((2, 32, 1024), BF),
        ],
        compiler_params=pltpu.CompilerParams(collective_id=0, has_side_effects=True),
        name="front",
    )(x, g, wq, wo, ain, bq, ao, bo)


def back_kernel(rows, dbq, dbu, dao, dad, dsh, dno,
                out, obq, obu, oao, oad, osh, ono,
                row_sems, share_sems, cross_sems, z_sems, last_sems, norm_sems,
                sh_in, sh, rbq, rbu, rao, rad, rsh, pbq, pbu, pao, pad, psh, qbq, qbu, qao, qad, qsh, no_in, no_sum):
    z, c, t = place()
    meet_all(z, c, t)
    d = 2 * z + c
    sibling = (2 * z + (c ^ 1), t)

    home = t % 2
    local = home == c
    spot = aligned(c, 256)

    def row(k):
        return remote(rows.at[t ^ k], out.at[t // 2, spot], row_sems.at[k], row_sems.at[4 + (t // 2) * 2 + c],
                      (2 * z + home, t ^ k))

    def own_row():
        return pltpu.make_async_copy(rows.at[t], out.at[t // 2, spot], row_sems.at[4 + (t // 2) * 2 + c])

    @pl.when(local)
    def _():
        own_row().start()

    @pl.when(jnp.logical_not(local))
    def _():
        row(0).start()

    for k in (1, 2, 3):
        row(k).start()

    peers = (sibling, (d, t ^ 1), (d, t ^ 2), (d ^ 2, t), (d ^ 4, t))

    def norm(i):
        return remote(dno if i == 0 else no_sum.at[i - 1], no_in.at[i], norm_sems.at[0, i], norm_sems.at[1, i], peers[i])

    def norm_next(i):
        norm(i).wait_recv()
        total = (dno[...] if i == 0 else no_sum[i - 1]) + no_in[i]
        if i < 4:
            no_sum[i] = total
            norm(i + 1).start()
        else:
            ono[...] = total

    norm(0).start()

    def share():
        return remote(dsh.at[:, :, aligned(c ^ 1, 512)], sh_in, share_sems.at[0], share_sems.at[1], sibling)

    share().start()
    share().wait_recv()
    norm_next(0)
    for i in range(6):
        sh[i] = (dsh[i, :, aligned(c, 512)].astype(F32) + sh_in[i].astype(F32)).astype(BF)

    def parts(j):
        return (dbq.at[:, :, aligned(j, 128)], dbu.at[:, aligned(j, 512)], dao.at[aligned(j, 128)],
                dad.at[aligned(j, 512)], sh.at[:, aligned(j, 32)])

    got = (rbq, rbu, rao, rad, rsh)

    def cross(k, i):
        return remote(parts(t ^ k)[i], got[i].at[k - 1], cross_sems.at[0, k - 1, i], cross_sems.at[1, k - 1, i], (d, t ^ k))

    for k in (1, 2, 3):
        for i in range(5):
            cross(k, i).start()
    norm_next(1)
    norm_next(2)
    sums = (pbq, pbu, pao, pad, psh)
    for i in range(5):
        for k in (1, 2, 3):
            cross(k, i).wait_recv()
        total = parts(t)[i][...].astype(F32)
        for k in (0, 1, 2):
            total = total + got[i][k].astype(F32)
        sums[i][0] = total.astype(BF)

    halves = (qbq, qbu, qao, qad, qsh)

    def along(step, i):
        return remote(sums[i].at[step], halves[i].at[step], z_sems.at[0, step, i], z_sems.at[1, step, i],
                      (d ^ (2 << step), t))

    for i in range(5):
        along(0, i).start()
    norm_next(3)
    for i in range(5):
        along(0, i).wait_recv()
        sums[i][1] = (sums[i][0].astype(F32) + halves[i][0].astype(F32)).astype(BF)
        along(1, i).start()
    norm_next(4)
    result = (obq.at[:, :, aligned(c, 128)], obu.at[:, aligned(c, 512)], oao.at[aligned(c, 128)],
              oad.at[aligned(c, 512)], osh.at[:, :, aligned(c, 512)])
    theirs = (obq.at[:, :, aligned(c ^ 1, 128)], obu.at[:, aligned(c ^ 1, 512)], oao.at[aligned(c ^ 1, 128)],
              oad.at[aligned(c ^ 1, 512)], osh.at[:, :, aligned(c ^ 1, 512)])

    def last(i):
        return remote(result[i], result[i], last_sems.at[0, i], last_sems.at[1, i], sibling)

    for i in range(5):
        along(1, i).wait_recv()
        result[i][...] = sums[i][1].astype(F32) + halves[i][1].astype(F32)
        last(i).start()

    for i in range(5):
        remote(theirs[i], theirs[i], last_sems.at[0, i], last_sems.at[1, i], sibling).wait_recv()
        last(i).wait_send()
        along(0, i).wait_send()
        along(1, i).wait_send()
        for k in (1, 2, 3):
            cross(k, i).wait_send()
    share().wait_send()
    for i in range(5):
        norm(i).wait_send()
    for k in (1, 2, 3):
        row(k).wait_send()

    @pl.when(jnp.logical_not(local))
    def _():
        row(0).wait_send()

    for m in (0, 1):
        for h in (0, 1):
            pltpu.make_async_copy(rows.at[0], out.at[m, pl.ds(256 * h, 256)], row_sems.at[4 + 2 * m + h]).wait()


def meet_all(z, c, t):
    barrier = pltpu.get_barrier_semaphore()
    for h in (0, 1):
        for k in range(4):
            if h or k:
                pl.semaphore_signal(barrier, 1, device_id=(2 * z + (c ^ h), t ^ k), device_id_type=MESH)
    for k in (1, 2):
        pl.semaphore_signal(barrier, 1, device_id=(2 * (z ^ k) + c, t), device_id_type=MESH)
    pl.semaphore_wait(barrier, 9)


def back(rows, dbq, dbu, dao, dad, dsh, dno):
    vmem = pl.BlockSpec(memory_space=pltpu.VMEM)
    part = [(3, 128, 128), (128, 512), (128, 128), (512, 128), (6, 32, 512)]
    outs = [((2, 512, 1024), BF), ((3, 128, 256), F32), ((128, 1024), F32), ((256, 128), F32), ((1024, 128), F32),
            ((6, 32, 1024), F32), ((4, 1024), F32)]
    return pl.pallas_call(
        back_kernel,
        in_specs=[vmem] * 7,
        out_specs=[pl.BlockSpec(memory_space=pl.ANY)] + [vmem] * 6,
        out_shape=[jax.ShapeDtypeStruct(s, d) for s, d in outs],
        scratch_shapes=[
            pltpu.SemaphoreType.DMA((8,)),
            pltpu.SemaphoreType.DMA((2,)),
            pltpu.SemaphoreType.DMA((2, 3, 5)),
            pltpu.SemaphoreType.DMA((2, 2, 5)),
            pltpu.SemaphoreType.DMA((2, 5)),
            pltpu.SemaphoreType.DMA((2, 5)),
            pltpu.VMEM((6, 128, 512), BF),
            pltpu.VMEM((6, 128, 512), BF),
        ] + [pltpu.VMEM((3,) + s, BF) for s in part] + [pltpu.VMEM((2,) + s, BF) for s in part + part] + [
            pltpu.VMEM((5, 4, 1024), F32),
            pltpu.VMEM((4, 4, 1024), F32),
        ],
        compiler_params=pltpu.CompilerParams(collective_id=1, has_side_effects=True),
        name="back",
    )(rows, dbq, dbu, dao, dad, dsh, dno)


def swap(v, k=1):
    return lax.ppermute(v, "dp", [(i, i ^ k) for i in range(lax.axis_size("dp"))])


def pick(v, axis, index, size):
    return lax.dynamic_slice_in_dim(v, index * size, size, axis)


def half_rows(v, c):
    return pick(v.reshape(4, 2, 256, -1), 1, c, 1)[:, 0]


def from_group(own, c):
    got = lax.all_to_all(own, "tensor", 0, 0, tiled=True).reshape(2, 2, 256, -1)
    mine = pick(got, 1, c, 1)[:, 0]
    other = swap(pick(got, 1, 1 - c, 1)[:, 0])
    return jnp.where(c == 0, jnp.stack([mine, other], 1), jnp.stack([other, mine], 1)).reshape(2, 512, -1)


def by_groups(x, gy, segment, keep, gain, bias, w_qkv, w_out, w_up, w_down,
              a_in, b_qkv, b_up, a_out, a_down, b_out):
    z, c, t = place()
    tables = jnp.stack([segment[:, 0], keep[:, 0]], 1)
    pair = jnp.where(t % 2 == c, tables, swap(tables))
    seg, kept = jnp.where(t // 2 == 0, pair[0], pair[1])

    x_full, g_full, qkv, out, a_full, b_qkv_all, a_out_all, b_full = front(
        x[:, 0], gy[:, 0], w_qkv, w_out, jnp.swapaxes(a_in, 1, 2), b_qkv, a_out, b_out)
    up, down = lax.optimization_barrier((
        jnp.concatenate([pick(w_up, 1, c, 512), pick(b_up, 1, c, 512)], axis=0),
        jnp.concatenate([pick(w_down, 0, c, 512), pick(a_down, 0, c, 512)], axis=1), x_full))[:2]
    up = lax.all_gather(up, "tensor", axis=0)
    down = lax.all_gather(down, "tensor", axis=0, tiled=True)
    w_up_all = jnp.concatenate([up[i, :1024] for i in range(4)], axis=1)
    b_up_all = jnp.concatenate([up[i, 1024:] for i in range(4)], axis=1)
    w_down_all, a_down_all = down[:, :1024], down[:, 1024:]

    m_qkv = (qkv.astype(F32) + SCALE * jnp.einsum("nrk,nrc->nkc", a_full[:3], b_qkv_all,
                                                  preferred_element_type=F32)).astype(BF)
    m_up = (w_up_all.astype(F32) + SCALE * dot(a_full[3], b_up_all, 0, 0)).astype(BF)
    m_out = (out.astype(F32) + SCALE * dot(a_out_all, b_full[0], 1, 0)).astype(BF)
    m_down = (w_down_all.astype(F32) + SCALE * dot(a_down_all, b_full[1], 1, 0)).astype(BF)
    a_three = a_full[:3].reshape(3 * RANK, 1024)
    b_both = b_full.reshape(2 * RANK, 1024)

    standard, inverse = normalized(x_full.astype(F32))
    n1 = (standard * gain[0] + bias[0]).astype(BF)
    n2 = (standard * gain[1] + bias[1]).astype(BF)
    lin = jnp.einsum("nkc,sk->ncs", m_qkv, n1, preferred_element_type=F32)
    low3 = dot(n1, a_three, 1, 1).astype(BF)
    low1 = dot(n2, a_full[3], 1, 1).astype(BF)
    g_ctx = dot(m_out, g_full, 1, 1).astype(BF)
    low_grad = (SCALE * dot(g_full, b_both, 1, 1)).astype(BF)
    cos, sin = rotary_tables(seg)
    ctx, d_lin = attention(lin, g_ctx, cos, sin, seg, kept)

    pre = dot(n2, m_up, 1, 0)
    cdf = 0.5 * (1.0 + lax.erf(pre * math.sqrt(0.5)))
    hidden = (pre * cdf).astype(BF)
    slope = cdf + pre * (math.sqrt(0.5 / math.pi) * jnp.exp(-0.5 * pre * pre))
    d_pre = (dot(g_full, m_down, 1, 1) * slope).astype(BF)

    part = dot(ctx, m_out, 0, 0) + dot(hidden, m_down, 1, 0)
    theirs = swap(half_rows(part, 1 - c).astype(BF))
    y = half_rows(x_full, c).astype(F32) + half_rows(part, c) + theirs.astype(F32)
    y = from_group(y.astype(BF), c)

    one = jnp.einsum("ncs,nkc->sk", d_lin, m_qkv, preferred_element_type=F32)
    two = dot(d_pre, m_up, 1, 1)
    total = gain[0] * one + gain[1] * two
    theirs = swap(half_rows(total, 1 - c).astype(BF))
    total = half_rows(total, c) + theirs.astype(F32)
    own = half_rows(standard, c)
    grad = total - jnp.mean(total, axis=-1, keepdims=True)
    grad = grad - own * jnp.mean(total * own, axis=-1, keepdims=True)
    grad = half_rows(g_full, c).astype(F32) + grad * half_rows(inverse, c)

    norms = jnp.stack([jnp.sum(one * standard, axis=0), jnp.sum(two * standard, axis=0),
                       jnp.sum(one, axis=0), jnp.sum(two, axis=0)])
    lo_ctx = dot(ctx, a_out_all, 0, 0).astype(BF)
    lo_hid = dot(hidden, a_down_all, 1, 0).astype(BF)
    d_a_out = dot(ctx, low_grad[:, :RANK], 1, 0).astype(BF)
    d_a_down = dot(hidden, low_grad[:, RANK:], 0, 0).astype(BF)
    d_b_qkv = jnp.stack([(SCALE * dot(low3[:, RANK * i:RANK * (i + 1)], d_lin[i], 0, 1)).astype(BF) for i in range(3)])
    d_b_up = (SCALE * dot(low1, d_pre, 0, 0)).astype(BF)
    back3 = [(SCALE * dot(d_lin[i], b_qkv_all[i], 0, 1)).astype(BF) for i in range(3)]
    back1 = (SCALE * dot(d_pre, b_up_all, 1, 1)).astype(BF)
    shared = jnp.stack([dot(v, n1, 0, 0).astype(BF) for v in back3] + [dot(back1, n2, 0, 0).astype(BF)]
                       + [(SCALE * dot(v, g_full, 0, 0)).astype(BF) for v in (lo_ctx, lo_hid)])
    grad, r_b_qkv, r_b_up, r_a_out, r_a_down, rest, norms = back(
        grad.astype(BF), d_b_qkv, d_b_up, d_a_out, d_a_down, shared, norms)
    r_a_in = jnp.swapaxes(rest[:4], 1, 2)
    return (y[:, None], grad[:, None], norms[:2], norms[2:], r_a_in, r_b_qkv, r_b_up, r_a_out, r_a_down, rest[4:])


def solution(mesh):
    in_specs = (
        P(None, "dp", "tensor", None),
        P(None, "dp", "tensor", None),
        P(None, "dp", None),
        P(None, "dp", None),
        P(),
        P(),
        P(None, None, "tensor"),
        P("tensor", None),
        P(None, "tensor"),
        P("tensor", None),
        P(None, None, "tensor"),
        P(None, None, "tensor"),
        P(None, "tensor"),
        P("tensor", None),
        P("tensor", None),
        P(None, "tensor", None),
    )
    out_specs = (
        P(None, "dp", "tensor", None),
        P(None, "dp", "tensor", None),
        P(),
        P(),
        P(None, None, "tensor"),
        P(None, None, "tensor"),
        P(None, "tensor"),
        P("tensor", None),
        P("tensor", None),
        P(None, "tensor", None),
    )
    small = mesh.shape["tensor"] == 4 and mesh.shape["dp"] == 8
    return jax.shard_map(
        by_groups if small else by_features, mesh=mesh, in_specs=in_specs, out_specs=out_specs, check_vma=False
    )
```

```python
import functools
import math

import jax
import jax.numpy as jnp
from jax import lax
from jax.experimental import pallas as pl
from jax.experimental.pallas import tpu as pltpu
from jax.sharding import PartitionSpec as P

HEAD = 64
HALF = 8
N_DOCS = 5
TILE = 256
SLOTS = 5
EPSILON = 1e-05
SCALE = 0.25
F32 = jnp.float32
BF = jnp.bfloat16


def dot(a, b, ca, cb):
    return lax.dot_general(a, b, (((ca,), (cb,)), ((), ())), preferred_element_type=F32)


def attention_kernel(heads, lo_ref, lin_ref, g_ref, cos_ref, sin_ref, segq_ref, segk_ref,
                     ctx_ref, dlin_ref, qt, kt, vt, kn, vn, qz, acc, s_scr, e_scr):
    length = lin_ref.shape[2]
    blocks = length // TILE

    def rotate(z, cos, sin):
        a, b = z[:HALF], z[HALF:2 * HALF]
        return jnp.concatenate([a * cos - b * sin, b * cos + a * sin, z[2 * HALF:]], axis=0)

    def prepare(c, carry):
        cols = pl.ds(pl.multiple_of(c * TILE, TILE), TILE)
        cos, sin = cos_ref[:, cols], sin_ref[:, cols]
        for h in range(heads):
            rows = pl.ds(h * HEAD, HEAD)
            q = rotate(lin_ref[0, pl.ds(h * HEAD, HEAD), cols], cos, sin).astype(BF).astype(F32) * 0.125
            k = rotate(lin_ref[1, pl.ds(h * HEAD, HEAD), cols], cos, sin)
            v = lin_ref[2, pl.ds(h * HEAD, HEAD), cols]
            qt[rows, cols] = q.astype(BF)
            kt[rows, cols] = k.astype(BF)
            vt[rows, cols] = v.astype(BF)
            kn[h, cols, :] = jnp.transpose(k).astype(BF)
            vn[h, cols, :] = jnp.transpose(v).astype(BF)
            qn = jnp.transpose(q)
            qz[h, cols, :] = jnp.concatenate([jnp.zeros_like(qn), qn], axis=1).astype(BF)
            acc[h, cols, :] = jnp.zeros((TILE, 2 * HEAD), F32)
        return carry

    lax.fori_loop(0, blocks, prepare, 0)

    def query_block(qb, carry):
        lo = lo_ref[qb]
        qcols = pl.ds(pl.multiple_of(qb * TILE, TILE), TILE)
        segq = segq_ref[:, qcols]

        def scores(kb, tops):
            krows = pl.ds(pl.multiple_of(kb * TILE, TILE), TILE)
            kpos = kb * TILE + lax.broadcasted_iota(jnp.int32, (TILE, TILE), 0)
            qpos = qb * TILE + lax.broadcasted_iota(jnp.int32, (TILE, TILE), 1)
            allowed = ((segk_ref[krows, :] == segq) & (kpos <= qpos)) | (kpos == qpos)
            out = []
            for h in range(heads):
                s = dot(kn[h, krows, :], qt[pl.ds(h * HEAD, HEAD), qcols], 1, 0)
                s = jnp.where(allowed, s, -1e30)
                s_scr[h, kb - lo] = s
                out.append(jnp.maximum(tops[h], jnp.max(s, axis=0, keepdims=True)))
            return tuple(out)

        tops = lax.fori_loop(lo, qb + 1, scores,
                             tuple(jnp.full((1, TILE), -1e30, F32) for _ in range(heads)))

        def weights(kb, sums):
            kcols = pl.ds(pl.multiple_of(kb * TILE, TILE), TILE)
            out = []
            for h in range(heads):
                e = jnp.exp(s_scr[h, kb - lo] - tops[h])
                low = e.astype(BF)
                e_scr[h, kb - lo] = low
                total, ctx = sums[h]
                out.append((total + jnp.sum(e, axis=0, keepdims=True),
                            ctx + dot(vt[pl.ds(h * HEAD, HEAD), kcols], low, 1, 0)))
            return tuple(out)

        sums = lax.fori_loop(lo, qb + 1, weights,
                             tuple((jnp.zeros((1, TILE), F32), jnp.zeros((HEAD, TILE), F32))
                                   for _ in range(heads)))
        gts, gzs, terms = [], [], []
        for h in range(heads):
            rows = pl.ds(h * HEAD, HEAD)
            inverse = 1.0 / sums[h][0]
            ctx = sums[h][1] * inverse
            ctx_ref[rows, qcols] = ctx.astype(BF)
            g = g_ref[rows, qcols].astype(F32)
            terms.append(jnp.sum(g * ctx, axis=0, keepdims=True) * inverse)
            g = g * inverse
            gts.append(g.astype(BF))
            gn = jnp.transpose(g)
            gzs.append(jnp.concatenate([gn, jnp.zeros_like(gn)], axis=1).astype(BF))

        def backward(kb, dqs):
            krows = pl.ds(pl.multiple_of(kb * TILE, TILE), TILE)
            out = []
            for h in range(heads):
                low = e_scr[h, kb - lo]
                dp = dot(vn[h, krows, :], gts[h], 1, 0)
                ds = (low.astype(F32) * (dp - terms[h])).astype(BF)
                acc[h, krows, :] += dot(low, gzs[h], 1, 0) + dot(ds, qz[h, qcols, :], 1, 0)
                out.append(dqs[h] + dot(kt[pl.ds(h * HEAD, HEAD), krows], ds, 1, 0))
            return tuple(out)

        dqs = lax.fori_loop(lo, qb + 1, backward,
                            tuple(jnp.zeros((HEAD, TILE), F32) for _ in range(heads)))
        cos, sin = cos_ref[:, qcols], sin_ref[:, qcols]
        for h in range(heads):
            dlin_ref[0, pl.ds(h * HEAD, HEAD), qcols] = rotate(dqs[h] * 0.125, cos, -sin).astype(BF)
        return carry

    lax.fori_loop(0, blocks, query_block, 0)

    def finish(c, carry):
        cols = pl.ds(pl.multiple_of(c * TILE, TILE), TILE)
        cos, sin = cos_ref[:, cols], sin_ref[:, cols]
        for h in range(heads):
            both = jnp.transpose(acc[h, cols, :])
            dlin_ref[1, pl.ds(h * HEAD, HEAD), cols] = rotate(both[HEAD:], cos, -sin).astype(BF)
            dlin_ref[2, pl.ds(h * HEAD, HEAD), cols] = both[:HEAD].astype(BF)
        return carry

    lax.fori_loop(0, blocks, finish, 0)


def attention(lin, g, cos, sin, segment, keep):
    width, length = g.shape
    heads = min(4, width // HEAD)
    wide = heads * HEAD
    starts = jnp.sum(segment[None, :] < jnp.arange(N_DOCS, dtype=jnp.int32)[:, None], axis=1)
    firsts = segment[::TILE]
    lo = jnp.sum(jnp.where(firsts[:, None] == jnp.arange(N_DOCS)[None, :], starts[None, :], 0), axis=1)
    lo = (lo // TILE).astype(jnp.int32)
    segk = jnp.where(keep == 1, segment, -1)[:, None]
    vmem = pl.BlockSpec(memory_space=pltpu.VMEM)
    three = pl.BlockSpec((3, wide, length), lambda i, lo: (0, i, 0))
    single = pl.BlockSpec((wide, length), lambda i, lo: (i, 0))
    return pl.pallas_call(
        functools.partial(attention_kernel, heads),
        grid_spec=pltpu.PrefetchScalarGridSpec(
            num_scalar_prefetch=1,
            grid=(width // wide,),
            in_specs=[three, single] + [vmem] * 4,
            out_specs=[single, three],
            scratch_shapes=[
                pltpu.VMEM((wide, length), BF),
                pltpu.VMEM((wide, length), BF),
                pltpu.VMEM((wide, length), BF),
                pltpu.VMEM((heads, length, HEAD), BF),
                pltpu.VMEM((heads, length, HEAD), BF),
                pltpu.VMEM((heads, length, 2 * HEAD), BF),
                pltpu.VMEM((heads, length, 2 * HEAD), F32),
                pltpu.VMEM((heads, SLOTS, TILE, TILE), F32),
                pltpu.VMEM((heads, SLOTS, TILE, TILE), BF),
            ]),
        out_shape=[jax.ShapeDtypeStruct((width, length), BF), jax.ShapeDtypeStruct((3, width, length), BF)],
        compiler_params=pltpu.CompilerParams(vmem_limit_bytes=60 << 20),
        name="attention",
        cost_estimate=pl.CostEstimate(flops=10 * width * length * 768, transcendentals=width * length * 12,
                                      bytes_accessed=26 * width * length),
    )(lo, lin, g, cos, sin, segment[None, :], segk)


def rotary_tables(segment):
    length = segment.shape[0]
    starts = jnp.sum(segment[None, :] < jnp.arange(N_DOCS, dtype=jnp.int32)[:, None], axis=1)
    begin = jnp.sum(jnp.where(segment[None, :] == jnp.arange(N_DOCS)[:, None], starts[:, None], 0), axis=0)
    position = (jnp.arange(length, dtype=jnp.int32) - begin).astype(F32)
    exponent = jnp.arange(HALF, dtype=F32) / HALF
    frequency = jnp.exp(-math.log(10000.0) * exponent)
    angles = frequency[:, None] * position[None, :]
    return jnp.cos(angles), jnp.sin(angles)


def normalized(values):
    average = jnp.mean(values, axis=-1, keepdims=True)
    centered = values - average
    variance = jnp.mean(centered * centered, axis=-1, keepdims=True)
    inverse = lax.rsqrt(variance + EPSILON)
    return centered * inverse, inverse


def by_features(x, gy, segment, keep, gain, bias, w_qkv, w_out, w_up, w_down,
              a_in, b_qkv, b_up, a_out, a_down, b_out):
    width = w_qkv.shape[2]
    micro = x.shape[0]
    a_full = lax.all_gather(a_in, "tensor", axis=2, tiled=True)
    b_full = lax.all_gather(b_out, "tensor", axis=1, tiled=True)

    m_qkv = jnp.concatenate([
        (w_qkv[i].astype(F32) + SCALE * dot(a_full[i], b_qkv[i], 1, 0)).astype(BF) for i in range(3)
    ], axis=1)
    m_up = (w_up.astype(F32) + SCALE * dot(a_full[3], b_up, 1, 0)).astype(BF)
    m_out = (w_out.astype(F32) + SCALE * dot(a_out, b_full[0], 1, 0)).astype(BF)
    m_down = (w_down.astype(F32) + SCALE * dot(a_down, b_full[1], 1, 0)).astype(BF)
    a_three = jnp.concatenate([a_full[0], a_full[1], a_full[2]], axis=1)
    b_both = jnp.concatenate([b_full[0], b_full[1]], axis=0)

    outs, grads, sums = [], [], None
    for m in range(micro):
        rows, seg = x[m, 0], segment[m, 0]
        xg = lax.all_gather(rows, "tensor", axis=0, tiled=True)
        gg = lax.all_gather(gy[m, 0], "tensor", axis=0, tiled=True)
        standard, _ = normalized(xg.astype(F32))
        n1 = (standard * gain[0] + bias[0]).astype(BF)
        n2 = (standard * gain[1] + bias[1]).astype(BF)
        lin = dot(m_qkv, n1, 0, 1)
        low3 = dot(n1, a_three, 1, 0).astype(BF)
        low1 = dot(n2, a_full[3], 1, 0).astype(BF)
        g_ctx = dot(m_out, gg, 1, 1).astype(BF)
        low_grad = (SCALE * dot(gg, b_both, 1, 1)).astype(BF)
        cos, sin = rotary_tables(seg)
        ctx, d_lin = attention(lin.reshape(3, width, -1), g_ctx, cos, sin, seg, keep[m, 0])
        d_lin = d_lin.reshape(3 * width, -1)

        pre = dot(n2, m_up, 1, 0)
        cdf = 0.5 * (1.0 + lax.erf(pre * math.sqrt(0.5)))
        hidden = (pre * cdf).astype(BF)
        slope = cdf + pre * (math.sqrt(0.5 / math.pi) * jnp.exp(-0.5 * pre * pre))
        d_pre = (dot(gg, m_down, 1, 1) * slope).astype(BF)

        part = dot(ctx, m_out, 0, 0) + dot(hidden, m_down, 1, 0)
        branch = lax.psum_scatter(part.astype(BF), "tensor", scatter_dimension=0, tiled=True)
        outs.append((rows.astype(F32) + branch.astype(F32)).astype(BF))

        one = dot(d_lin, m_qkv, 0, 1)
        two = dot(d_pre, m_up, 1, 1)
        total = (gain[0] * one + gain[1] * two).astype(BF)
        total = lax.psum_scatter(total, "tensor", scatter_dimension=0, tiled=True).astype(F32)
        own, inverse = normalized(rows.astype(F32))
        grad = total - jnp.mean(total, axis=-1, keepdims=True)
        grad = grad - own * jnp.mean(total * own, axis=-1, keepdims=True)
        grads.append((gy[m, 0].astype(F32) + grad * inverse).astype(BF))

        norms = jnp.stack([jnp.sum(one * standard, axis=0), jnp.sum(two * standard, axis=0),
                           jnp.sum(one, axis=0), jnp.sum(two, axis=0)])
        lo_ctx = dot(ctx, a_out, 0, 0).astype(BF)
        lo_hid = dot(hidden, a_down, 1, 0).astype(BF)
        d_b_out = SCALE * jnp.stack([dot(lo_ctx, gg, 0, 0), dot(lo_hid, gg, 0, 0)], axis=1)
        d_a_out = dot(ctx, low_grad[:, :128], 1, 0)
        d_a_down = dot(hidden, low_grad[:, 128:], 0, 0)
        d_b_qkv = SCALE * jnp.stack([
            dot(low3[:, 128 * i:128 * (i + 1)], d_lin[width * i:width * (i + 1)], 0, 1) for i in range(3)])
        d_b_up = SCALE * dot(low1, d_pre, 0, 0)
        back = [(SCALE * dot(d_lin[width * i:width * (i + 1)], b_qkv[i], 0, 1)).astype(BF) for i in range(3)]
        back.append((SCALE * dot(d_pre, b_up, 1, 1)).astype(BF))
        d_a_in = jnp.stack([dot(back[i], n1 if i < 3 else n2, 0, 0) for i in range(4)], axis=1)
        terms = (d_a_in, d_b_qkv, d_b_up, d_a_out, d_a_down, d_b_out, norms)
        sums = terms if sums is None else tuple(p + q for p, q in zip(sums, terms))

    d_a_in, d_b_qkv, d_b_up, d_a_out, d_a_down, d_b_out, norms = sums
    d_a_in = lax.psum_scatter(d_a_in, "tensor", scatter_dimension=0, tiled=True)
    d_b_out = lax.psum_scatter(d_b_out, "tensor", scatter_dimension=0, tiled=True)
    d_a_in, d_b_qkv, d_b_up, d_a_out, d_a_down, d_b_out = lax.psum(
        (d_a_in, d_b_qkv, d_b_up, d_a_out, d_a_down, d_b_out), "dp")
    norms = lax.psum(norms, ("dp", "tensor"))
    return (jnp.stack(outs)[:, None], jnp.stack(grads)[:, None], norms[:2], norms[2:],
            jnp.transpose(d_a_in, (1, 2, 0)), d_b_qkv, d_b_up, d_a_out, d_a_down,
            jnp.transpose(d_b_out, (1, 0, 2)))


RANK = 128


MESH = pl.DeviceIdType.MESH


def place():
    d = lax.axis_index("dp")
    return d // 2, d % 2, lax.axis_index("tensor")


def meet(z, c, t):
    barrier = pltpu.get_barrier_semaphore()
    for h in (0, 1):
        for k in range(4):
            if h or k:
                pl.semaphore_signal(barrier, 1, device_id=(2 * z + (c ^ h), t ^ k), device_id_type=MESH)
    pl.semaphore_wait(barrier, 7)


def remote(src, dst, send_sem, recv_sem, device):
    return pltpu.make_async_remote_copy(src_ref=src, dst_ref=dst, send_sem=send_sem, recv_sem=recv_sem,
                                        device_id=device, device_id_type=MESH)


class Rows:
    def __init__(self, v, full, sems, stage, local, z, c, t):
        self.v, self.full, self.sems, self.stage, self.local = v, full, sems, stage, local
        self.z, self.c, self.t = z, c, t

    def rows(self, s, h):
        return self.full.at[pl.ds(pl.multiple_of(s * 512 + h * 256, 256), 256)]

    def block(self, m, h):
        return self.v.at[m, pl.ds(pl.multiple_of(h * 256, 256), 256)]

    def copy(self, m, other):
        h = self.c ^ other
        return remote(self.block(m, h), self.rows(self.t, h), self.sems.at[2 * m + other], self.sems.at[4 + self.t],
                      (2 * self.z + h, 2 * m + self.c))

    def forward(self, s):
        part = self.rows(s, self.c)
        return remote(part, part, self.sems.at[8 + s], self.sems.at[12 + s], (2 * self.z + (self.c ^ 1), self.t))

    def start(self):
        for m in (0, 1):
            away = 2 * m + self.c != self.t

            @pl.when(away)
            def _():
                self.copy(m, 0).start()

            self.copy(m, 1).start()

            @pl.when(jnp.logical_not(away))
            def _():
                pltpu.make_async_copy(self.block(m, self.c), self.stage, self.local.at[0]).start()

    def relay(self):
        mine = self.t % 2 == self.c

        @pl.when(mine)
        def _():
            pltpu.make_async_copy(self.block(0, self.c), self.stage, self.local.at[0]).wait()
            pltpu.make_async_copy(self.stage, self.rows(self.t, self.c), self.sems.at[4 + self.t]).start()

        for k in (0, 1, 2, 3):
            s = self.t ^ k
            pltpu.make_async_copy(self.stage, self.rows(s, self.c), self.sems.at[4 + s]).wait()
            self.forward(s).start()

    def finish(self):
        for s in range(4):
            part = self.rows(s, self.c ^ 1)
            remote(part, part, self.sems.at[8 + s], self.sems.at[12 + s], (2 * self.z + (self.c ^ 1), self.t)).wait_recv()
            self.forward(s).wait_send()
        for m in (0, 1):
            @pl.when(2 * m + self.c != self.t)
            def _():
                self.copy(m, 0).wait_send()

            self.copy(m, 1).wait_send()


class Blocks:
    def __init__(self, own, where, sems, stage, local, halves, z, c, t):
        self.own, self.where, self.sems, self.stage, self.local = own, where, sems, stage, local
        self.halves, self.t, self.d = halves, t, 2 * z + c

    def first(self, k):
        return remote(self.own, self.where(self.t), self.sems.at[k - 1], self.sems.at[3 + k - 1], (self.d, self.t ^ k))

    def arrival(self, k):
        spot = self.where(self.t ^ k)
        return remote(spot, spot, self.sems.at[k - 1], self.sems.at[3 + k - 1], (self.d, self.t ^ k))

    def second(self, k):
        part = self.halves(self.where(self.t ^ (3 - k)), k - 1)
        return remote(part, part, self.sems.at[6 + k - 1], self.sems.at[8 + k - 1], (self.d, self.t ^ k))

    def start(self):
        for k in ((1, 2) if self.halves else (1, 2, 3)):
            self.first(k).start()
        pltpu.make_async_copy(self.own, self.stage, self.local.at[0]).start()

    def store(self):
        pltpu.make_async_copy(self.own, self.stage, self.local.at[0]).wait()
        pltpu.make_async_copy(self.stage, self.where(self.t), self.local.at[1]).start()

    def relay(self):
        if self.halves:
            for k in (1, 2):
                self.arrival(3 - k).wait_recv()
                self.second(k).start()

    def finish(self):
        pltpu.make_async_copy(self.stage, self.where(self.t), self.local.at[1]).wait()
        if self.halves:
            for k in (1, 2):
                part = self.halves(self.where(self.t ^ 3), k - 1)
                remote(part, part, self.sems.at[6 + k - 1], self.sems.at[8 + k - 1], (self.d, self.t ^ k)).wait_recv()
                self.first(k).wait_send()
                self.second(k).wait_send()
        else:
            for k in (1, 2, 3):
                self.arrival(k).wait_recv()
                self.first(k).wait_send()


def aligned(i, n):
    return pl.ds(pl.multiple_of(i * n, n), n)


def front_kernel(x, g, wq, wo, ain, bq, ao, bo,
                 xf, gf, wqf, wof, ainf, bqf, aof, bof,
                 row_sems, sems, local, xs, gs, wqs, wos, ains, bqs, aos, bos):
    z, c, t = place()
    meet(z, c, t)
    at = dict(z=z, c=c, t=t)
    x_rows = Rows(x, xf, row_sems.at[0], xs, local.at[0], **at)
    g_rows = Rows(g, gf, row_sems.at[1], gs, local.at[1], **at)
    qkv = Blocks(wq.at[:, :, aligned(c, 128)], lambda i: wqf.at[:, :, aligned(i, 128)], sems.at[0], wqs, local.at[2],
                 lambda v, h: v.at[:, pl.ds(h * 512, 512)], **at)
    into = Blocks(ain, lambda i: ainf.at[:, aligned(i, 32)], sems.at[1], ains, local.at[3], None, **at)
    second = Blocks(bq.at[:, :, aligned(c, 128)], lambda i: bqf.at[:, :, aligned(i, 128)], sems.at[2], bqs, local.at[4],
                    None, **at)
    out = Blocks(wo.at[aligned(c, 128)], lambda i: wof.at[aligned(i, 128)], sems.at[3], wos, local.at[5],
                 lambda v, h: v.at[pl.ds(h * 64, 64)], **at)
    a_out = Blocks(ao.at[aligned(c, 128)], lambda i: aof.at[aligned(i, 128)], sems.at[4], aos, local.at[6], None, **at)
    b_out = Blocks(bo, lambda i: bof.at[:, aligned(i, 32)], sems.at[5], bos, local.at[7], None, **at)
    x_rows.start()
    into.start()
    second.start()
    qkv.start()
    x_rows.relay()
    for v in (into, second, qkv):
        v.store()
    g_rows.start()
    qkv.relay()
    for v in (b_out, a_out, out):
        v.start()
    g_rows.relay()
    for v in (b_out, a_out, out):
        v.store()
    out.relay()
    for v in (x_rows, into, second, qkv, g_rows, b_out, a_out, out):
        v.finish()


def front(x, g, wq, wo, ain, bq, ao, bo):
    shapes = [(2048, 1024), (2048, 1024), (3, 1024, 512), (512, 1024), (4, 128, 1024), (3, 128, 512), (512, 128),
              (2, 128, 1024)]
    anywhere = pl.BlockSpec(memory_space=pl.ANY)
    return pl.pallas_call(
        front_kernel,
        in_specs=[anywhere] * 8,
        out_specs=[anywhere] * 8,
        out_shape=[jax.ShapeDtypeStruct(s, BF) for s in shapes],
        scratch_shapes=[
            pltpu.SemaphoreType.DMA((2, 16)),
            pltpu.SemaphoreType.DMA((6, 10)),
            pltpu.SemaphoreType.DMA((8, 2)),
            pltpu.VMEM((256, 1024), BF),
            pltpu.VMEM((256, 1024), BF),
            pltpu.VMEM((3, 1024, 128), BF),
            pltpu.VMEM((128, 1024), BF),
            pltpu.VMEM((4, 32, 1024), BF),
            pltpu.VMEM((3, 128, 128), BF),
            pltpu.VMEM((128, 128), BF),
            pltpu.VMEM((2, 32, 1024), BF),
        ],
        compiler_params=pltpu.CompilerParams(collective_id=0, has_side_effects=True),
        name="front",
    )(x, g, wq, wo, ain, bq, ao, bo)


def back_kernel(rows, dbq, dbu, dao, dad, dsh, dno,
                out, obq, obu, oao, oad, osh, ono,
                row_sems, share_sems, cross_sems, z_sems, last_sems, norm_sems,
                sh_in, sh, rbq, rbu, rao, rad, rsh, pbq, pbu, pao, pad, psh, qbq, qbu, qao, qad, qsh, no_in, no_sum):
    z, c, t = place()
    meet_all(z, c, t)
    d = 2 * z + c
    sibling = (2 * z + (c ^ 1), t)

    home = t % 2
    local = home == c
    spot = aligned(c, 256)

    def row(k):
        return remote(rows.at[t ^ k], out.at[t // 2, spot], row_sems.at[k], row_sems.at[4 + (t // 2) * 2 + c],
                      (2 * z + home, t ^ k))

    def own_row():
        return pltpu.make_async_copy(rows.at[t], out.at[t // 2, spot], row_sems.at[4 + (t // 2) * 2 + c])

    @pl.when(local)
    def _():
        own_row().start()

    @pl.when(jnp.logical_not(local))
    def _():
        row(0).start()

    for k in (1, 2, 3):
        row(k).start()

    peers = (sibling, (d, t ^ 1), (d, t ^ 2), (d ^ 2, t), (d ^ 4, t))

    def norm(i):
        return remote(dno if i == 0 else no_sum.at[i - 1], no_in.at[i], norm_sems.at[0, i], norm_sems.at[1, i], peers[i])

    def norm_next(i):
        norm(i).wait_recv()
        total = (dno[...] if i == 0 else no_sum[i - 1]) + no_in[i]
        if i < 4:
            no_sum[i] = total
            norm(i + 1).start()
        else:
            ono[...] = total

    norm(0).start()

    def share():
        return remote(dsh.at[:, :, aligned(c ^ 1, 512)], sh_in, share_sems.at[0], share_sems.at[1], sibling)

    share().start()
    share().wait_recv()
    norm_next(0)
    for i in range(6):
        sh[i] = (dsh[i, :, aligned(c, 512)].astype(F32) + sh_in[i].astype(F32)).astype(BF)

    def parts(j):
        return (dbq.at[:, :, aligned(j, 128)], dbu.at[:, aligned(j, 512)], dao.at[aligned(j, 128)],
                dad.at[:, aligned(j, 512)], sh.at[:, aligned(j, 32)])

    got = (rbq, rbu, rao, rad, rsh)

    def cross(k, i):
        return remote(parts(t ^ k)[i], got[i].at[k - 1], cross_sems.at[0, k - 1, i], cross_sems.at[1, k - 1, i], (d, t ^ k))

    for k in (1, 2, 3):
        for i in range(5):
            cross(k, i).start()
    norm_next(1)
    norm_next(2)

    sums = (pbq, pbu, pao, pad, psh)
    halves = (qbq, qbu, qao, qad, qsh)
    low = z % 2

    def half(v, i, j):
        if i == 0:
            return v.at[:, aligned(j, 64)]
        if i == 4:
            return v.at[:, aligned(j, 16)]
        return v.at[aligned(j, 64)]

    def along(step, i):
        j = low ^ 1 if step == 0 else low
        dst = sums[i].at[2] if step == 2 else halves[i].at[step]
        return remote(half(sums[i].at[step], i, j), half(dst, i, j), z_sems.at[0, step, i], z_sems.at[1, step, i],
                      (d ^ (4 if step == 1 else 2), t))

    def arrived(step, i):
        j = low ^ 1 if step == 2 else low
        dst = sums[i].at[2] if step == 2 else halves[i].at[step]
        return remote(half(dst, i, j), half(dst, i, j), z_sems.at[0, step, i], z_sems.at[1, step, i], (d, t ^ 1))

    for i in range(5):
        for k in (1, 2, 3):
            cross(k, i).wait_recv()
        total = parts(t)[i][...].astype(F32)
        for k in (0, 1, 2):
            total = total + got[i][k].astype(F32)
        sums[i][0] = total.astype(BF)
        along(0, i).start()
    norm_next(3)
    for step in (0, 1):
        for i in range(5):
            arrived(step, i).wait_recv()
            mine, other = half(sums[i].at[step], i, low), half(halves[i].at[step], i, low)
            half(sums[i].at[step + 1], i, low)[...] = (mine[...].astype(F32) + other[...].astype(F32)).astype(BF)
            along(step + 1, i).start()
        if step == 0:
            norm_next(4)
    result = (obq.at[:, :, aligned(c, 128)], obu.at[:, aligned(c, 512)], oao.at[aligned(c, 128)],
              oad.at[:, aligned(c, 512)], osh.at[:, :, aligned(c, 512)])
    theirs = (obq.at[:, :, aligned(c ^ 1, 128)], obu.at[:, aligned(c ^ 1, 512)], oao.at[aligned(c ^ 1, 128)],
              oad.at[:, aligned(c ^ 1, 512)], osh.at[:, :, aligned(c ^ 1, 512)])

    def last(i):
        return remote(result[i], result[i], last_sems.at[0, i], last_sems.at[1, i], sibling)

    for i in range(5):
        arrived(2, i).wait_recv()
        result[i][...] = sums[i][2].astype(F32)
        last(i).start()

    for i in range(5):
        remote(theirs[i], theirs[i], last_sems.at[0, i], last_sems.at[1, i], sibling).wait_recv()
        last(i).wait_send()
        for step in (0, 1, 2):
            along(step, i).wait_send()
        for k in (1, 2, 3):
            cross(k, i).wait_send()
    share().wait_send()
    for i in range(5):
        norm(i).wait_send()
    for k in (1, 2, 3):
        row(k).wait_send()

    @pl.when(jnp.logical_not(local))
    def _():
        row(0).wait_send()

    for m in (0, 1):
        for h in (0, 1):
            pltpu.make_async_copy(rows.at[0], out.at[m, pl.ds(256 * h, 256)], row_sems.at[4 + 2 * m + h]).wait()


def meet_all(z, c, t):
    barrier = pltpu.get_barrier_semaphore()
    for h in (0, 1):
        for k in range(4):
            if h or k:
                pl.semaphore_signal(barrier, 1, device_id=(2 * z + (c ^ h), t ^ k), device_id_type=MESH)
    for k in (1, 2):
        pl.semaphore_signal(barrier, 1, device_id=(2 * (z ^ k) + c, t), device_id_type=MESH)
    pl.semaphore_wait(barrier, 9)


def back(rows, dbq, dbu, dao, dad, dsh, dno):
    vmem = pl.BlockSpec(memory_space=pltpu.VMEM)
    part = [(3, 128, 128), (128, 512), (128, 128), (128, 512), (6, 32, 512)]
    outs = [((2, 512, 1024), BF), ((3, 128, 256), F32), ((128, 1024), F32), ((256, 128), F32), ((128, 1024), F32),
            ((6, 32, 1024), F32), ((4, 1024), F32)]
    return pl.pallas_call(
        back_kernel,
        in_specs=[vmem] * 7,
        out_specs=[pl.BlockSpec(memory_space=pl.ANY)] + [vmem] * 6,
        out_shape=[jax.ShapeDtypeStruct(s, d) for s, d in outs],
        scratch_shapes=[
            pltpu.SemaphoreType.DMA((8,)),
            pltpu.SemaphoreType.DMA((2,)),
            pltpu.SemaphoreType.DMA((2, 3, 5)),
            pltpu.SemaphoreType.DMA((2, 3, 5)),
            pltpu.SemaphoreType.DMA((2, 5)),
            pltpu.SemaphoreType.DMA((2, 5)),
            pltpu.VMEM((6, 128, 512), BF),
            pltpu.VMEM((6, 128, 512), BF),
        ] + [pltpu.VMEM((3,) + s, BF) for s in part + part] + [pltpu.VMEM((2,) + s, BF) for s in part] + [
            pltpu.VMEM((5, 4, 1024), F32),
            pltpu.VMEM((4, 4, 1024), F32),
        ],
        compiler_params=pltpu.CompilerParams(collective_id=1, has_side_effects=True),
        name="back",
    )(rows, dbq, dbu, dao, dad, dsh, dno)


def swap(v, k=1):
    return lax.ppermute(v, "dp", [(i, i ^ k) for i in range(lax.axis_size("dp"))])


def pick(v, axis, index, size):
    return lax.dynamic_slice_in_dim(v, index * size, size, axis)


def half_rows(v, c):
    return pick(v.reshape(4, 2, 256, -1), 1, c, 1)[:, 0]


def from_group(own, c):
    got = lax.all_to_all(own, "tensor", 0, 0, tiled=True).reshape(2, 2, 256, -1)
    mine = pick(got, 1, c, 1)[:, 0]
    other = swap(pick(got, 1, 1 - c, 1)[:, 0])
    return jnp.where(c == 0, jnp.stack([mine, other], 1), jnp.stack([other, mine], 1)).reshape(2, 512, -1)


def by_groups(x, gy, segment, keep, gain, bias, w_qkv, w_out, w_up, w_down,
              a_in, b_qkv, b_up, a_out, a_down, b_out):
    z, c, t = place()
    tables = jnp.stack([segment[:, 0], keep[:, 0]], 1)
    pair = jnp.where(t % 2 == c, tables, swap(tables))
    seg, kept = jnp.where(t // 2 == 0, pair[0], pair[1])

    x_full, g_full, qkv, out, a_full, b_qkv_all, a_out_all, b_full = front(
        x[:, 0], gy[:, 0], w_qkv, w_out, jnp.swapaxes(a_in, 1, 2), b_qkv, a_out, b_out)
    up, down = lax.optimization_barrier((
        jnp.concatenate([pick(w_up, 1, c, 512), pick(b_up, 1, c, 512)], axis=0),
        jnp.concatenate([pick(w_down, 0, c, 512), pick(a_down, 0, c, 512)], axis=1), x_full))[:2]
    up = lax.all_gather(up, "tensor", axis=0)
    down = lax.all_gather(down, "tensor", axis=0, tiled=True)
    w_up_all = jnp.concatenate([up[i, :1024] for i in range(4)], axis=1)
    b_up_all = jnp.concatenate([up[i, 1024:] for i in range(4)], axis=1)
    w_down_all, a_down_all = down[:, :1024], down[:, 1024:]

    m_qkv = (qkv.astype(F32) + SCALE * jnp.einsum("nrk,nrc->nkc", a_full[:3], b_qkv_all,
                                                  preferred_element_type=F32)).astype(BF)
    m_up = (w_up_all.astype(F32) + SCALE * dot(a_full[3], b_up_all, 0, 0)).astype(BF)
    m_out = (out.astype(F32) + SCALE * dot(a_out_all, b_full[0], 1, 0)).astype(BF)
    m_down = (w_down_all.astype(F32) + SCALE * dot(a_down_all, b_full[1], 1, 0)).astype(BF)
    a_three = a_full[:3].reshape(3 * RANK, 1024)
    b_both = b_full.reshape(2 * RANK, 1024)

    standard, inverse = normalized(x_full.astype(F32))
    n1 = (standard * gain[0] + bias[0]).astype(BF)
    n2 = (standard * gain[1] + bias[1]).astype(BF)
    lin = jnp.einsum("nkc,sk->ncs", m_qkv, n1, preferred_element_type=F32)
    low3 = dot(a_three, n1, 1, 1).astype(BF).reshape(3, RANK, 2048)
    low1 = dot(a_full[3], n2, 1, 1).astype(BF)
    g_ctx = dot(m_out, g_full, 1, 1).astype(BF)
    low_grad = (SCALE * dot(b_both, g_full, 1, 1)).astype(BF)
    cos, sin = rotary_tables(seg)
    ctx, d_lin = attention(lin, g_ctx, cos, sin, seg, kept)

    pre = dot(n2, m_up, 1, 0)
    cdf = 0.5 * (1.0 + lax.erf(pre * math.sqrt(0.5)))
    hidden = (pre * cdf).astype(BF)
    slope = cdf + pre * (math.sqrt(0.5 / math.pi) * jnp.exp(-0.5 * pre * pre))
    d_pre = (dot(g_full, m_down, 1, 1) * slope).astype(BF)

    part = dot(ctx, m_out, 0, 0) + dot(hidden, m_down, 1, 0)
    theirs = swap(half_rows(part, 1 - c).astype(BF))
    y = half_rows(x_full, c).astype(F32) + half_rows(part, c) + theirs.astype(F32)
    y = from_group(y.astype(BF), c)

    one = jnp.einsum("ncs,nkc->sk", d_lin, m_qkv, preferred_element_type=F32)
    two = dot(d_pre, m_up, 1, 1)
    total = gain[0] * one + gain[1] * two
    theirs = swap(half_rows(total, 1 - c).astype(BF))
    total = half_rows(total, c) + theirs.astype(F32)
    own = half_rows(standard, c)
    grad = total - jnp.mean(total, axis=-1, keepdims=True)
    grad = grad - own * jnp.mean(total * own, axis=-1, keepdims=True)
    grad = half_rows(g_full, c).astype(F32) + grad * half_rows(inverse, c)

    norms = jnp.stack([jnp.sum(one * standard, axis=0), jnp.sum(two * standard, axis=0),
                       jnp.sum(one, axis=0), jnp.sum(two, axis=0)])
    lo = jnp.concatenate([dot(a_out_all, ctx, 0, 0), dot(a_down_all, hidden, 0, 1)], axis=0).astype(BF)
    d_a_out = dot(ctx, low_grad[:RANK], 1, 1).astype(BF)
    d_a_down = dot(low_grad[RANK:], hidden, 1, 0).astype(BF)
    d_b_qkv = (SCALE * jnp.einsum("nrs,ncs->nrc", low3, d_lin, preferred_element_type=F32)).astype(BF)
    d_b_up = (SCALE * dot(low1, d_pre, 1, 0)).astype(BF)
    back3 = (SCALE * jnp.einsum("nrc,ncs->nrs", b_qkv_all, d_lin, preferred_element_type=F32)).astype(BF)
    back1 = (SCALE * dot(b_up_all, d_pre, 1, 1)).astype(BF)
    shared = jnp.concatenate([dot(back3.reshape(3 * RANK, 2048), n1, 1, 0).astype(BF), dot(back1, n2, 1, 0).astype(BF),
                              (SCALE * dot(lo, g_full, 1, 0)).astype(BF)], axis=0).reshape(6, RANK, 1024)
    grad, r_b_qkv, r_b_up, r_a_out, r_a_down, rest, norms = back(
        grad.astype(BF), d_b_qkv, d_b_up, d_a_out, d_a_down, shared, norms)
    r_a_in = jnp.swapaxes(rest[:4], 1, 2)
    return (y[:, None], grad[:, None], norms[:2], norms[2:], r_a_in, r_b_qkv, r_b_up, r_a_out, jnp.transpose(r_a_down), rest[4:])


def solution(mesh):
    in_specs = (
        P(None, "dp", "tensor", None),
        P(None, "dp", "tensor", None),
        P(None, "dp", None),
        P(None, "dp", None),
        P(),
        P(),
        P(None, None, "tensor"),
        P("tensor", None),
        P(None, "tensor"),
        P("tensor", None),
        P(None, None, "tensor"),
        P(None, None, "tensor"),
        P(None, "tensor"),
        P("tensor", None),
        P("tensor", None),
        P(None, "tensor", None),
    )
    out_specs = (
        P(None, "dp", "tensor", None),
        P(None, "dp", "tensor", None),
        P(),
        P(),
        P(None, None, "tensor"),
        P(None, None, "tensor"),
        P(None, "tensor"),
        P("tensor", None),
        P("tensor", None),
        P(None, "tensor", None),
    )
    small = mesh.shape["tensor"] == 4 and mesh.shape["dp"] == 8
    return jax.shard_map(
        by_groups if small else by_features, mesh=mesh, in_specs=in_specs, out_specs=out_specs, check_vma=False
    )
```

```python
import functools
import math

import jax
import jax.numpy as jnp
from jax import lax
from jax.experimental import pallas as pl
from jax.experimental.pallas import tpu as pltpu
from jax.sharding import PartitionSpec as P

HEAD = 64
HALF = 8
N_DOCS = 5
TILE = 256
SLOTS = 5
EPSILON = 1e-05
SCALE = 0.25
F32 = jnp.float32
BF = jnp.bfloat16


def dot(a, b, ca, cb):
    return lax.dot_general(a, b, (((ca,), (cb,)), ((), ())), preferred_element_type=F32)


def attention_kernel(heads, lo_ref, lin_ref, g_ref, cos_ref, sin_ref, segq_ref, segk_ref,
                     ctx_ref, dlin_ref, qt, kt, vt, kn, vn, acc, s_scr, e_scr, p_scr, row):
    length = lin_ref.shape[2]
    blocks = length // TILE

    def rotate(z, cos, sin):
        a, b = z[:HALF], z[HALF:2 * HALF]
        return jnp.concatenate([a * cos - b * sin, b * cos + a * sin, z[2 * HALF:]], axis=0)

    def prepare(c, carry):
        cols = pl.ds(pl.multiple_of(c * TILE, TILE), TILE)
        cos, sin = cos_ref[:, cols], sin_ref[:, cols]
        for h in range(heads):
            rows = pl.ds(h * HEAD, HEAD)
            q = rotate(lin_ref[0, pl.ds(h * HEAD, HEAD), cols], cos, sin).astype(BF).astype(F32) * 0.125
            k = rotate(lin_ref[1, pl.ds(h * HEAD, HEAD), cols], cos, sin)
            v = lin_ref[2, pl.ds(h * HEAD, HEAD), cols]
            qt[rows, cols] = q.astype(BF)
            kt[rows, cols] = k.astype(BF)
            vt[rows, cols] = v.astype(BF)
            kn[h, cols, :] = jnp.transpose(k).astype(BF)
            vn[h, cols, :] = jnp.transpose(v).astype(BF)
            acc[h, :, cols] = jnp.zeros((2 * HEAD, TILE), F32)
        return carry

    lax.fori_loop(0, blocks, prepare, 0)

    def query_block(qb, carry):
        lo = lo_ref[qb]
        qcols = pl.ds(pl.multiple_of(qb * TILE, TILE), TILE)
        segq = segq_ref[:, qcols]

        def scores(kb, tops, last=False):
            krows = pl.ds(pl.multiple_of(kb * TILE, TILE), TILE)
            allowed = segk_ref[krows, :] == segq
            if last:
                k, q = (lax.broadcasted_iota(jnp.int32, (TILE, TILE), i) for i in (0, 1))
                allowed = (allowed & (k < q)) | (k == q)
            out = []
            for h in range(heads):
                rows = pl.ds(h * HEAD, HEAD)
                s = dot(kn[h, krows, :], qt[rows, qcols], 1, 0)
                s = jnp.where(allowed, s, -1e30)
                s_scr[h, kb - lo] = s
                p_scr[h, kb - lo] = dot(vn[h, krows, :], g_ref[rows, qcols], 1, 0)
                out.append(jnp.maximum(tops[h], jnp.max(s, axis=0, keepdims=True)))
            return tuple(out)

        tops = lax.fori_loop(lo, qb, scores, tuple(jnp.full((1, TILE), -1e30, F32) for _ in range(heads)))
        tops = scores(qb, tops, True)

        def weights(kb, sums):
            kcols = pl.ds(pl.multiple_of(kb * TILE, TILE), TILE)
            out = []
            for h in range(heads):
                e = jnp.exp(s_scr[h, kb - lo] - tops[h])
                low = e.astype(BF)
                e_scr[h, kb - lo] = low
                out.append(sums[h] + jnp.sum(e, axis=0, keepdims=True))
                row[h] += dot(vt[pl.ds(h * HEAD, HEAD), kcols], low, 1, 0)
            return tuple(out)

        row[...] = jnp.zeros_like(row)
        sums = lax.fori_loop(lo, qb + 1, weights, tuple(jnp.zeros((1, TILE), F32) for _ in range(heads)))
        gts, terms, scales = [], [], []
        for h in range(heads):
            rows = pl.ds(h * HEAD, HEAD)
            inverse = 1.0 / sums[h]
            ctx = row[h] * inverse
            ctx_ref[rows, qcols] = ctx.astype(BF)
            g = g_ref[rows, qcols].astype(F32)
            terms.append(jnp.sum(g * ctx, axis=0, keepdims=True))
            scales.append(inverse)
            gts.append((g * inverse).astype(BF))

        row[...] = jnp.zeros_like(row)

        def backward(kb, carry):
            krows = pl.ds(pl.multiple_of(kb * TILE, TILE), TILE)
            for h in range(heads):
                low = e_scr[h, kb - lo]
                ds = (low.astype(F32) * ((p_scr[h, kb - lo] - terms[h]) * scales[h])).astype(BF)
                acc[h, :HEAD, krows] += dot(gts[h], low, 1, 1)
                acc[h, HEAD:, krows] += dot(qt[pl.ds(h * HEAD, HEAD), qcols], ds, 1, 1)
                row[h] += dot(kt[pl.ds(h * HEAD, HEAD), krows], ds, 1, 0)
            return carry

        lax.fori_loop(lo, qb + 1, backward, 0)
        cos, sin = cos_ref[:, qcols], sin_ref[:, qcols]
        for h in range(heads):
            dlin_ref[0, pl.ds(h * HEAD, HEAD), qcols] = rotate(row[h] * 0.125, cos, -sin).astype(BF)
        return carry

    lax.fori_loop(0, blocks, query_block, 0)

    def finish(c, carry):
        cols = pl.ds(pl.multiple_of(c * TILE, TILE), TILE)
        cos, sin = cos_ref[:, cols], sin_ref[:, cols]
        for h in range(heads):
            both = acc[h, :, cols]
            dlin_ref[1, pl.ds(h * HEAD, HEAD), cols] = rotate(both[HEAD:], cos, -sin).astype(BF)
            dlin_ref[2, pl.ds(h * HEAD, HEAD), cols] = both[:HEAD].astype(BF)
        return carry

    lax.fori_loop(0, blocks, finish, 0)


def attention(lin, g, cos, sin, segment, keep):
    width, length = g.shape
    heads = min(4, width // HEAD)
    wide = heads * HEAD
    starts = jnp.sum(segment[None, :] < jnp.arange(N_DOCS, dtype=jnp.int32)[:, None], axis=1)
    firsts = segment[::TILE]
    lo = jnp.sum(jnp.where(firsts[:, None] == jnp.arange(N_DOCS)[None, :], starts[None, :], 0), axis=1)
    lo = (lo // TILE).astype(jnp.int32)
    segk = jnp.where(keep == 1, segment, -1)[:, None]
    vmem = pl.BlockSpec(memory_space=pltpu.VMEM)
    three = pl.BlockSpec((3, wide, length), lambda i, lo: (0, i, 0))
    single = pl.BlockSpec((wide, length), lambda i, lo: (i, 0))
    return pl.pallas_call(
        functools.partial(attention_kernel, heads),
        grid_spec=pltpu.PrefetchScalarGridSpec(
            num_scalar_prefetch=1,
            grid=(width // wide,),
            in_specs=[three, single] + [vmem] * 4,
            out_specs=[single, three],
            scratch_shapes=[
                pltpu.VMEM((wide, length), BF),
                pltpu.VMEM((wide, length), BF),
                pltpu.VMEM((wide, length), BF),
                pltpu.VMEM((heads, length, HEAD), BF),
                pltpu.VMEM((heads, length, HEAD), BF),
                pltpu.VMEM((heads, 2 * HEAD, length), F32),
                pltpu.VMEM((heads, SLOTS, TILE, TILE), F32),
                pltpu.VMEM((heads, SLOTS, TILE, TILE), BF),
                pltpu.VMEM((heads, SLOTS, TILE, TILE), F32),
                pltpu.VMEM((heads, HEAD, TILE), F32),
            ]),
        out_shape=[jax.ShapeDtypeStruct((width, length), BF), jax.ShapeDtypeStruct((3, width, length), BF)],
        compiler_params=pltpu.CompilerParams(vmem_limit_bytes=60 << 20),
        name="attention",
        cost_estimate=pl.CostEstimate(flops=10 * width * length * 768, transcendentals=width * length * 12,
                                      bytes_accessed=26 * width * length),
    )(lo, lin, g, cos, sin, segment[None, :], segk)


def rotary_tables(segment):
    length = segment.shape[0]
    starts = jnp.sum(segment[None, :] < jnp.arange(N_DOCS, dtype=jnp.int32)[:, None], axis=1)
    begin = jnp.sum(jnp.where(segment[None, :] == jnp.arange(N_DOCS)[:, None], starts[:, None], 0), axis=0)
    position = (jnp.arange(length, dtype=jnp.int32) - begin).astype(F32)
    exponent = jnp.arange(HALF, dtype=F32) / HALF
    frequency = jnp.exp(-math.log(10000.0) * exponent)
    angles = frequency[:, None] * position[None, :]
    return jnp.cos(angles), jnp.sin(angles)


def normalized(values):
    average = jnp.mean(values, axis=-1, keepdims=True)
    centered = values - average
    variance = jnp.mean(centered * centered, axis=-1, keepdims=True)
    inverse = lax.rsqrt(variance + EPSILON)
    return centered * inverse, inverse


def by_features(x, gy, segment, keep, gain, bias, w_qkv, w_out, w_up, w_down,
              a_in, b_qkv, b_up, a_out, a_down, b_out):
    width = w_qkv.shape[2]
    micro = x.shape[0]
    a_full = lax.all_gather(a_in, "tensor", axis=2, tiled=True)
    b_full = lax.all_gather(b_out, "tensor", axis=1, tiled=True)

    m_qkv = jnp.concatenate([
        (w_qkv[i].astype(F32) + SCALE * dot(a_full[i], b_qkv[i], 1, 0)).astype(BF) for i in range(3)
    ], axis=1)
    m_up = (w_up.astype(F32) + SCALE * dot(a_full[3], b_up, 1, 0)).astype(BF)
    m_out = (w_out.astype(F32) + SCALE * dot(a_out, b_full[0], 1, 0)).astype(BF)
    m_down = (w_down.astype(F32) + SCALE * dot(a_down, b_full[1], 1, 0)).astype(BF)
    a_three = jnp.concatenate([a_full[0], a_full[1], a_full[2]], axis=1)
    b_both = jnp.concatenate([b_full[0], b_full[1]], axis=0)

    outs, grads, sums = [], [], None
    for m in range(micro):
        rows, seg = x[m, 0], segment[m, 0]
        xg = lax.all_gather(rows, "tensor", axis=0, tiled=True)
        gg = lax.all_gather(gy[m, 0], "tensor", axis=0, tiled=True)
        standard, _ = normalized(xg.astype(F32))
        n1 = (standard * gain[0] + bias[0]).astype(BF)
        n2 = (standard * gain[1] + bias[1]).astype(BF)
        lin = dot(m_qkv, n1, 0, 1)
        low3 = dot(n1, a_three, 1, 0).astype(BF)
        low1 = dot(n2, a_full[3], 1, 0).astype(BF)
        g_ctx = dot(m_out, gg, 1, 1).astype(BF)
        low_grad = (SCALE * dot(gg, b_both, 1, 1)).astype(BF)
        cos, sin = rotary_tables(seg)
        ctx, d_lin = attention(lin.reshape(3, width, -1), g_ctx, cos, sin, seg, keep[m, 0])
        d_lin = d_lin.reshape(3 * width, -1)

        pre = dot(n2, m_up, 1, 0)
        cdf = 0.5 * (1.0 + lax.erf(pre * math.sqrt(0.5)))
        hidden = (pre * cdf).astype(BF)
        slope = cdf + pre * (math.sqrt(0.5 / math.pi) * jnp.exp(-0.5 * pre * pre))
        d_pre = (dot(gg, m_down, 1, 1) * slope).astype(BF)

        part = dot(ctx, m_out, 0, 0) + dot(hidden, m_down, 1, 0)
        branch = lax.psum_scatter(part.astype(BF), "tensor", scatter_dimension=0, tiled=True)
        outs.append((rows.astype(F32) + branch.astype(F32)).astype(BF))

        one = dot(d_lin, m_qkv, 0, 1)
        two = dot(d_pre, m_up, 1, 1)
        total = (gain[0] * one + gain[1] * two).astype(BF)
        total = lax.psum_scatter(total, "tensor", scatter_dimension=0, tiled=True).astype(F32)
        own, inverse = normalized(rows.astype(F32))
        grad = total - jnp.mean(total, axis=-1, keepdims=True)
        grad = grad - own * jnp.mean(total * own, axis=-1, keepdims=True)
        grads.append((gy[m, 0].astype(F32) + grad * inverse).astype(BF))

        norms = jnp.stack([jnp.sum(one * standard, axis=0), jnp.sum(two * standard, axis=0),
                           jnp.sum(one, axis=0), jnp.sum(two, axis=0)])
        lo_ctx = dot(ctx, a_out, 0, 0).astype(BF)
        lo_hid = dot(hidden, a_down, 1, 0).astype(BF)
        d_b_out = SCALE * jnp.stack([dot(lo_ctx, gg, 0, 0), dot(lo_hid, gg, 0, 0)], axis=1)
        d_a_out = dot(ctx, low_grad[:, :128], 1, 0)
        d_a_down = dot(hidden, low_grad[:, 128:], 0, 0)
        d_b_qkv = SCALE * jnp.stack([
            dot(low3[:, 128 * i:128 * (i + 1)], d_lin[width * i:width * (i + 1)], 0, 1) for i in range(3)])
        d_b_up = SCALE * dot(low1, d_pre, 0, 0)
        back = [(SCALE * dot(d_lin[width * i:width * (i + 1)], b_qkv[i], 0, 1)).astype(BF) for i in range(3)]
        back.append((SCALE * dot(d_pre, b_up, 1, 1)).astype(BF))
        d_a_in = jnp.stack([dot(back[i], n1 if i < 3 else n2, 0, 0) for i in range(4)], axis=1)
        terms = (d_a_in, d_b_qkv, d_b_up, d_a_out, d_a_down, d_b_out, norms)
        sums = terms if sums is None else tuple(p + q for p, q in zip(sums, terms))

    d_a_in, d_b_qkv, d_b_up, d_a_out, d_a_down, d_b_out, norms = sums
    d_a_in = lax.psum_scatter(d_a_in, "tensor", scatter_dimension=0, tiled=True)
    d_b_out = lax.psum_scatter(d_b_out, "tensor", scatter_dimension=0, tiled=True)
    d_a_in, d_b_qkv, d_b_up, d_a_out, d_a_down, d_b_out = lax.psum(
        (d_a_in, d_b_qkv, d_b_up, d_a_out, d_a_down, d_b_out), "dp")
    norms = lax.psum(norms, ("dp", "tensor"))
    return (jnp.stack(outs)[:, None], jnp.stack(grads)[:, None], norms[:2], norms[2:],
            jnp.transpose(d_a_in, (1, 2, 0)), d_b_qkv, d_b_up, d_a_out, d_a_down,
            jnp.transpose(d_b_out, (1, 0, 2)))


RANK = 128


MESH = pl.DeviceIdType.MESH


def place():
    d = lax.axis_index("dp")
    return d // 2, d % 2, lax.axis_index("tensor")


def meet(z, c, t, planes):
    barrier = pltpu.get_barrier_semaphore()
    for h in (0, 1):
        for k in range(4):
            if h or k:
                pl.semaphore_signal(barrier, 1, device_id=(2 * z + (c ^ h), t ^ k), device_id_type=MESH)
    for k in planes:
        pl.semaphore_signal(barrier, 1, device_id=(2 * (z ^ k) + c, t), device_id_type=MESH)
    pl.semaphore_wait(barrier, 7 + len(planes))


def remote(src, dst, send_sem, recv_sem, device):
    return pltpu.make_async_remote_copy(src_ref=src, dst_ref=dst, send_sem=send_sem, recv_sem=recv_sem,
                                        device_id=device, device_id_type=MESH)


class Rows:
    def __init__(self, v, full, sems, stage, local, z, c, t):
        self.v, self.full, self.sems, self.stage, self.local = v, full, sems, stage, local
        self.z, self.c, self.t = z, c, t

    def rows(self, s, h):
        return self.full.at[pl.ds(pl.multiple_of(s * 512 + h * 256, 256), 256)]

    def block(self, m, h):
        return self.v.at[m, pl.ds(pl.multiple_of(h * 256, 256), 256)]

    def copy(self, m, other):
        h = self.c ^ other
        return remote(self.block(m, h), self.rows(self.t, h), self.sems.at[2 * m + other], self.sems.at[4 + self.t],
                      (2 * self.z + h, 2 * m + self.c))

    def forward(self, s):
        part = self.rows(s, self.c)
        return remote(part, part, self.sems.at[8 + s], self.sems.at[12 + s], (2 * self.z + (self.c ^ 1), self.t))

    def start(self):
        for m in (0, 1):
            away = 2 * m + self.c != self.t

            @pl.when(away)
            def _():
                self.copy(m, 0).start()

            self.copy(m, 1).start()

            @pl.when(jnp.logical_not(away))
            def _():
                pltpu.make_async_copy(self.block(m, self.c), self.stage, self.local.at[0]).start()

    def relay(self):
        mine = self.t % 2 == self.c

        @pl.when(mine)
        def _():
            pltpu.make_async_copy(self.block(0, self.c), self.stage, self.local.at[0]).wait()
            pltpu.make_async_copy(self.stage, self.rows(self.t, self.c), self.sems.at[4 + self.t]).start()

        for k in (0, 1, 2, 3):
            s = self.t ^ k
            pltpu.make_async_copy(self.stage, self.rows(s, self.c), self.sems.at[4 + s]).wait()
            self.forward(s).start()

    def finish(self):
        for s in range(4):
            part = self.rows(s, self.c ^ 1)
            remote(part, part, self.sems.at[8 + s], self.sems.at[12 + s], (2 * self.z + (self.c ^ 1), self.t)).wait_recv()
            self.forward(s).wait_send()
        for m in (0, 1):
            @pl.when(2 * m + self.c != self.t)
            def _():
                self.copy(m, 0).wait_send()

            self.copy(m, 1).wait_send()


class Blocks:
    def __init__(self, own, where, sems, stage, local, cut, quarter, z, c, t):
        self.own, self.where, self.sems, self.stage, self.local = own, where, sems, stage, local
        self.cut, self.quarter, self.t, self.d, self.half = cut, quarter, t, 2 * z + c, z % 2

    def spot(self, k, other=0):
        return self.cut(self.where(self.t ^ k), self.half ^ other)

    def first(self, k):
        return remote(self.cut(self.own, self.half), self.spot(0), self.sems.at[k - 1], self.sems.at[2 + k],
                      (self.d, self.t ^ k))

    def arrival(self, k):
        return remote(self.spot(k), self.spot(k), self.sems.at[k - 1], self.sems.at[2 + k], (self.d, self.t ^ k))

    def second(self, k):
        part = self.quarter(self.spot(3 - k), k - 1)
        return remote(part, part, self.sems.at[5 + k], self.sems.at[7 + k], (self.d, self.t ^ k))

    def last(self, k):
        part = self.quarter(self.spot(3), k - 1)
        return remote(part, part, self.sems.at[5 + k], self.sems.at[7 + k], (self.d, self.t ^ k))

    def across(self, k, other=0):
        return remote(self.spot(k, other), self.spot(k, other), self.sems.at[9 + k], self.sems.at[12 + k],
                      (self.d ^ 2, self.t))

    def start(self):
        for k in ((1, 2) if self.quarter else (1, 2, 3)):
            self.first(k).start()
        pltpu.make_async_copy(self.own, self.stage, self.local.at[0]).start()

    def store(self):
        pltpu.make_async_copy(self.own, self.stage, self.local.at[0]).wait()
        pltpu.make_async_copy(self.stage, self.where(self.t), self.local.at[1]).start()

    def relay(self):
        for k in (1, 2):
            self.arrival(3 - k).wait_recv()
            if self.quarter:
                self.second(k).start()
            self.across(3 - k).start()

    def pass_on(self):
        if self.quarter:
            for k in (1, 2):
                self.last(k).wait_recv()
        else:
            self.arrival(3).wait_recv()
        self.across(3).start()

    def finish(self):
        pltpu.make_async_copy(self.stage, self.where(self.t), self.local.at[1]).wait()
        for k in (1, 2, 3):
            self.across(k, 1).wait_recv()
            self.across(k).wait_send()
            if k < 3 or not self.quarter:
                self.first(k).wait_send()
            if k < 3 and self.quarter:
                self.second(k).wait_send()


def aligned(i, n):
    return pl.ds(pl.multiple_of(i * n, n), n)


def front_kernel(x, g, wq, wo, ain, bq, ao, bo,
                 xf, gf, wqf, wof, ainf, bqf, aof, bof,
                 row_sems, sems, local, xs, gs, wqs, wos, ains, bqs, aos, bos):
    z, c, t = place()
    meet(z, c, t, (1,))
    at = dict(z=z, c=c, t=t)
    x_rows = Rows(x, xf, row_sems.at[0], xs, local.at[0], **at)
    g_rows = Rows(g, gf, row_sems.at[1], gs, local.at[1], **at)
    qkv = Blocks(wq.at[:, :, aligned(c, 128)], lambda i: wqf.at[:, :, aligned(i, 128)], sems.at[0], wqs, local.at[2],
                 lambda v, h: v.at[:, aligned(h, 512)], lambda v, h: v.at[:, pl.ds(h * 256, 256)], **at)
    into = Blocks(ain, lambda i: ainf.at[:, aligned(i, 32)], sems.at[1], ains, local.at[3],
                  lambda v, h: v.at[pl.ds(2 * h, 2)], None, **at)
    second = Blocks(bq.at[:, :, aligned(c, 128)], lambda i: bqf.at[:, :, aligned(i, 128)], sems.at[2], bqs, local.at[4],
                    lambda v, h: v.at[:, aligned(h, 64)], None, **at)
    out = Blocks(wo.at[aligned(c, 128)], lambda i: wof.at[aligned(i, 128)], sems.at[3], wos, local.at[5],
                 lambda v, h: v.at[aligned(h, 64)], lambda v, h: v.at[pl.ds(h * 32, 32)], **at)
    a_out = Blocks(ao.at[aligned(c, 128)], lambda i: aof.at[aligned(i, 128)], sems.at[4], aos, local.at[6],
                   lambda v, h: v.at[aligned(h, 64)], None, **at)
    b_out = Blocks(bo, lambda i: bof.at[:, aligned(i, 32)], sems.at[5], bos, local.at[7],
                   lambda v, h: v.at[pl.ds(h, 1)], None, **at)
    x_rows.start()
    for v in (into, second, qkv, b_out, a_out, out):
        v.start()
    g_rows.start()
    x_rows.relay()
    for v in (into, second, qkv, b_out, a_out, out):
        v.store()
    for v in (into, second, qkv, b_out, a_out, out):
        v.relay()
    for v in (into, second, qkv, b_out, a_out, out):
        v.pass_on()
    g_rows.relay()
    for v in (x_rows, into, second, qkv, b_out, a_out, out, g_rows):
        v.finish()


def front(x, g, wq, wo, ain, bq, ao, bo):
    shapes = [(2048, 1024), (2048, 1024), (3, 1024, 512), (512, 1024), (4, 128, 1024), (3, 128, 512), (512, 128),
              (2, 128, 1024)]
    anywhere = pl.BlockSpec(memory_space=pl.ANY)
    return pl.pallas_call(
        front_kernel,
        in_specs=[anywhere] * 8,
        out_specs=[anywhere] * 8,
        out_shape=[jax.ShapeDtypeStruct(s, BF) for s in shapes],
        scratch_shapes=[
            pltpu.SemaphoreType.DMA((2, 16)),
            pltpu.SemaphoreType.DMA((6, 16)),
            pltpu.SemaphoreType.DMA((8, 2)),
            pltpu.VMEM((256, 1024), BF),
            pltpu.VMEM((256, 1024), BF),
            pltpu.VMEM((3, 1024, 128), BF),
            pltpu.VMEM((128, 1024), BF),
            pltpu.VMEM((4, 32, 1024), BF),
            pltpu.VMEM((3, 128, 128), BF),
            pltpu.VMEM((128, 128), BF),
            pltpu.VMEM((2, 32, 1024), BF),
        ],
        compiler_params=pltpu.CompilerParams(collective_id=0, has_side_effects=True),
        name="front",
    )(x, g, wq, wo, ain, bq, ao, bo)


def back_kernel(rows, dbq, dbu, dao, dad, dsh, dno,
                out, obq, obu, oao, oad, osh, ono,
                row_sems, share_sems, cross_sems, z_sems, last_sems, norm_sems,
                sh_in, sh, rbq, rbu, rao, rad, rsh, pbq, pbu, pao, pad, psh, qbq, qbu, qao, qad, qsh, no_in, no_sum):
    z, c, t = place()
    meet(z, c, t, (1, 2))
    d = 2 * z + c
    sibling = (2 * z + (c ^ 1), t)

    home = t % 2
    local = home == c
    spot = aligned(c, 256)

    def row(k):
        return remote(rows.at[t ^ k], out.at[t // 2, spot], row_sems.at[k], row_sems.at[4 + (t // 2) * 2 + c],
                      (2 * z + home, t ^ k))

    def own_row():
        return pltpu.make_async_copy(rows.at[t], out.at[t // 2, spot], row_sems.at[4 + (t // 2) * 2 + c])

    @pl.when(local)
    def _():
        own_row().start()

    @pl.when(jnp.logical_not(local))
    def _():
        row(0).start()

    for k in (1, 2, 3):
        row(k).start()

    peers = (sibling, (d, t ^ 1), (d, t ^ 2), (d ^ 2, t), (d ^ 4, t))

    def norm(i):
        return remote(dno if i == 0 else no_sum.at[i - 1], no_in.at[i], norm_sems.at[0, i], norm_sems.at[1, i], peers[i])

    def norm_next(i):
        norm(i).wait_recv()
        total = (dno[...] if i == 0 else no_sum[i - 1]) + no_in[i]
        if i < 4:
            no_sum[i] = total
            norm(i + 1).start()
        else:
            ono[...] = total

    norm(0).start()

    def share():
        return remote(dsh.at[:, :, aligned(c ^ 1, 512)], sh_in, share_sems.at[0], share_sems.at[1], sibling)

    share().start()
    share().wait_recv()
    norm_next(0)
    for i in range(6):
        sh[i] = (dsh[i, :, aligned(c, 512)].astype(F32) + sh_in[i].astype(F32)).astype(BF)

    def parts(j):
        return (dbq.at[:, :, aligned(j, 128)], dbu.at[:, aligned(j, 512)], dao.at[aligned(j, 128)],
                dad.at[:, aligned(j, 512)], sh.at[:, aligned(j, 32)])

    got = (rbq, rbu, rao, rad, rsh)

    def cross(k, i):
        return remote(parts(t ^ k)[i], got[i].at[k - 1], cross_sems.at[0, k - 1, i], cross_sems.at[1, k - 1, i], (d, t ^ k))

    for k in (1, 2, 3):
        for i in range(5):
            cross(k, i).start()
    norm_next(1)
    norm_next(2)

    sums = (pbq, pbu, pao, pad, psh)
    halves = (qbq, qbu, qao, qad, qsh)
    low = z % 2

    def half(v, i, j):
        if i == 0:
            return v.at[:, aligned(j, 64)]
        if i == 4:
            return v.at[:, aligned(j, 16)]
        return v.at[aligned(j, 64)]

    def along(step, i):
        j = low ^ 1 if step == 0 else low
        dst = sums[i].at[2] if step == 2 else halves[i].at[step]
        return remote(half(sums[i].at[step], i, j), half(dst, i, j), z_sems.at[0, step, i], z_sems.at[1, step, i],
                      (d ^ (4 if step == 1 else 2), t))

    def arrived(step, i):
        j = low ^ 1 if step == 2 else low
        dst = sums[i].at[2] if step == 2 else halves[i].at[step]
        return remote(half(dst, i, j), half(dst, i, j), z_sems.at[0, step, i], z_sems.at[1, step, i], (d, t ^ 1))

    for i in range(5):
        for k in (1, 2, 3):
            cross(k, i).wait_recv()
        total = parts(t)[i][...].astype(F32)
        for k in (0, 1, 2):
            total = total + got[i][k].astype(F32)
        sums[i][0] = total.astype(BF)
        along(0, i).start()
    norm_next(3)
    for step in (0, 1):
        for i in range(5):
            arrived(step, i).wait_recv()
            mine, other = half(sums[i].at[step], i, low), half(halves[i].at[step], i, low)
            half(sums[i].at[step + 1], i, low)[...] = (mine[...].astype(F32) + other[...].astype(F32)).astype(BF)
            along(step + 1, i).start()
        if step == 0:
            norm_next(4)
    result = (obq.at[:, :, aligned(c, 128)], obu.at[:, aligned(c, 512)], oao.at[aligned(c, 128)],
              oad.at[:, aligned(c, 512)], osh.at[:, :, aligned(c, 512)])
    theirs = (obq.at[:, :, aligned(c ^ 1, 128)], obu.at[:, aligned(c ^ 1, 512)], oao.at[aligned(c ^ 1, 128)],
              oad.at[:, aligned(c ^ 1, 512)], osh.at[:, :, aligned(c ^ 1, 512)])

    def last(i):
        return remote(result[i], result[i], last_sems.at[0, i], last_sems.at[1, i], sibling)

    for i in range(5):
        arrived(2, i).wait_recv()
        result[i][...] = sums[i][2].astype(F32)
        last(i).start()

    for i in range(5):
        remote(theirs[i], theirs[i], last_sems.at[0, i], last_sems.at[1, i], sibling).wait_recv()
        last(i).wait_send()
        for step in (0, 1, 2):
            along(step, i).wait_send()
        for k in (1, 2, 3):
            cross(k, i).wait_send()
    share().wait_send()
    for i in range(5):
        norm(i).wait_send()
    for k in (1, 2, 3):
        row(k).wait_send()

    @pl.when(jnp.logical_not(local))
    def _():
        row(0).wait_send()

    for m in (0, 1):
        for h in (0, 1):
            pltpu.make_async_copy(rows.at[0], out.at[m, pl.ds(256 * h, 256)], row_sems.at[4 + 2 * m + h]).wait()


def back(rows, dbq, dbu, dao, dad, dsh, dno):
    vmem = pl.BlockSpec(memory_space=pltpu.VMEM)
    part = [(3, 128, 128), (128, 512), (128, 128), (128, 512), (6, 32, 512)]
    outs = [((2, 512, 1024), BF), ((3, 128, 256), F32), ((128, 1024), F32), ((256, 128), F32), ((128, 1024), F32),
            ((6, 32, 1024), F32), ((4, 1024), F32)]
    return pl.pallas_call(
        back_kernel,
        in_specs=[vmem] * 7,
        out_specs=[pl.BlockSpec(memory_space=pl.ANY)] + [vmem] * 6,
        out_shape=[jax.ShapeDtypeStruct(s, d) for s, d in outs],
        scratch_shapes=[
            pltpu.SemaphoreType.DMA((8,)),
            pltpu.SemaphoreType.DMA((2,)),
            pltpu.SemaphoreType.DMA((2, 3, 5)),
            pltpu.SemaphoreType.DMA((2, 3, 5)),
            pltpu.SemaphoreType.DMA((2, 5)),
            pltpu.SemaphoreType.DMA((2, 5)),
            pltpu.VMEM((6, 128, 512), BF),
            pltpu.VMEM((6, 128, 512), BF),
        ] + [pltpu.VMEM((3,) + s, BF) for s in part + part] + [pltpu.VMEM((2,) + s, BF) for s in part] + [
            pltpu.VMEM((5, 4, 1024), F32),
            pltpu.VMEM((4, 4, 1024), F32),
        ],
        compiler_params=pltpu.CompilerParams(collective_id=1, has_side_effects=True),
        name="back",
    )(rows, dbq, dbu, dao, dad, dsh, dno)


def swap(v, k=1):
    return lax.ppermute(v, "dp", [(i, i ^ k) for i in range(lax.axis_size("dp"))])


def pick(v, axis, index, size):
    return lax.dynamic_slice_in_dim(v, index * size, size, axis)


def half_rows(v, c):
    return pick(v.reshape(4, 2, 256, -1), 1, c, 1)[:, 0]


def from_group(own, c):
    got = lax.all_to_all(own, "tensor", 0, 0, tiled=True).reshape(2, 2, 256, -1)
    mine = pick(got, 1, c, 1)[:, 0]
    other = swap(pick(got, 1, 1 - c, 1)[:, 0])
    return jnp.where(c == 0, jnp.stack([mine, other], 1), jnp.stack([other, mine], 1)).reshape(2, 512, -1)


def by_groups(x, gy, segment, keep, gain, bias, w_qkv, w_out, w_up, w_down,
              a_in, b_qkv, b_up, a_out, a_down, b_out):
    z, c, t = place()
    tables = jnp.stack([segment[:, 0], keep[:, 0]], 1)
    pair = jnp.where(t % 2 == c, tables, swap(tables))
    seg, kept = jnp.where(t // 2 == 0, pair[0], pair[1])

    x_full, g_full, qkv, out, a_full, b_qkv_all, a_out_all, b_full = front(
        x[:, 0], gy[:, 0], w_qkv, w_out, jnp.swapaxes(a_in, 1, 2), b_qkv, a_out, b_out)
    up, down = lax.optimization_barrier((
        jnp.concatenate([pick(w_up, 1, c, 512), pick(b_up, 1, c, 512)], axis=0),
        jnp.concatenate([pick(w_down, 0, c, 512), pick(a_down, 0, c, 512)], axis=1), x_full))[:2]
    up = lax.all_gather(up, "tensor", axis=0)
    down = lax.all_gather(down, "tensor", axis=0, tiled=True)
    w_up_all = jnp.concatenate([up[i, :1024] for i in range(4)], axis=1)
    b_up_all = jnp.concatenate([up[i, 1024:] for i in range(4)], axis=1)
    w_down_all, a_down_all = down[:, :1024], down[:, 1024:]

    m_qkv = (qkv.astype(F32) + SCALE * jnp.einsum("nrk,nrc->nkc", a_full[:3], b_qkv_all,
                                                  preferred_element_type=F32)).astype(BF)
    m_up = (w_up_all.astype(F32) + SCALE * dot(a_full[3], b_up_all, 0, 0)).astype(BF)
    m_out = (out.astype(F32) + SCALE * dot(a_out_all, b_full[0], 1, 0)).astype(BF)
    m_down = (w_down_all.astype(F32) + SCALE * dot(a_down_all, b_full[1], 1, 0)).astype(BF)
    a_three = a_full[:3].reshape(3 * RANK, 1024)
    b_both = b_full.reshape(2 * RANK, 1024)

    standard, inverse = normalized(x_full.astype(F32))
    n1 = (standard * gain[0] + bias[0]).astype(BF)
    n2 = (standard * gain[1] + bias[1]).astype(BF)
    lin = jnp.einsum("nkc,sk->ncs", m_qkv, n1, preferred_element_type=F32)
    low3 = dot(a_three, n1, 1, 1).astype(BF).reshape(3, RANK, 2048)
    low1 = dot(a_full[3], n2, 1, 1).astype(BF)
    g_ctx = dot(m_out, g_full, 1, 1).astype(BF)
    low_grad = (SCALE * dot(b_both, g_full, 1, 1)).astype(BF)
    cos, sin = rotary_tables(seg)
    ctx, d_lin = attention(lin, g_ctx, cos, sin, seg, kept)

    pre = dot(n2, m_up, 1, 0)
    cdf = 0.5 * (1.0 + lax.erf(pre * math.sqrt(0.5)))
    hidden = (pre * cdf).astype(BF)
    slope = cdf + pre * (math.sqrt(0.5 / math.pi) * jnp.exp(-0.5 * pre * pre))
    d_pre = (dot(g_full, m_down, 1, 1) * slope).astype(BF)

    part = dot(ctx, m_out, 0, 0) + dot(hidden, m_down, 1, 0)
    theirs = swap(half_rows(part, 1 - c).astype(BF))
    y = half_rows(x_full, c).astype(F32) + half_rows(part, c) + theirs.astype(F32)
    y = from_group(y.astype(BF), c)

    one = jnp.einsum("ncs,nkc->sk", d_lin, m_qkv, preferred_element_type=F32)
    two = dot(d_pre, m_up, 1, 1)
    total = gain[0] * one + gain[1] * two
    theirs = swap(half_rows(total, 1 - c).astype(BF))
    total = half_rows(total, c) + theirs.astype(F32)
    own = half_rows(standard, c)
    grad = total - jnp.mean(total, axis=-1, keepdims=True)
    grad = grad - own * jnp.mean(total * own, axis=-1, keepdims=True)
    grad = half_rows(g_full, c).astype(F32) + grad * half_rows(inverse, c)

    norms = jnp.stack([jnp.sum(one * standard, axis=0), jnp.sum(two * standard, axis=0),
                       jnp.sum(one, axis=0), jnp.sum(two, axis=0)])
    lo = jnp.concatenate([dot(a_out_all, ctx, 0, 0), dot(a_down_all, hidden, 0, 1)], axis=0).astype(BF)
    d_a_out = dot(ctx, low_grad[:RANK], 1, 1).astype(BF)
    d_a_down = dot(low_grad[RANK:], hidden, 1, 0).astype(BF)
    d_b_qkv = (SCALE * jnp.einsum("nrs,ncs->nrc", low3, d_lin, preferred_element_type=F32)).astype(BF)
    d_b_up = (SCALE * dot(low1, d_pre, 1, 0)).astype(BF)
    back3 = (SCALE * jnp.einsum("nrc,ncs->nrs", b_qkv_all, d_lin, preferred_element_type=F32)).astype(BF)
    back1 = (SCALE * dot(b_up_all, d_pre, 1, 1)).astype(BF)
    shared = jnp.concatenate([dot(back3.reshape(3 * RANK, 2048), n1, 1, 0).astype(BF), dot(back1, n2, 1, 0).astype(BF),
                              (SCALE * dot(lo, g_full, 1, 0)).astype(BF)], axis=0).reshape(6, RANK, 1024)
    grad, r_b_qkv, r_b_up, r_a_out, r_a_down, rest, norms = back(
        grad.astype(BF), d_b_qkv, d_b_up, d_a_out, d_a_down, shared, norms)
    r_a_in = jnp.swapaxes(rest[:4], 1, 2)
    return (y[:, None], grad[:, None], norms[:2], norms[2:], r_a_in, r_b_qkv, r_b_up, r_a_out, jnp.transpose(r_a_down), rest[4:])


def solution(mesh):
    in_specs = (
        P(None, "dp", "tensor", None),
        P(None, "dp", "tensor", None),
        P(None, "dp", None),
        P(None, "dp", None),
        P(),
        P(),
        P(None, None, "tensor"),
        P("tensor", None),
        P(None, "tensor"),
        P("tensor", None),
        P(None, None, "tensor"),
        P(None, None, "tensor"),
        P(None, "tensor"),
        P("tensor", None),
        P("tensor", None),
        P(None, "tensor", None),
    )
    out_specs = (
        P(None, "dp", "tensor", None),
        P(None, "dp", "tensor", None),
        P(),
        P(),
        P(None, None, "tensor"),
        P(None, None, "tensor"),
        P(None, "tensor"),
        P("tensor", None),
        P("tensor", None),
        P(None, "tensor", None),
    )
    small = mesh.shape["tensor"] == 4 and mesh.shape["dp"] == 8
    return jax.shard_map(
        by_groups if small else by_features, mesh=mesh, in_specs=in_specs, out_specs=out_specs, check_vma=False
    )
```

```python
import functools
import math

import jax
import jax.numpy as jnp
from jax import lax
from jax.experimental import pallas as pl
from jax.experimental.pallas import tpu as pltpu
from jax.sharding import PartitionSpec as P

HEAD = 64
HALF = 8
N_DOCS = 5
TILE = 256
SLOTS = 5
EPSILON = 1e-05
SCALE = 0.25
F32 = jnp.float32
BF = jnp.bfloat16


def dot(a, b, ca, cb):
    return lax.dot_general(a, b, (((ca,), (cb,)), ((), ())), preferred_element_type=F32)


def attention_kernel(heads, lo_ref, lin_ref, g_ref, cos_ref, sin_ref, segq_ref, segk_ref,
                     ctx_ref, dlin_ref, qt, kt, vt, kn, vn, acc, s_scr, e_scr, p_scr, row):
    length = lin_ref.shape[2]
    blocks = length // TILE

    def rotate(z, cos, sin):
        a, b = z[:HALF], z[HALF:2 * HALF]
        return jnp.concatenate([a * cos - b * sin, b * cos + a * sin, z[2 * HALF:]], axis=0)

    def prepare(c, carry):
        cols = pl.ds(pl.multiple_of(c * TILE, TILE), TILE)
        cos, sin = cos_ref[:, cols], sin_ref[:, cols]
        for h in range(heads):
            rows = pl.ds(h * HEAD, HEAD)
            q = rotate(lin_ref[0, pl.ds(h * HEAD, HEAD), cols], cos, sin).astype(BF).astype(F32) * 0.125
            k = rotate(lin_ref[1, pl.ds(h * HEAD, HEAD), cols], cos, sin)
            v = lin_ref[2, pl.ds(h * HEAD, HEAD), cols]
            qt[rows, cols] = q.astype(BF)
            kt[rows, cols] = k.astype(BF)
            vt[rows, cols] = v.astype(BF)
            kn[h, cols, :] = jnp.transpose(k).astype(BF)
            vn[h, cols, :] = jnp.transpose(v).astype(BF)
            acc[h, :, cols] = jnp.zeros((2 * HEAD, TILE), F32)
        return carry

    lax.fori_loop(0, blocks, prepare, 0)

    def query_block(qb, carry):
        lo = lo_ref[qb]
        qcols = pl.ds(pl.multiple_of(qb * TILE, TILE), TILE)
        segq = segq_ref[:, qcols]

        def scores(kb, tops, last=False):
            krows = pl.ds(pl.multiple_of(kb * TILE, TILE), TILE)
            allowed = segk_ref[krows, :] == segq
            if last:
                k, q = (lax.broadcasted_iota(jnp.int32, (TILE, TILE), i) for i in (0, 1))
                allowed = (allowed & (k < q)) | (k == q)
            out = []
            for h in range(heads):
                rows = pl.ds(h * HEAD, HEAD)
                s = dot(kn[h, krows, :], qt[rows, qcols], 1, 0)
                s = jnp.where(allowed, s, -1e30)
                s_scr[h, kb - lo] = s
                p_scr[h, kb - lo] = dot(vn[h, krows, :], g_ref[rows, qcols], 1, 0)
                out.append(jnp.maximum(tops[h], jnp.max(s, axis=0, keepdims=True)))
            return tuple(out)

        tops = lax.fori_loop(lo, qb, scores, tuple(jnp.full((1, TILE), -1e30, F32) for _ in range(heads)))
        tops = scores(qb, tops, True)

        def weights(kb, sums):
            kcols = pl.ds(pl.multiple_of(kb * TILE, TILE), TILE)
            out = []
            for h in range(heads):
                e = jnp.exp(s_scr[h, kb - lo] - tops[h])
                low = e.astype(BF)
                e_scr[h, kb - lo] = low
                out.append(sums[h] + jnp.sum(e, axis=0, keepdims=True))
                row[h] += dot(vt[pl.ds(h * HEAD, HEAD), kcols], low, 1, 0)
            return tuple(out)

        row[...] = jnp.zeros_like(row)
        sums = lax.fori_loop(lo, qb + 1, weights, tuple(jnp.zeros((1, TILE), F32) for _ in range(heads)))
        gts, terms, scales = [], [], []
        for h in range(heads):
            rows = pl.ds(h * HEAD, HEAD)
            inverse = 1.0 / sums[h]
            ctx = row[h] * inverse
            ctx_ref[rows, qcols] = ctx.astype(BF)
            g = g_ref[rows, qcols].astype(F32)
            terms.append(jnp.sum(g * ctx, axis=0, keepdims=True))
            scales.append(inverse)
            gts.append((g * inverse).astype(BF))

        row[...] = jnp.zeros_like(row)

        def backward(kb, carry):
            krows = pl.ds(pl.multiple_of(kb * TILE, TILE), TILE)
            for h in range(heads):
                low = e_scr[h, kb - lo]
                ds = (low.astype(F32) * ((p_scr[h, kb - lo] - terms[h]) * scales[h])).astype(BF)
                acc[h, :HEAD, krows] += dot(gts[h], low, 1, 1)
                acc[h, HEAD:, krows] += dot(qt[pl.ds(h * HEAD, HEAD), qcols], ds, 1, 1)
                row[h] += dot(kt[pl.ds(h * HEAD, HEAD), krows], ds, 1, 0)
            return carry

        lax.fori_loop(lo, qb + 1, backward, 0)
        cos, sin = cos_ref[:, qcols], sin_ref[:, qcols]
        for h in range(heads):
            dlin_ref[0, pl.ds(h * HEAD, HEAD), qcols] = rotate(row[h] * 0.125, cos, -sin).astype(BF)
        return carry

    lax.fori_loop(0, blocks, query_block, 0)

    def finish(c, carry):
        cols = pl.ds(pl.multiple_of(c * TILE, TILE), TILE)
        cos, sin = cos_ref[:, cols], sin_ref[:, cols]
        for h in range(heads):
            both = acc[h, :, cols]
            dlin_ref[1, pl.ds(h * HEAD, HEAD), cols] = rotate(both[HEAD:], cos, -sin).astype(BF)
            dlin_ref[2, pl.ds(h * HEAD, HEAD), cols] = both[:HEAD].astype(BF)
        return carry

    lax.fori_loop(0, blocks, finish, 0)


def attention(lin, g, cos, sin, segment, keep):
    width, length = g.shape
    heads = min(4, width // HEAD)
    wide = heads * HEAD
    starts = jnp.sum(segment[None, :] < jnp.arange(N_DOCS, dtype=jnp.int32)[:, None], axis=1)
    firsts = segment[::TILE]
    lo = jnp.sum(jnp.where(firsts[:, None] == jnp.arange(N_DOCS)[None, :], starts[None, :], 0), axis=1)
    lo = (lo // TILE).astype(jnp.int32)
    segk = jnp.where(keep == 1, segment, -1)[:, None]
    vmem = pl.BlockSpec(memory_space=pltpu.VMEM)
    three = pl.BlockSpec((3, wide, length), lambda i, lo: (0, i, 0))
    single = pl.BlockSpec((wide, length), lambda i, lo: (i, 0))
    return pl.pallas_call(
        functools.partial(attention_kernel, heads),
        grid_spec=pltpu.PrefetchScalarGridSpec(
            num_scalar_prefetch=1,
            grid=(width // wide,),
            in_specs=[three, single] + [vmem] * 4,
            out_specs=[single, three],
            scratch_shapes=[
                pltpu.VMEM((wide, length), BF),
                pltpu.VMEM((wide, length), BF),
                pltpu.VMEM((wide, length), BF),
                pltpu.VMEM((heads, length, HEAD), BF),
                pltpu.VMEM((heads, length, HEAD), BF),
                pltpu.VMEM((heads, 2 * HEAD, length), F32),
                pltpu.VMEM((heads, SLOTS, TILE, TILE), F32),
                pltpu.VMEM((heads, SLOTS, TILE, TILE), BF),
                pltpu.VMEM((heads, SLOTS, TILE, TILE), F32),
                pltpu.VMEM((heads, HEAD, TILE), F32),
            ]),
        out_shape=[jax.ShapeDtypeStruct((width, length), BF), jax.ShapeDtypeStruct((3, width, length), BF)],
        compiler_params=pltpu.CompilerParams(vmem_limit_bytes=60 << 20),
        name="attention",
        cost_estimate=pl.CostEstimate(flops=10 * width * length * 768, transcendentals=width * length * 12,
                                      bytes_accessed=26 * width * length),
    )(lo, lin, g, cos, sin, segment[None, :], segk)


def rotary_tables(segment):
    length = segment.shape[0]
    starts = jnp.sum(segment[None, :] < jnp.arange(N_DOCS, dtype=jnp.int32)[:, None], axis=1)
    begin = jnp.sum(jnp.where(segment[None, :] == jnp.arange(N_DOCS)[:, None], starts[:, None], 0), axis=0)
    position = (jnp.arange(length, dtype=jnp.int32) - begin).astype(F32)
    exponent = jnp.arange(HALF, dtype=F32) / HALF
    frequency = jnp.exp(-math.log(10000.0) * exponent)
    angles = frequency[:, None] * position[None, :]
    return jnp.cos(angles), jnp.sin(angles)


def normalized(values):
    average = jnp.mean(values, axis=-1, keepdims=True)
    centered = values - average
    variance = jnp.mean(centered * centered, axis=-1, keepdims=True)
    inverse = lax.rsqrt(variance + EPSILON)
    return centered * inverse, inverse


def by_features(x, gy, segment, keep, gain, bias, w_qkv, w_out, w_up, w_down,
              a_in, b_qkv, b_up, a_out, a_down, b_out):
    width = w_qkv.shape[2]
    micro = x.shape[0]
    a_full = lax.all_gather(a_in, "tensor", axis=2, tiled=True)
    b_full = lax.all_gather(b_out, "tensor", axis=1, tiled=True)

    m_qkv = jnp.concatenate([
        (w_qkv[i].astype(F32) + SCALE * dot(a_full[i], b_qkv[i], 1, 0)).astype(BF) for i in range(3)
    ], axis=1)
    m_up = (w_up.astype(F32) + SCALE * dot(a_full[3], b_up, 1, 0)).astype(BF)
    m_out = (w_out.astype(F32) + SCALE * dot(a_out, b_full[0], 1, 0)).astype(BF)
    m_down = (w_down.astype(F32) + SCALE * dot(a_down, b_full[1], 1, 0)).astype(BF)
    a_three = jnp.concatenate([a_full[0], a_full[1], a_full[2]], axis=1)
    b_both = jnp.concatenate([b_full[0], b_full[1]], axis=0)

    outs, grads, sums = [], [], None
    for m in range(micro):
        rows, seg = x[m, 0], segment[m, 0]
        xg = lax.all_gather(rows, "tensor", axis=0, tiled=True)
        gg = lax.all_gather(gy[m, 0], "tensor", axis=0, tiled=True)
        standard, _ = normalized(xg.astype(F32))
        n1 = (standard * gain[0] + bias[0]).astype(BF)
        n2 = (standard * gain[1] + bias[1]).astype(BF)
        lin = dot(m_qkv, n1, 0, 1)
        low3 = dot(n1, a_three, 1, 0).astype(BF)
        low1 = dot(n2, a_full[3], 1, 0).astype(BF)
        g_ctx = dot(m_out, gg, 1, 1).astype(BF)
        low_grad = (SCALE * dot(gg, b_both, 1, 1)).astype(BF)
        cos, sin = rotary_tables(seg)
        ctx, d_lin = attention(lin.reshape(3, width, -1), g_ctx, cos, sin, seg, keep[m, 0])
        d_lin = d_lin.reshape(3 * width, -1)

        pre = dot(n2, m_up, 1, 0)
        cdf = 0.5 * (1.0 + lax.erf(pre * math.sqrt(0.5)))
        hidden = (pre * cdf).astype(BF)
        slope = cdf + pre * (math.sqrt(0.5 / math.pi) * jnp.exp(-0.5 * pre * pre))
        d_pre = (dot(gg, m_down, 1, 1) * slope).astype(BF)

        part = dot(ctx, m_out, 0, 0) + dot(hidden, m_down, 1, 0)
        branch = lax.psum_scatter(part.astype(BF), "tensor", scatter_dimension=0, tiled=True)
        outs.append((rows.astype(F32) + branch.astype(F32)).astype(BF))

        one = dot(d_lin, m_qkv, 0, 1)
        two = dot(d_pre, m_up, 1, 1)
        total = (gain[0] * one + gain[1] * two).astype(BF)
        total = lax.psum_scatter(total, "tensor", scatter_dimension=0, tiled=True).astype(F32)
        own, inverse = normalized(rows.astype(F32))
        grad = total - jnp.mean(total, axis=-1, keepdims=True)
        grad = grad - own * jnp.mean(total * own, axis=-1, keepdims=True)
        grads.append((gy[m, 0].astype(F32) + grad * inverse).astype(BF))

        norms = jnp.stack([jnp.sum(one * standard, axis=0), jnp.sum(two * standard, axis=0),
                           jnp.sum(one, axis=0), jnp.sum(two, axis=0)])
        lo_ctx = dot(ctx, a_out, 0, 0).astype(BF)
        lo_hid = dot(hidden, a_down, 1, 0).astype(BF)
        d_b_out = SCALE * jnp.stack([dot(lo_ctx, gg, 0, 0), dot(lo_hid, gg, 0, 0)], axis=1)
        d_a_out = dot(ctx, low_grad[:, :128], 1, 0)
        d_a_down = dot(hidden, low_grad[:, 128:], 0, 0)
        d_b_qkv = SCALE * jnp.stack([
            dot(low3[:, 128 * i:128 * (i + 1)], d_lin[width * i:width * (i + 1)], 0, 1) for i in range(3)])
        d_b_up = SCALE * dot(low1, d_pre, 0, 0)
        back = [(SCALE * dot(d_lin[width * i:width * (i + 1)], b_qkv[i], 0, 1)).astype(BF) for i in range(3)]
        back.append((SCALE * dot(d_pre, b_up, 1, 1)).astype(BF))
        d_a_in = jnp.stack([dot(back[i], n1 if i < 3 else n2, 0, 0) for i in range(4)], axis=1)
        terms = (d_a_in, d_b_qkv, d_b_up, d_a_out, d_a_down, d_b_out, norms)
        sums = terms if sums is None else tuple(p + q for p, q in zip(sums, terms))

    d_a_in, d_b_qkv, d_b_up, d_a_out, d_a_down, d_b_out, norms = sums
    d_a_in = lax.psum_scatter(d_a_in, "tensor", scatter_dimension=0, tiled=True)
    d_b_out = lax.psum_scatter(d_b_out, "tensor", scatter_dimension=0, tiled=True)
    d_a_in, d_b_qkv, d_b_up, d_a_out, d_a_down, d_b_out = lax.psum(
        (d_a_in, d_b_qkv, d_b_up, d_a_out, d_a_down, d_b_out), "dp")
    norms = lax.psum(norms, ("dp", "tensor"))
    return (jnp.stack(outs)[:, None], jnp.stack(grads)[:, None], norms[:2], norms[2:],
            jnp.transpose(d_a_in, (1, 2, 0)), d_b_qkv, d_b_up, d_a_out, d_a_down,
            jnp.transpose(d_b_out, (1, 0, 2)))


RANK = 128


MESH = pl.DeviceIdType.MESH


def place():
    d = lax.axis_index("dp")
    return d // 2, d % 2, lax.axis_index("tensor")


def meet(z, c, t, planes):
    barrier = pltpu.get_barrier_semaphore()
    for h in (0, 1):
        for k in range(4):
            if h or k:
                pl.semaphore_signal(barrier, 1, device_id=(2 * z + (c ^ h), t ^ k), device_id_type=MESH)
    for k in planes:
        pl.semaphore_signal(barrier, 1, device_id=(2 * (z ^ k) + c, t), device_id_type=MESH)
    pl.semaphore_wait(barrier, 7 + len(planes))


def remote(src, dst, send_sem, recv_sem, device):
    return pltpu.make_async_remote_copy(src_ref=src, dst_ref=dst, send_sem=send_sem, recv_sem=recv_sem,
                                        device_id=device, device_id_type=MESH)


class Rows:
    def __init__(self, v, full, sems, stage, local, z, c, t):
        self.v, self.full, self.sems, self.stage, self.local = v, full, sems, stage, local
        self.z, self.c, self.t = z, c, t

    def rows(self, s, h):
        return self.full.at[pl.ds(pl.multiple_of(s * 512 + h * 256, 256), 256)]

    def block(self, m, h):
        return self.v.at[m, pl.ds(pl.multiple_of(h * 256, 256), 256)]

    def copy(self, m, other):
        h = self.c ^ other
        return remote(self.block(m, h), self.rows(self.t, h), self.sems.at[2 * m + other], self.sems.at[4 + self.t],
                      (2 * self.z + h, 2 * m + self.c))

    def forward(self, s):
        part = self.rows(s, self.c)
        return remote(part, part, self.sems.at[8 + s], self.sems.at[12 + s], (2 * self.z + (self.c ^ 1), self.t))

    def start(self):
        for m in (0, 1):
            away = 2 * m + self.c != self.t

            @pl.when(away)
            def _():
                self.copy(m, 0).start()

            self.copy(m, 1).start()

            @pl.when(jnp.logical_not(away))
            def _():
                pltpu.make_async_copy(self.block(m, self.c), self.stage, self.local.at[0]).start()

    def relay(self):
        mine = self.t % 2 == self.c

        @pl.when(mine)
        def _():
            pltpu.make_async_copy(self.block(0, self.c), self.stage, self.local.at[0]).wait()
            pltpu.make_async_copy(self.stage, self.rows(self.t, self.c), self.sems.at[4 + self.t]).start()

        for k in (0, 1, 2, 3):
            s = self.t ^ k
            pltpu.make_async_copy(self.stage, self.rows(s, self.c), self.sems.at[4 + s]).wait()
            self.forward(s).start()

    def finish(self):
        for s in range(4):
            part = self.rows(s, self.c ^ 1)
            remote(part, part, self.sems.at[8 + s], self.sems.at[12 + s], (2 * self.z + (self.c ^ 1), self.t)).wait_recv()
            self.forward(s).wait_send()
        for m in (0, 1):
            @pl.when(2 * m + self.c != self.t)
            def _():
                self.copy(m, 0).wait_send()

            self.copy(m, 1).wait_send()


class Blocks:
    def __init__(self, own, where, sems, stage, local, cut, quarter, z, c, t):
        self.own, self.where, self.sems, self.stage, self.local = own, where, sems, stage, local
        self.cut, self.quarter, self.t, self.d, self.half = cut, quarter, t, 2 * z + c, z % 2

    def spot(self, k, other=0):
        return self.cut(self.where(self.t ^ k), self.half ^ other)

    def first(self, k):
        return remote(self.cut(self.own, self.half), self.spot(0), self.sems.at[k - 1], self.sems.at[2 + k],
                      (self.d, self.t ^ k))

    def arrival(self, k):
        return remote(self.spot(k), self.spot(k), self.sems.at[k - 1], self.sems.at[2 + k], (self.d, self.t ^ k))

    def second(self, k):
        part = self.quarter(self.spot(3 - k), k - 1)
        return remote(part, part, self.sems.at[5 + k], self.sems.at[7 + k], (self.d, self.t ^ k))

    def last(self, k):
        part = self.quarter(self.spot(3), k - 1)
        return remote(part, part, self.sems.at[5 + k], self.sems.at[7 + k], (self.d, self.t ^ k))

    def across(self, k, other=0):
        return remote(self.spot(k, other), self.spot(k, other), self.sems.at[9 + k], self.sems.at[12 + k],
                      (self.d ^ 2, self.t))

    def start(self):
        for k in ((1, 2) if self.quarter else (1, 2, 3)):
            self.first(k).start()
        pltpu.make_async_copy(self.own, self.stage, self.local.at[0]).start()

    def store(self):
        pltpu.make_async_copy(self.own, self.stage, self.local.at[0]).wait()
        pltpu.make_async_copy(self.stage, self.where(self.t), self.local.at[1]).start()

    def relay(self):
        for k in (1, 2):
            self.arrival(3 - k).wait_recv()
            if self.quarter:
                self.second(k).start()
            self.across(3 - k).start()

    def pass_on(self):
        if self.quarter:
            for k in (1, 2):
                self.last(k).wait_recv()
        else:
            self.arrival(3).wait_recv()
        self.across(3).start()

    def finish(self):
        pltpu.make_async_copy(self.stage, self.where(self.t), self.local.at[1]).wait()
        for k in (1, 2, 3):
            self.across(k, 1).wait_recv()
            self.across(k).wait_send()
            if k < 3 or not self.quarter:
                self.first(k).wait_send()
            if k < 3 and self.quarter:
                self.second(k).wait_send()


def aligned(i, n):
    return pl.ds(pl.multiple_of(i * n, n), n)


def front_kernel(x, g, wq, wo, ain, bq, ao, bo,
                 xf, gf, wqf, wof, ainf, bqf, aof, bof,
                 row_sems, sems, local, xs, gs, wqs, wos, ains, bqs, aos, bos):
    z, c, t = place()
    meet(z, c, t, (1,))
    at = dict(z=z, c=c, t=t)
    x_rows = Rows(x, xf, row_sems.at[0], xs, local.at[0], **at)
    g_rows = Rows(g, gf, row_sems.at[1], gs, local.at[1], **at)
    qkv = Blocks(wq.at[:, :, aligned(c, 128)], lambda i: wqf.at[:, :, aligned(i, 128)], sems.at[0], wqs, local.at[2],
                 lambda v, h: v.at[:, aligned(h, 512)], lambda v, h: v.at[:, pl.ds(h * 256, 256)], **at)
    into = Blocks(ain, lambda i: ainf.at[:, aligned(i, 32)], sems.at[1], ains, local.at[3],
                  lambda v, h: v.at[pl.ds(2 * h, 2)], None, **at)
    second = Blocks(bq.at[:, :, aligned(c, 128)], lambda i: bqf.at[:, :, aligned(i, 128)], sems.at[2], bqs, local.at[4],
                    lambda v, h: v.at[:, aligned(h, 64)], None, **at)
    out = Blocks(wo.at[aligned(c, 128)], lambda i: wof.at[aligned(i, 128)], sems.at[3], wos, local.at[5],
                 lambda v, h: v.at[aligned(h, 64)], lambda v, h: v.at[pl.ds(h * 32, 32)], **at)
    a_out = Blocks(ao.at[aligned(c, 128)], lambda i: aof.at[aligned(i, 128)], sems.at[4], aos, local.at[6],
                   lambda v, h: v.at[aligned(h, 64)], None, **at)
    b_out = Blocks(bo, lambda i: bof.at[:, aligned(i, 32)], sems.at[5], bos, local.at[7],
                   lambda v, h: v.at[pl.ds(h, 1)], None, **at)
    x_rows.start()
    for v in (into, second, qkv, b_out, a_out, out):
        v.start()
    g_rows.start()
    x_rows.relay()
    for v in (into, second, qkv, b_out, a_out, out):
        v.store()
    for v in (into, second, qkv, b_out, a_out, out):
        v.relay()
    for v in (into, second, qkv, b_out, a_out, out):
        v.pass_on()
    g_rows.relay()
    for v in (x_rows, into, second, qkv, b_out, a_out, out, g_rows):
        v.finish()


def front(x, g, wq, wo, ain, bq, ao, bo):
    shapes = [(2048, 1024), (2048, 1024), (3, 1024, 512), (512, 1024), (4, 128, 1024), (3, 128, 512), (512, 128),
              (2, 128, 1024)]
    anywhere = pl.BlockSpec(memory_space=pl.ANY)
    return pl.pallas_call(
        front_kernel,
        in_specs=[anywhere] * 8,
        out_specs=[anywhere] * 8,
        out_shape=[jax.ShapeDtypeStruct(s, BF) for s in shapes],
        scratch_shapes=[
            pltpu.SemaphoreType.DMA((2, 16)),
            pltpu.SemaphoreType.DMA((6, 16)),
            pltpu.SemaphoreType.DMA((8, 2)),
            pltpu.VMEM((256, 1024), BF),
            pltpu.VMEM((256, 1024), BF),
            pltpu.VMEM((3, 1024, 128), BF),
            pltpu.VMEM((128, 1024), BF),
            pltpu.VMEM((4, 32, 1024), BF),
            pltpu.VMEM((3, 128, 128), BF),
            pltpu.VMEM((128, 128), BF),
            pltpu.VMEM((2, 32, 1024), BF),
        ],
        compiler_params=pltpu.CompilerParams(collective_id=0, has_side_effects=True),
        name="front",
    )(x, g, wq, wo, ain, bq, ao, bo)


def back_kernel(dl, dp, mq, mu, xf, gf, gain, dbq, dbu, dao, dad, dsh,
                out, obq, obu, oao, oad, osh, ono,
                row_sems, share_sems, cross_sems, z_sems, last_sems, norm_sems, local, weight_sems,
                sh_in, sh, rbq, rbu, rao, rad, rsh, pbq, pbu, pao, pad, psh, qbq, qbu, qao, qad, qsh,
                no_plane, no_z, no_own, no_mid, wq, wu, dlb, dpb, xb, gb, dlt, one, two, std, inv, sends, gets, rows):
    z, c, t = place()
    d = 2 * z + c
    sibling = (2 * z + (c ^ 1), t)

    def first_row(j):
        return (t ^ (j % 4)) * 512 + ((c + 1 + j // 4) % 2) * 256

    def loads(j):
        n = j % 2
        at = pl.ds(pl.multiple_of(first_row(j), 256), 256)
        return [pltpu.make_async_copy(v, w.at[n], local.at[i, n]) for i, (v, w) in enumerate((
            (dl.at[:, :, at], dlb), (dp.at[at], dpb), (xf.at[at], xb), (gf.at[at], gb)))]

    weights = (pltpu.make_async_copy(mq, wq, weight_sems.at[0]), pltpu.make_async_copy(mu, wu, weight_sems.at[1]))
    for v in loads(0):
        v.start()
    for v in weights:
        v.start()
    meet(z, c, t, (1, 2, 3))

    home = t % 2
    local_row = home == c
    slot = (t // 2) * 2 + c

    def row(k):
        return remote(rows.at[k], out.at[t // 2, aligned(c, 256)], row_sems.at[k], row_sems.at[4 + slot],
                      (2 * z + home, t ^ k))

    def own_row():
        return pltpu.make_async_copy(rows.at[0], out.at[t // 2, aligned(c, 256)], row_sems.at[4 + slot])

    def give(k):
        return remote(sends.at[k], gets.at[k], row_sems.at[8 + k], row_sems.at[12 + k], sibling)

    def share():
        return remote(dsh.at[:, :, aligned(c ^ 1, 512)], sh_in, share_sems.at[0], share_sems.at[1], sibling)

    def parts(j):
        return (dbq.at[:, :, aligned(j, 128)], dbu.at[:, aligned(j, 512)], dao.at[aligned(j, 128)],
                dad.at[:, aligned(j, 512)], sh.at[:, aligned(j, 32)])

    got = (rbq, rbu, rao, rad, rsh)

    def cross(k, i):
        return remote(parts(t ^ k)[i], got[i].at[k - 1], cross_sems.at[0, k - 1, i], cross_sems.at[1, k - 1, i], (d, t ^ k))

    sums = (pbq, pbu, pao, pad, psh)
    halves = (qbq, qbu, qao, qad, qsh)
    low = z % 2

    def half(v, i, j):
        if i == 0:
            return v.at[:, aligned(j, 64)]
        if i == 4:
            return v.at[:, aligned(j, 16)]
        return v.at[aligned(j, 64)]

    def along(step, i):
        j = low ^ 1 if step == 0 else low
        dst = sums[i].at[2] if step == 2 else halves[i].at[step]
        return remote(half(sums[i].at[step], i, j), half(dst, i, j), z_sems.at[0, step, i], z_sems.at[1, step, i],
                      (d ^ (4 if step == 1 else 2), t))

    def arrived(step, i):
        j = low ^ 1 if step == 2 else low
        dst = sums[i].at[2] if step == 2 else halves[i].at[step]
        return remote(half(dst, i, j), half(dst, i, j), z_sems.at[0, step, i], z_sems.at[1, step, i], (d, t ^ 1))

    result = (obq.at[:, :, aligned(c, 128)], obu.at[:, aligned(c, 512)], oao.at[aligned(c, 128)],
              oad.at[:, aligned(c, 512)], osh.at[:, :, aligned(c, 512)])
    theirs = (obq.at[:, :, aligned(c ^ 1, 128)], obu.at[:, aligned(c ^ 1, 512)], oao.at[aligned(c ^ 1, 128)],
              oad.at[:, aligned(c ^ 1, 512)], osh.at[:, :, aligned(c ^ 1, 512)])

    def last(i):
        return remote(result[i], result[i], last_sems.at[0, i], last_sems.at[1, i], sibling)

    share().start()
    for v in weights:
        v.wait()
    no_own[...] = jnp.zeros_like(no_own)

    def block(j, carry):
        n, k = j % 2, j % 4
        for v in loads(j):
            v.wait()

        @pl.when(j < 7)
        def _():
            for v in loads(j + 1):
                v.start()

        for i in range(3):
            dlt[i] = jnp.transpose(dlb[n, i])

        def columns(m, carry):
            at = aligned(m, 256)
            one[:, at] = (dot(dlt[0], wq[0, at, :], 1, 1) + dot(dlt[1], wq[1, at, :], 1, 1)
                          + dot(dlt[2], wq[2, at, :], 1, 1))
            two[:, at] = dot(dpb[n], wu[at, :], 1, 1)
            return carry

        lax.fori_loop(0, 4, columns, 0)

        def norms(r, carry):
            at = aligned(r, 32)
            v = xb[n, at, :].astype(F32)
            v = v - jnp.mean(v, axis=1, keepdims=True)
            inverse = lax.rsqrt(jnp.mean(v * v, axis=1, keepdims=True) + EPSILON)
            v = v * inverse
            a, b = one[at, :], two[at, :]
            for i, w in enumerate((a * v, b * v, a, b)):
                no_own[i] += jnp.sum(w.reshape(4, 8, 1024), axis=0)
            one[at, :] = gain[0:1, :] * a + gain[1:2, :] * b
            std[at, :] = v
            inv[at, :] = inverse
            return carry

        lax.fori_loop(0, 8, norms, 0)

        @pl.when(j < 4)
        def _():
            sends[k] = one[...].astype(BF)
            give(k).start()

        @pl.when(j >= 4)
        def _():
            give(k).wait_recv()

            def finish(r, carry):
                at = aligned(r, 32)
                v, own = one[at, :] + gets[k, at, :].astype(F32), std[at, :]
                v = v - jnp.mean(v, axis=1, keepdims=True) - own * jnp.mean(v * own, axis=1, keepdims=True)
                rows[k, at, :] = (gb[n, at, :].astype(F32) + v * inv[at, :]).astype(BF)
                return carry

            lax.fori_loop(0, 8, finish, 0)
            here = (k == 0) & local_row

            @pl.when(here)
            def _():
                own_row().start()

            @pl.when(jnp.logical_not(here))
            def _():
                row(k).start()

        @pl.when(j == 0)
        def _():
            share().wait_recv()
            for i in range(6):
                sh[i] = (dsh[i, :, aligned(c, 512)].astype(F32) + sh_in[i].astype(F32)).astype(BF)
            for i in range(5):
                for p in (1, 2, 3):
                    cross(p, i).start()

        @pl.when(j == 3)
        def _():
            for i in range(5):
                for p in (1, 2, 3):
                    cross(p, i).wait_recv()
                total = parts(t)[i][...].astype(F32)
                for p in (0, 1, 2):
                    total = total + got[i][p].astype(F32)
                sums[i][0] = total.astype(BF)
                along(0, i).start()

        for step, when in ((0, 4), (1, 6)):
            @pl.when(j == when)
            def _():
                for i in range(5):
                    arrived(step, i).wait_recv()
                    mine, other = half(sums[i].at[step], i, low), half(halves[i].at[step], i, low)
                    half(sums[i].at[step + 1], i, low)[...] = (mine[...].astype(F32) + other[...].astype(F32)).astype(BF)
                    along(step + 1, i).start()

        return carry

    lax.fori_loop(0, 8, block, 0)

    plane = [(h, k) for h in (0, 1) for k in range(4) if h or k]

    def norm(n):
        h, k = plane[n]
        return remote(no_mid.at[0], no_plane.at[2 * t + c], norm_sems.at[0, n], norm_sems.at[1, n], (2 * z + (c ^ h), t ^ k))

    def norm_from(n):
        h, k = plane[n]
        spot = no_plane.at[2 * (t ^ k) + (c ^ h)]
        return remote(spot, spot, norm_sems.at[0, n], norm_sems.at[1, n], sibling)

    def norm_z(k):
        return remote(no_mid.at[1], no_z.at[z], norm_sems.at[0, 6 + k], norm_sems.at[1, 6 + k], (d ^ (2 * k), t))

    def norm_z_from(k):
        return remote(no_z.at[z ^ k], no_z.at[z ^ k], norm_sems.at[0, 6 + k], norm_sems.at[1, 6 + k], sibling)

    own = jnp.sum(no_own[...], axis=1)
    no_mid[0] = own
    for n in range(7):
        norm(n).start()
    no_plane[2 * t + c] = own
    for i in range(5):
        arrived(2, i).wait_recv()
        result[i][...] = sums[i][2].astype(F32)
        last(i).start()
    for n in range(7):
        norm_from(n).wait_recv()
    own = no_plane[0]
    for n in range(1, 8):
        own = own + no_plane[n]
    no_mid[1] = own
    for k in (1, 2, 3):
        norm_z(k).start()
    no_z[z] = own
    for i in range(5):
        remote(theirs[i], theirs[i], last_sems.at[0, i], last_sems.at[1, i], sibling).wait_recv()
        last(i).wait_send()
        for step in (0, 1, 2):
            along(step, i).wait_send()
        for k in (1, 2, 3):
            cross(k, i).wait_send()
    share().wait_send()
    for k in (1, 2, 3):
        norm_z_from(k).wait_recv()
    ono[...] = ((no_z[0] + no_z[1]) + no_z[2]) + no_z[3]
    for n in range(7):
        norm(n).wait_send()
    for k in (1, 2, 3):
        norm_z(k).wait_send()
        row(k).wait_send()
    for k in range(4):
        give(k).wait_send()

    @pl.when(jnp.logical_not(local_row))
    def _():
        row(0).wait_send()

    for m in (0, 1):
        for h in (0, 1):
            pltpu.make_async_copy(rows.at[0], out.at[m, pl.ds(256 * h, 256)], row_sems.at[4 + 2 * m + h]).wait()


def back(dl, dp, mq, mu, xf, gf, gain, dbq, dbu, dao, dad, dsh):
    vmem = pl.BlockSpec(memory_space=pltpu.VMEM)
    anywhere = pl.BlockSpec(memory_space=pl.ANY)
    part = [(3, 128, 128), (128, 512), (128, 128), (128, 512), (6, 32, 512)]
    outs = [((2, 512, 1024), BF), ((3, 128, 256), F32), ((128, 1024), F32), ((256, 128), F32), ((128, 1024), F32),
            ((6, 32, 1024), F32), ((4, 1024), F32)]
    return pl.pallas_call(
        back_kernel,
        in_specs=[anywhere] * 6 + [vmem] * 6,
        out_specs=[anywhere] + [vmem] * 6,
        out_shape=[jax.ShapeDtypeStruct(s, d) for s, d in outs],
        scratch_shapes=[
            pltpu.SemaphoreType.DMA((16,)),
            pltpu.SemaphoreType.DMA((2,)),
            pltpu.SemaphoreType.DMA((2, 3, 5)),
            pltpu.SemaphoreType.DMA((2, 3, 5)),
            pltpu.SemaphoreType.DMA((2, 5)),
            pltpu.SemaphoreType.DMA((2, 10)),
            pltpu.SemaphoreType.DMA((4, 2)),
            pltpu.SemaphoreType.DMA((2,)),
            pltpu.VMEM((6, 128, 512), BF),
            pltpu.VMEM((6, 128, 512), BF),
        ] + [pltpu.VMEM((3,) + s, BF) for s in part + part] + [pltpu.VMEM((2,) + s, BF) for s in part] + [
            pltpu.VMEM((8, 4, 1024), F32),
            pltpu.VMEM((4, 4, 1024), F32),
            pltpu.VMEM((4, 8, 1024), F32),
            pltpu.VMEM((2, 4, 1024), F32),
            pltpu.VMEM((3, 1024, 512), BF),
            pltpu.VMEM((1024, 2048), BF),
            pltpu.VMEM((2, 3, 512, 256), BF),
            pltpu.VMEM((2, 256, 2048), BF),
            pltpu.VMEM((2, 256, 1024), BF),
            pltpu.VMEM((2, 256, 1024), BF),
            pltpu.VMEM((3, 256, 512), BF),
            pltpu.VMEM((256, 1024), F32),
            pltpu.VMEM((256, 1024), F32),
            pltpu.VMEM((256, 1024), F32),
            pltpu.VMEM((256, 1), F32),
            pltpu.VMEM((4, 256, 1024), BF),
            pltpu.VMEM((4, 256, 1024), BF),
            pltpu.VMEM((4, 256, 1024), BF),
        ],
        compiler_params=pltpu.CompilerParams(collective_id=1, has_side_effects=True, vmem_limit_bytes=56 << 20),
        name="back",
    )(dl, dp, mq, mu, xf, gf, gain, dbq, dbu, dao, dad, dsh)


def swap(v, k=1):
    return lax.ppermute(v, "dp", [(i, i ^ k) for i in range(lax.axis_size("dp"))])


def pick(v, axis, index, size):
    return lax.dynamic_slice_in_dim(v, index * size, size, axis)


def half_rows(v, c):
    return pick(v.reshape(4, 2, 256, -1), 1, c, 1)[:, 0]


def from_group(own, c):
    got = lax.all_to_all(own, "tensor", 0, 0, tiled=True).reshape(2, 2, 256, -1)
    mine = pick(got, 1, c, 1)[:, 0]
    other = swap(pick(got, 1, 1 - c, 1)[:, 0])
    return jnp.where(c == 0, jnp.stack([mine, other], 1), jnp.stack([other, mine], 1)).reshape(2, 512, -1)


def by_groups(x, gy, segment, keep, gain, bias, w_qkv, w_out, w_up, w_down,
              a_in, b_qkv, b_up, a_out, a_down, b_out):
    z, c, t = place()
    tables = jnp.stack([segment[:, 0], keep[:, 0]], 1)
    pair = jnp.where(t % 2 == c, tables, swap(tables))
    seg, kept = jnp.where(t // 2 == 0, pair[0], pair[1])

    x_full, g_full, qkv, out, a_full, b_qkv_all, a_out_all, b_full = front(
        x[:, 0], gy[:, 0], w_qkv, w_out, jnp.swapaxes(a_in, 1, 2), b_qkv, a_out, b_out)
    up, down = lax.optimization_barrier((
        jnp.concatenate([pick(w_up, 1, c, 512), pick(b_up, 1, c, 512)], axis=0),
        jnp.concatenate([pick(w_down, 0, c, 512), pick(a_down, 0, c, 512)], axis=1), x_full))[:2]
    up = lax.all_gather(up, "tensor", axis=0)
    down = lax.all_gather(down, "tensor", axis=0, tiled=True)
    w_up_all = jnp.concatenate([up[i, :1024] for i in range(4)], axis=1)
    b_up_all = jnp.concatenate([up[i, 1024:] for i in range(4)], axis=1)
    w_down_all, a_down_all = down[:, :1024], down[:, 1024:]

    m_qkv = (qkv.astype(F32) + SCALE * jnp.einsum("nrk,nrc->nkc", a_full[:3], b_qkv_all,
                                                  preferred_element_type=F32)).astype(BF)
    m_up = (w_up_all.astype(F32) + SCALE * dot(a_full[3], b_up_all, 0, 0)).astype(BF)
    m_out = (out.astype(F32) + SCALE * dot(a_out_all, b_full[0], 1, 0)).astype(BF)
    m_down = (w_down_all.astype(F32) + SCALE * dot(a_down_all, b_full[1], 1, 0)).astype(BF)
    a_three = a_full[:3].reshape(3 * RANK, 1024)
    b_both = b_full.reshape(2 * RANK, 1024)

    standard, _ = normalized(x_full.astype(F32))
    n1 = (standard * gain[0] + bias[0]).astype(BF)
    n2 = (standard * gain[1] + bias[1]).astype(BF)
    lin = jnp.einsum("nkc,sk->ncs", m_qkv, n1, preferred_element_type=F32)
    low3 = dot(a_three, n1, 1, 1).astype(BF).reshape(3, RANK, 2048)
    low1 = dot(a_full[3], n2, 1, 1).astype(BF)
    g_ctx = dot(m_out, g_full, 1, 1).astype(BF)
    low_grad = (SCALE * dot(b_both, g_full, 1, 1)).astype(BF)
    cos, sin = rotary_tables(seg)
    ctx, d_lin = attention(lin, g_ctx, cos, sin, seg, kept)

    pre = dot(n2, m_up, 1, 0)
    cdf = 0.5 * (1.0 + lax.erf(pre * math.sqrt(0.5)))
    hidden = (pre * cdf).astype(BF)
    slope = cdf + pre * (math.sqrt(0.5 / math.pi) * jnp.exp(-0.5 * pre * pre))
    d_pre = (dot(g_full, m_down, 1, 1) * slope).astype(BF)

    part = dot(ctx, m_out, 0, 0) + dot(hidden, m_down, 1, 0)
    theirs = swap(half_rows(part, 1 - c).astype(BF))
    y = half_rows(x_full, c).astype(F32) + half_rows(part, c) + theirs.astype(F32)
    y = from_group(y.astype(BF), c)

    lo = jnp.concatenate([dot(a_out_all, ctx, 0, 0), dot(a_down_all, hidden, 0, 1)], axis=0).astype(BF)
    d_a_out = dot(ctx, low_grad[:RANK], 1, 1).astype(BF)
    d_a_down = dot(low_grad[RANK:], hidden, 1, 0).astype(BF)
    d_b_qkv = (SCALE * jnp.einsum("nrs,ncs->nrc", low3, d_lin, preferred_element_type=F32)).astype(BF)
    d_b_up = (SCALE * dot(low1, d_pre, 1, 0)).astype(BF)
    back3 = (SCALE * jnp.einsum("nrc,ncs->nrs", b_qkv_all, d_lin, preferred_element_type=F32)).astype(BF)
    back1 = (SCALE * dot(b_up_all, d_pre, 1, 1)).astype(BF)
    shared = jnp.concatenate([dot(back3.reshape(3 * RANK, 2048), n1, 1, 0).astype(BF), dot(back1, n2, 1, 0).astype(BF),
                              (SCALE * dot(lo, g_full, 1, 0)).astype(BF)], axis=0).reshape(6, RANK, 1024)
    grad, r_b_qkv, r_b_up, r_a_out, r_a_down, rest, norms = back(
        d_lin, d_pre, m_qkv, m_up, x_full, g_full, gain, d_b_qkv, d_b_up, d_a_out, d_a_down, shared)
    r_a_in = jnp.swapaxes(rest[:4], 1, 2)
    return (y[:, None], grad[:, None], norms[:2], norms[2:], r_a_in, r_b_qkv, r_b_up, r_a_out, jnp.transpose(r_a_down), rest[4:])


def solution(mesh):
    in_specs = (
        P(None, "dp", "tensor", None),
        P(None, "dp", "tensor", None),
        P(None, "dp", None),
        P(None, "dp", None),
        P(),
        P(),
        P(None, None, "tensor"),
        P("tensor", None),
        P(None, "tensor"),
        P("tensor", None),
        P(None, None, "tensor"),
        P(None, None, "tensor"),
        P(None, "tensor"),
        P("tensor", None),
        P("tensor", None),
        P(None, "tensor", None),
    )
    out_specs = (
        P(None, "dp", "tensor", None),
        P(None, "dp", "tensor", None),
        P(),
        P(),
        P(None, None, "tensor"),
        P(None, None, "tensor"),
        P(None, "tensor"),
        P("tensor", None),
        P("tensor", None),
        P(None, "tensor", None),
    )
    small = mesh.shape["tensor"] == 4 and mesh.shape["dp"] == 8
    return jax.shard_map(
        by_groups if small else by_features, mesh=mesh, in_specs=in_specs, out_specs=out_specs, check_vma=False
    )
```

```python
import functools
import math

import jax
import jax.numpy as jnp
from jax import lax
from jax.experimental import pallas as pl
from jax.experimental.pallas import tpu as pltpu
from jax.sharding import PartitionSpec as P

HEAD = 64
HALF = 8
N_DOCS = 5
TILE = 256
SLOTS = 5
EPSILON = 1e-05
SCALE = 0.25
F32 = jnp.float32
BF = jnp.bfloat16


def dot(a, b, ca, cb):
    return lax.dot_general(a, b, (((ca,), (cb,)), ((), ())), preferred_element_type=F32)


def attention_kernel(heads, lo_ref, lin_ref, g_ref, cos_ref, sin_ref, segq_ref, segk_ref,
                     ctx_ref, dlin_ref, qt, kt, vt, kn, vn, acc, s_scr, e_scr, p_scr, row):
    length = lin_ref.shape[2]
    blocks = length // TILE

    def rotate(z, cos, sin):
        a, b = z[:HALF], z[HALF:2 * HALF]
        return jnp.concatenate([a * cos - b * sin, b * cos + a * sin, z[2 * HALF:]], axis=0)

    def prepare(c, carry):
        cols = pl.ds(pl.multiple_of(c * TILE, TILE), TILE)
        cos, sin = cos_ref[:, cols], sin_ref[:, cols]
        for h in range(heads):
            rows = pl.ds(h * HEAD, HEAD)
            q = rotate(lin_ref[0, pl.ds(h * HEAD, HEAD), cols], cos, sin).astype(BF).astype(F32) * 0.125
            k = rotate(lin_ref[1, pl.ds(h * HEAD, HEAD), cols], cos, sin)
            v = lin_ref[2, pl.ds(h * HEAD, HEAD), cols]
            qt[rows, cols] = q.astype(BF)
            kt[rows, cols] = k.astype(BF)
            vt[rows, cols] = v.astype(BF)
            kn[h, cols, :] = jnp.transpose(k).astype(BF)
            vn[h, cols, :] = jnp.transpose(v).astype(BF)
            acc[h, :, cols] = jnp.zeros((2 * HEAD, TILE), F32)
        return carry

    lax.fori_loop(0, blocks, prepare, 0)

    def query_block(qb, carry):
        lo = lo_ref[qb]
        qcols = pl.ds(pl.multiple_of(qb * TILE, TILE), TILE)
        segq = segq_ref[:, qcols]

        def scores(kb, tops, last=False):
            krows = pl.ds(pl.multiple_of(kb * TILE, TILE), TILE)
            allowed = segk_ref[krows, :] == segq
            if last:
                k, q = (lax.broadcasted_iota(jnp.int32, (TILE, TILE), i) for i in (0, 1))
                allowed = (allowed & (k < q)) | (k == q)
            out = []
            for h in range(heads):
                rows = pl.ds(h * HEAD, HEAD)
                s = dot(kn[h, krows, :], qt[rows, qcols], 1, 0)
                s = jnp.where(allowed, s, -1e30)
                s_scr[h, kb - lo] = s
                p_scr[h, kb - lo] = dot(vn[h, krows, :], g_ref[rows, qcols], 1, 0)
                out.append(jnp.maximum(tops[h], jnp.max(s, axis=0, keepdims=True)))
            return tuple(out)

        tops = lax.fori_loop(lo, qb, scores, tuple(jnp.full((1, TILE), -1e30, F32) for _ in range(heads)))
        tops = scores(qb, tops, True)

        def weights(kb, sums):
            kcols = pl.ds(pl.multiple_of(kb * TILE, TILE), TILE)
            out = []
            for h in range(heads):
                e = jnp.exp(s_scr[h, kb - lo] - tops[h])
                low = e.astype(BF)
                e_scr[h, kb - lo] = low
                out.append(sums[h] + jnp.sum(e, axis=0, keepdims=True))
                row[h] += dot(vt[pl.ds(h * HEAD, HEAD), kcols], low, 1, 0)
            return tuple(out)

        row[...] = jnp.zeros_like(row)
        sums = lax.fori_loop(lo, qb + 1, weights, tuple(jnp.zeros((1, TILE), F32) for _ in range(heads)))
        gts, terms, scales = [], [], []
        for h in range(heads):
            rows = pl.ds(h * HEAD, HEAD)
            inverse = 1.0 / sums[h]
            ctx = row[h] * inverse
            ctx_ref[rows, qcols] = ctx.astype(BF)
            g = g_ref[rows, qcols].astype(F32)
            terms.append(jnp.sum(g * ctx, axis=0, keepdims=True))
            scales.append(inverse)
            gts.append((g * inverse).astype(BF))

        row[...] = jnp.zeros_like(row)

        def backward(kb, carry):
            krows = pl.ds(pl.multiple_of(kb * TILE, TILE), TILE)
            for h in range(heads):
                low = e_scr[h, kb - lo]
                ds = (low.astype(F32) * ((p_scr[h, kb - lo] - terms[h]) * scales[h])).astype(BF)
                acc[h, :HEAD, krows] += dot(gts[h], low, 1, 1)
                acc[h, HEAD:, krows] += dot(qt[pl.ds(h * HEAD, HEAD), qcols], ds, 1, 1)
                row[h] += dot(kt[pl.ds(h * HEAD, HEAD), krows], ds, 1, 0)
            return carry

        lax.fori_loop(lo, qb + 1, backward, 0)
        cos, sin = cos_ref[:, qcols], sin_ref[:, qcols]
        for h in range(heads):
            dlin_ref[0, pl.ds(h * HEAD, HEAD), qcols] = rotate(row[h] * 0.125, cos, -sin).astype(BF)
        return carry

    lax.fori_loop(0, blocks, query_block, 0)

    def finish(c, carry):
        cols = pl.ds(pl.multiple_of(c * TILE, TILE), TILE)
        cos, sin = cos_ref[:, cols], sin_ref[:, cols]
        for h in range(heads):
            both = acc[h, :, cols]
            dlin_ref[1, pl.ds(h * HEAD, HEAD), cols] = rotate(both[HEAD:], cos, -sin).astype(BF)
            dlin_ref[2, pl.ds(h * HEAD, HEAD), cols] = both[:HEAD].astype(BF)
        return carry

    lax.fori_loop(0, blocks, finish, 0)


def attention(lin, g, cos, sin, segment, keep):
    width, length = g.shape
    heads = min(4, width // HEAD)
    wide = heads * HEAD
    starts = jnp.sum(segment[None, :] < jnp.arange(N_DOCS, dtype=jnp.int32)[:, None], axis=1)
    firsts = segment[::TILE]
    lo = jnp.sum(jnp.where(firsts[:, None] == jnp.arange(N_DOCS)[None, :], starts[None, :], 0), axis=1)
    lo = (lo // TILE).astype(jnp.int32)
    segk = jnp.where(keep == 1, segment, -1)[:, None]
    vmem = pl.BlockSpec(memory_space=pltpu.VMEM)
    three = pl.BlockSpec((3, wide, length), lambda i, lo: (0, i, 0))
    single = pl.BlockSpec((wide, length), lambda i, lo: (i, 0))
    return pl.pallas_call(
        functools.partial(attention_kernel, heads),
        grid_spec=pltpu.PrefetchScalarGridSpec(
            num_scalar_prefetch=1,
            grid=(width // wide,),
            in_specs=[three, single] + [vmem] * 4,
            out_specs=[single, three],
            scratch_shapes=[
                pltpu.VMEM((wide, length), BF),
                pltpu.VMEM((wide, length), BF),
                pltpu.VMEM((wide, length), BF),
                pltpu.VMEM((heads, length, HEAD), BF),
                pltpu.VMEM((heads, length, HEAD), BF),
                pltpu.VMEM((heads, 2 * HEAD, length), F32),
                pltpu.VMEM((heads, SLOTS, TILE, TILE), F32),
                pltpu.VMEM((heads, SLOTS, TILE, TILE), BF),
                pltpu.VMEM((heads, SLOTS, TILE, TILE), F32),
                pltpu.VMEM((heads, HEAD, TILE), F32),
            ]),
        out_shape=[jax.ShapeDtypeStruct((width, length), BF), jax.ShapeDtypeStruct((3, width, length), BF)],
        compiler_params=pltpu.CompilerParams(vmem_limit_bytes=60 << 20),
        name="attention",
        cost_estimate=pl.CostEstimate(flops=10 * width * length * 768, transcendentals=width * length * 12,
                                      bytes_accessed=26 * width * length),
    )(lo, lin, g, cos, sin, segment[None, :], segk)


def rotary_tables(segment):
    length = segment.shape[0]
    starts = jnp.sum(segment[None, :] < jnp.arange(N_DOCS, dtype=jnp.int32)[:, None], axis=1)
    begin = jnp.sum(jnp.where(segment[None, :] == jnp.arange(N_DOCS)[:, None], starts[:, None], 0), axis=0)
    position = (jnp.arange(length, dtype=jnp.int32) - begin).astype(F32)
    exponent = jnp.arange(HALF, dtype=F32) / HALF
    frequency = jnp.exp(-math.log(10000.0) * exponent)
    angles = frequency[:, None] * position[None, :]
    return jnp.cos(angles), jnp.sin(angles)


def normalized(values):
    average = jnp.mean(values, axis=-1, keepdims=True)
    centered = values - average
    variance = jnp.mean(centered * centered, axis=-1, keepdims=True)
    inverse = lax.rsqrt(variance + EPSILON)
    return centered * inverse, inverse


def by_features(x, gy, segment, keep, gain, bias, w_qkv, w_out, w_up, w_down,
              a_in, b_qkv, b_up, a_out, a_down, b_out):
    width = w_qkv.shape[2]
    micro = x.shape[0]
    a_full = lax.all_gather(a_in, "tensor", axis=2, tiled=True)
    b_full = lax.all_gather(b_out, "tensor", axis=1, tiled=True)

    m_qkv = jnp.concatenate([
        (w_qkv[i].astype(F32) + SCALE * dot(a_full[i], b_qkv[i], 1, 0)).astype(BF) for i in range(3)
    ], axis=1)
    m_up = (w_up.astype(F32) + SCALE * dot(a_full[3], b_up, 1, 0)).astype(BF)
    m_out = (w_out.astype(F32) + SCALE * dot(a_out, b_full[0], 1, 0)).astype(BF)
    m_down = (w_down.astype(F32) + SCALE * dot(a_down, b_full[1], 1, 0)).astype(BF)
    a_three = jnp.concatenate([a_full[0], a_full[1], a_full[2]], axis=1)
    b_both = jnp.concatenate([b_full[0], b_full[1]], axis=0)

    outs, grads, sums = [], [], None
    for m in range(micro):
        rows, seg = x[m, 0], segment[m, 0]
        xg = lax.all_gather(rows, "tensor", axis=0, tiled=True)
        gg = lax.all_gather(gy[m, 0], "tensor", axis=0, tiled=True)
        standard, _ = normalized(xg.astype(F32))
        n1 = (standard * gain[0] + bias[0]).astype(BF)
        n2 = (standard * gain[1] + bias[1]).astype(BF)
        lin = dot(m_qkv, n1, 0, 1)
        low3 = dot(n1, a_three, 1, 0).astype(BF)
        low1 = dot(n2, a_full[3], 1, 0).astype(BF)
        g_ctx = dot(m_out, gg, 1, 1).astype(BF)
        low_grad = (SCALE * dot(gg, b_both, 1, 1)).astype(BF)
        cos, sin = rotary_tables(seg)
        ctx, d_lin = attention(lin.reshape(3, width, -1), g_ctx, cos, sin, seg, keep[m, 0])
        d_lin = d_lin.reshape(3 * width, -1)

        pre = dot(n2, m_up, 1, 0)
        cdf = 0.5 * (1.0 + lax.erf(pre * math.sqrt(0.5)))
        hidden = (pre * cdf).astype(BF)
        slope = cdf + pre * (math.sqrt(0.5 / math.pi) * jnp.exp(-0.5 * pre * pre))
        d_pre = (dot(gg, m_down, 1, 1) * slope).astype(BF)

        part = dot(ctx, m_out, 0, 0) + dot(hidden, m_down, 1, 0)
        branch = lax.psum_scatter(part.astype(BF), "tensor", scatter_dimension=0, tiled=True)
        outs.append((rows.astype(F32) + branch.astype(F32)).astype(BF))

        one = dot(d_lin, m_qkv, 0, 1)
        two = dot(d_pre, m_up, 1, 1)
        total = (gain[0] * one + gain[1] * two).astype(BF)
        total = lax.psum_scatter(total, "tensor", scatter_dimension=0, tiled=True).astype(F32)
        own, inverse = normalized(rows.astype(F32))
        grad = total - jnp.mean(total, axis=-1, keepdims=True)
        grad = grad - own * jnp.mean(total * own, axis=-1, keepdims=True)
        grads.append((gy[m, 0].astype(F32) + grad * inverse).astype(BF))

        norms = jnp.stack([jnp.sum(one * standard, axis=0), jnp.sum(two * standard, axis=0),
                           jnp.sum(one, axis=0), jnp.sum(two, axis=0)])
        lo_ctx = dot(ctx, a_out, 0, 0).astype(BF)
        lo_hid = dot(hidden, a_down, 1, 0).astype(BF)
        d_b_out = SCALE * jnp.stack([dot(lo_ctx, gg, 0, 0), dot(lo_hid, gg, 0, 0)], axis=1)
        d_a_out = dot(ctx, low_grad[:, :128], 1, 0)
        d_a_down = dot(hidden, low_grad[:, 128:], 0, 0)
        d_b_qkv = SCALE * jnp.stack([
            dot(low3[:, 128 * i:128 * (i + 1)], d_lin[width * i:width * (i + 1)], 0, 1) for i in range(3)])
        d_b_up = SCALE * dot(low1, d_pre, 0, 0)
        back = [(SCALE * dot(d_lin[width * i:width * (i + 1)], b_qkv[i], 0, 1)).astype(BF) for i in range(3)]
        back.append((SCALE * dot(d_pre, b_up, 1, 1)).astype(BF))
        d_a_in = jnp.stack([dot(back[i], n1 if i < 3 else n2, 0, 0) for i in range(4)], axis=1)
        terms = (d_a_in, d_b_qkv, d_b_up, d_a_out, d_a_down, d_b_out, norms)
        sums = terms if sums is None else tuple(p + q for p, q in zip(sums, terms))

    d_a_in, d_b_qkv, d_b_up, d_a_out, d_a_down, d_b_out, norms = sums
    d_a_in = lax.psum_scatter(d_a_in, "tensor", scatter_dimension=0, tiled=True)
    d_b_out = lax.psum_scatter(d_b_out, "tensor", scatter_dimension=0, tiled=True)
    d_a_in, d_b_qkv, d_b_up, d_a_out, d_a_down, d_b_out = lax.psum(
        (d_a_in, d_b_qkv, d_b_up, d_a_out, d_a_down, d_b_out), "dp")
    norms = lax.psum(norms, ("dp", "tensor"))
    return (jnp.stack(outs)[:, None], jnp.stack(grads)[:, None], norms[:2], norms[2:],
            jnp.transpose(d_a_in, (1, 2, 0)), d_b_qkv, d_b_up, d_a_out, d_a_down,
            jnp.transpose(d_b_out, (1, 0, 2)))


RANK = 128


MESH = pl.DeviceIdType.MESH


def place():
    d = lax.axis_index("dp")
    return d // 2, d % 2, lax.axis_index("tensor")


def meet(z, c, t, planes):
    barrier = pltpu.get_barrier_semaphore()
    for h in (0, 1):
        for k in range(4):
            if h or k:
                pl.semaphore_signal(barrier, 1, device_id=(2 * z + (c ^ h), t ^ k), device_id_type=MESH)
    for k in planes:
        pl.semaphore_signal(barrier, 1, device_id=(2 * (z ^ k) + c, t), device_id_type=MESH)
    pl.semaphore_wait(barrier, 7 + len(planes))


def remote(src, dst, send_sem, recv_sem, device):
    return pltpu.make_async_remote_copy(src_ref=src, dst_ref=dst, send_sem=send_sem, recv_sem=recv_sem,
                                        device_id=device, device_id_type=MESH)


class Rows:
    def __init__(self, v, full, sems, stage, local, z, c, t):
        self.v, self.full, self.sems, self.stage, self.local = v, full, sems, stage, local
        self.z, self.c, self.t = z, c, t

    def rows(self, s, h):
        return self.full.at[pl.ds(pl.multiple_of(s * 512 + h * 256, 256), 256)]

    def block(self, m, h):
        return self.v.at[m, pl.ds(pl.multiple_of(h * 256, 256), 256)]

    def copy(self, m, other):
        h = self.c ^ other
        return remote(self.block(m, h), self.rows(self.t, h), self.sems.at[2 * m + other], self.sems.at[4 + self.t],
                      (2 * self.z + h, 2 * m + self.c))

    def forward(self, s):
        part = self.rows(s, self.c)
        return remote(part, part, self.sems.at[8 + s], self.sems.at[12 + s], (2 * self.z + (self.c ^ 1), self.t))

    def start(self):
        for m in (0, 1):
            away = 2 * m + self.c != self.t

            @pl.when(away)
            def _():
                self.copy(m, 0).start()

            self.copy(m, 1).start()

            @pl.when(jnp.logical_not(away))
            def _():
                pltpu.make_async_copy(self.block(m, self.c), self.stage, self.local.at[0]).start()

    def relay(self):
        mine = self.t % 2 == self.c

        @pl.when(mine)
        def _():
            pltpu.make_async_copy(self.block(0, self.c), self.stage, self.local.at[0]).wait()
            pltpu.make_async_copy(self.stage, self.rows(self.t, self.c), self.sems.at[4 + self.t]).start()

        for k in (0, 1, 2, 3):
            s = self.t ^ k
            pltpu.make_async_copy(self.stage, self.rows(s, self.c), self.sems.at[4 + s]).wait()
            self.forward(s).start()

    def finish(self):
        for s in range(4):
            part = self.rows(s, self.c ^ 1)
            remote(part, part, self.sems.at[8 + s], self.sems.at[12 + s], (2 * self.z + (self.c ^ 1), self.t)).wait_recv()
            self.forward(s).wait_send()
        for m in (0, 1):
            @pl.when(2 * m + self.c != self.t)
            def _():
                self.copy(m, 0).wait_send()

            self.copy(m, 1).wait_send()


class Blocks:
    def __init__(self, own, where, sems, stage, local, cut, quarter, z, c, t):
        self.own, self.where, self.sems, self.stage, self.local = own, where, sems, stage, local
        self.cut, self.quarter, self.t, self.d, self.half = cut, quarter, t, 2 * z + c, z % 2

    def spot(self, k, other=0):
        return self.cut(self.where(self.t ^ k), self.half ^ other)

    def first(self, k):
        return remote(self.cut(self.own, self.half), self.spot(0), self.sems.at[k - 1], self.sems.at[2 + k],
                      (self.d, self.t ^ k))

    def arrival(self, k):
        return remote(self.spot(k), self.spot(k), self.sems.at[k - 1], self.sems.at[2 + k], (self.d, self.t ^ k))

    def second(self, k):
        part = self.quarter(self.spot(3 - k), k - 1)
        return remote(part, part, self.sems.at[5 + k], self.sems.at[7 + k], (self.d, self.t ^ k))

    def last(self, k):
        part = self.quarter(self.spot(3), k - 1)
        return remote(part, part, self.sems.at[5 + k], self.sems.at[7 + k], (self.d, self.t ^ k))

    def across(self, k, other=0):
        return remote(self.spot(k, other), self.spot(k, other), self.sems.at[9 + k], self.sems.at[12 + k],
                      (self.d ^ 2, self.t))

    def start(self):
        for k in ((1, 2) if self.quarter else (1, 2, 3)):
            self.first(k).start()
        pltpu.make_async_copy(self.own, self.stage, self.local.at[0]).start()

    def store(self):
        pltpu.make_async_copy(self.own, self.stage, self.local.at[0]).wait()
        pltpu.make_async_copy(self.stage, self.where(self.t), self.local.at[1]).start()

    def relay(self):
        for k in (1, 2):
            self.arrival(3 - k).wait_recv()
            if self.quarter:
                self.second(k).start()
            self.across(3 - k).start()

    def pass_on(self):
        if self.quarter:
            for k in (1, 2):
                self.last(k).wait_recv()
        else:
            self.arrival(3).wait_recv()
        self.across(3).start()

    def finish(self):
        pltpu.make_async_copy(self.stage, self.where(self.t), self.local.at[1]).wait()
        for k in (1, 2, 3):
            self.across(k, 1).wait_recv()
            self.across(k).wait_send()
            if k < 3 or not self.quarter:
                self.first(k).wait_send()
            if k < 3 and self.quarter:
                self.second(k).wait_send()


def aligned(i, n):
    return pl.ds(pl.multiple_of(i * n, n), n)


def front_kernel(x, g, wq, wo, ain, bq, ao, bo, gain, bias,
                 xf, gf, wqf, wof, ainf, bqf, aof, bof, n1, n2, mq, lin, low3, low1,
                 row_sems, sems, local, xs, gs, wqs, wos, ains, bqs, aos, bos,
                 block_sems, work_sems, xb, n1s, n2s, wv, av, bv, mt, stage):
    z, c, t = place()
    meet(z, c, t, (1,))
    at = dict(z=z, c=c, t=t)
    x_rows = Rows(x, xf, row_sems.at[0], xs, local.at[0], **at)
    g_rows = Rows(g, gf, row_sems.at[1], gs, local.at[1], **at)
    qkv = Blocks(wq.at[:, :, aligned(c, 128)], lambda i: wqf.at[:, :, aligned(i, 128)], sems.at[0], wqs, local.at[2],
                 lambda v, h: v.at[:, aligned(h, 512)], lambda v, h: v.at[:, pl.ds(h * 256, 256)], **at)
    into = Blocks(ain, lambda i: ainf.at[:, aligned(i, 32)], sems.at[1], ains, local.at[3],
                  lambda v, h: v.at[pl.ds(2 * h, 2)], None, **at)
    second = Blocks(bq.at[:, :, aligned(c, 128)], lambda i: bqf.at[:, :, aligned(i, 128)], sems.at[2], bqs, local.at[4],
                    lambda v, h: v.at[:, aligned(h, 64)], None, **at)
    out = Blocks(wo.at[aligned(c, 128)], lambda i: wof.at[aligned(i, 128)], sems.at[3], wos, local.at[5],
                 lambda v, h: v.at[aligned(h, 64)], lambda v, h: v.at[pl.ds(h * 32, 32)], **at)
    a_out = Blocks(ao.at[aligned(c, 128)], lambda i: aof.at[aligned(i, 128)], sems.at[4], aos, local.at[6],
                   lambda v, h: v.at[aligned(h, 64)], None, **at)
    b_out = Blocks(bo, lambda i: bof.at[:, aligned(i, 32)], sems.at[5], bos, local.at[7],
                   lambda v, h: v.at[pl.ds(h, 1)], None, **at)
    blocks = (into, second, qkv, b_out, a_out, out)
    x_rows.start()
    for v in blocks:
        v.start()
    x_rows.relay()
    g_rows.start()
    for v in blocks:
        v.store()
    for v in blocks:
        v.relay()
    x_rows.finish()

    def load(j):
        return pltpu.make_async_copy(xf.at[aligned(j, 256)], xb.at[j % 2], block_sems.at[j % 2])

    load(0).start()

    def norms(j, carry):
        load(j).wait()

        @pl.when(j < 7)
        def _():
            load(j + 1).start()

        def some(r, carry):
            v = xb[j % 2, aligned(r, 32), :].astype(F32)
            v = v - jnp.mean(v, axis=1, keepdims=True)
            v = v * lax.rsqrt(jnp.mean(v * v, axis=1, keepdims=True) + EPSILON)
            at = aligned(j * 8 + r, 32)
            n1s[at, :] = (v * gain[0:1, :] + bias[0:1, :]).astype(BF)
            n2s[at, :] = (v * gain[1:2, :] + bias[1:2, :]).astype(BF)
            return carry

        return lax.fori_loop(0, 8, some, carry)

    lax.fori_loop(0, 8, norms, 0)
    saves = (pltpu.make_async_copy(n1s, n1, work_sems.at[0]), pltpu.make_async_copy(n2s, n2, work_sems.at[1]))
    for v in saves:
        v.start()
    for v in blocks:
        v.pass_on()
    for v in (into, second, qkv):
        v.finish()
    loads = (pltpu.make_async_copy(wqf, wv, work_sems.at[2]), pltpu.make_async_copy(ainf, av, work_sems.at[3]),
             pltpu.make_async_copy(bqf, bv, work_sems.at[4]))
    for v in loads:
        v.start()
    for v in loads:
        v.wait()

    def fold(m, carry):
        at = aligned(m, 256)
        for i in range(3):
            v = (wv[i, at, :].astype(F32) + SCALE * dot(av[i, :, at], bv[i], 0, 0)).astype(BF)
            wv[i, at, :] = v
            mt[i, :, at] = jnp.transpose(v)
        return carry

    lax.fori_loop(0, 4, fold, 0)
    folded = pltpu.make_async_copy(wv, mq, work_sems.at[5])
    folded.start()

    def put(j):
        return pltpu.make_async_copy(stage.at[j % 2], lin.at[:, :, aligned(j, 256)], block_sems.at[2 + j % 2])

    def project(j, carry):
        at = aligned(j, 256)

        @pl.when(j > 1)
        def _():
            put(j - 2).wait()

        for i in range(3):
            stage[j % 2, i] = dot(mt[i], n1s[at, :], 1, 1)
            low3[i, :, at] = dot(av[i], n1s[at, :], 1, 1).astype(BF)
        low1[:, at] = dot(av[3], n2s[at, :], 1, 1).astype(BF)
        put(j).start()
        return carry

    lax.fori_loop(0, 8, project, 0)
    g_rows.relay()
    for v in (b_out, a_out, out, g_rows):
        v.finish()
    put(6).wait()
    put(7).wait()
    folded.wait()
    for v in saves:
        v.wait()


def front(x, g, wq, wo, ain, bq, ao, bo, gain, bias):
    shapes = [(2048, 1024), (2048, 1024), (3, 1024, 512), (512, 1024), (4, 128, 1024), (3, 128, 512), (512, 128),
              (2, 128, 1024), (2048, 1024), (2048, 1024), (3, 1024, 512), (3, 512, 2048), (3, 128, 2048), (128, 2048)]
    anywhere, vmem = pl.BlockSpec(memory_space=pl.ANY), pl.BlockSpec(memory_space=pltpu.VMEM)
    return pl.pallas_call(
        front_kernel,
        in_specs=[anywhere] * 8 + [vmem] * 2,
        out_specs=[anywhere] * 12 + [vmem] * 2,
        out_shape=[jax.ShapeDtypeStruct(s, F32 if i == 11 else BF) for i, s in enumerate(shapes)],
        scratch_shapes=[
            pltpu.SemaphoreType.DMA((2, 16)),
            pltpu.SemaphoreType.DMA((6, 16)),
            pltpu.SemaphoreType.DMA((8, 2)),
            pltpu.VMEM((256, 1024), BF),
            pltpu.VMEM((256, 1024), BF),
            pltpu.VMEM((3, 1024, 128), BF),
            pltpu.VMEM((128, 1024), BF),
            pltpu.VMEM((4, 32, 1024), BF),
            pltpu.VMEM((3, 128, 128), BF),
            pltpu.VMEM((128, 128), BF),
            pltpu.VMEM((2, 32, 1024), BF),
            pltpu.SemaphoreType.DMA((4,)),
            pltpu.SemaphoreType.DMA((6,)),
            pltpu.VMEM((2, 256, 1024), BF),
            pltpu.VMEM((2048, 1024), BF),
            pltpu.VMEM((2048, 1024), BF),
            pltpu.VMEM((3, 1024, 512), BF),
            pltpu.VMEM((4, 128, 1024), BF),
            pltpu.VMEM((3, 128, 512), BF),
            pltpu.VMEM((3, 512, 1024), BF),
            pltpu.VMEM((2, 3, 512, 256), F32),
        ],
        compiler_params=pltpu.CompilerParams(collective_id=0, has_side_effects=True, vmem_limit_bytes=56 << 20),
        name="front",
    )(x, g, wq, wo, ain, bq, ao, bo, gain, bias)


def back_kernel(dl, dp, mq, mu, xf, gf, gain, y, dbq, dbu, dao, dad, dsh,
                out, yout, obq, obu, oao, oad, osh, ono,
                row_sems, share_sems, cross_sems, z_sems, last_sems, norm_sems, local, weight_sems,
                sh_in, sh, rbq, rbu, rao, rad, rsh, pbq, pbu, pao, pad, psh, qbq, qbu, qao, qad, qsh,
                no_plane, no_z, no_own, no_mid, wq, wu, dlb, dpb, xb, gb, dlt, one, two, std, inv, sends, gets, rows):
    z, c, t = place()
    d = 2 * z + c
    sibling = (2 * z + (c ^ 1), t)

    def first_row(j):
        return (t ^ (j % 4)) * 512 + ((c + 1 + j // 4) % 2) * 256

    def loads(j):
        n = j % 2
        at = pl.ds(pl.multiple_of(first_row(j), 256), 256)
        return [pltpu.make_async_copy(v, w.at[n], local.at[i, n]) for i, (v, w) in enumerate((
            (dl.at[:, :, at], dlb), (dp.at[at], dpb), (xf.at[at], xb), (gf.at[at], gb)))]

    weights = (pltpu.make_async_copy(mq, wq, weight_sems.at[0]), pltpu.make_async_copy(mu, wu, weight_sems.at[1]))
    for v in loads(0):
        v.start()
    for v in weights:
        v.start()
    meet(z, c, t, (1, 2, 3))

    home = t % 2
    local_row = home == c
    slot = (t // 2) * 2 + c

    def row(k):
        return remote(rows.at[k], out.at[t // 2, aligned(c, 256)], row_sems.at[k], row_sems.at[4 + slot],
                      (2 * z + home, t ^ k))

    def own_row():
        return pltpu.make_async_copy(rows.at[0], out.at[t // 2, aligned(c, 256)], row_sems.at[4 + slot])

    def y_row(k):
        return remote(y.at[t ^ k], yout.at[t // 2, aligned(c, 256)], row_sems.at[16 + k], row_sems.at[20 + slot],
                      (2 * z + home, t ^ k))

    def own_y():
        return pltpu.make_async_copy(y.at[t], yout.at[t // 2, aligned(c, 256)], row_sems.at[20 + slot])

    def give(k):
        return remote(sends.at[k], gets.at[k], row_sems.at[8 + k], row_sems.at[12 + k], sibling)

    def share():
        return remote(dsh.at[:, :, aligned(c ^ 1, 512)], sh_in, share_sems.at[0], share_sems.at[1], sibling)

    def parts(j):
        return (dbq.at[:, :, aligned(j, 128)], dbu.at[:, aligned(j, 512)], dao.at[aligned(j, 128)],
                dad.at[:, aligned(j, 512)], sh.at[:, aligned(j, 32)])

    got = (rbq, rbu, rao, rad, rsh)

    def cross(k, i):
        return remote(parts(t ^ k)[i], got[i].at[k - 1], cross_sems.at[0, k - 1, i], cross_sems.at[1, k - 1, i], (d, t ^ k))

    sums = (pbq, pbu, pao, pad, psh)
    halves = (qbq, qbu, qao, qad, qsh)
    low = z % 2

    def half(v, i, j):
        if i == 0:
            return v.at[:, aligned(j, 64)]
        if i == 4:
            return v.at[:, aligned(j, 16)]
        return v.at[aligned(j, 64)]

    def along(step, i):
        j = low ^ 1 if step == 0 else low
        dst = sums[i].at[2] if step == 2 else halves[i].at[step]
        return remote(half(sums[i].at[step], i, j), half(dst, i, j), z_sems.at[0, step, i], z_sems.at[1, step, i],
                      (d ^ (4 if step == 1 else 2), t))

    def arrived(step, i):
        j = low ^ 1 if step == 2 else low
        dst = sums[i].at[2] if step == 2 else halves[i].at[step]
        return remote(half(dst, i, j), half(dst, i, j), z_sems.at[0, step, i], z_sems.at[1, step, i], (d, t ^ 1))

    result = (obq.at[:, :, aligned(c, 128)], obu.at[:, aligned(c, 512)], oao.at[aligned(c, 128)],
              oad.at[:, aligned(c, 512)], osh.at[:, :, aligned(c, 512)])
    theirs = (obq.at[:, :, aligned(c ^ 1, 128)], obu.at[:, aligned(c ^ 1, 512)], oao.at[aligned(c ^ 1, 128)],
              oad.at[:, aligned(c ^ 1, 512)], osh.at[:, :, aligned(c ^ 1, 512)])

    def last(i):
        return remote(result[i], result[i], last_sems.at[0, i], last_sems.at[1, i], sibling)

    share().start()
    for k in (1, 2, 3):
        y_row(k).start()

    @pl.when(local_row)
    def _():
        own_y().start()

    @pl.when(jnp.logical_not(local_row))
    def _():
        y_row(0).start()

    for v in weights:
        v.wait()
    no_own[...] = jnp.zeros_like(no_own)

    def block(j, carry):
        n, k = j % 2, j % 4
        for v in loads(j):
            v.wait()

        @pl.when(j < 7)
        def _():
            for v in loads(j + 1):
                v.start()

        for i in range(3):
            dlt[i] = jnp.transpose(dlb[n, i])

        def columns(m, carry):
            at = aligned(m, 256)
            one[:, at] = (dot(dlt[0], wq[0, at, :], 1, 1) + dot(dlt[1], wq[1, at, :], 1, 1)
                          + dot(dlt[2], wq[2, at, :], 1, 1))
            two[:, at] = dot(dpb[n], wu[at, :], 1, 1)
            return carry

        lax.fori_loop(0, 4, columns, 0)

        def norms(r, carry):
            at = aligned(r, 32)
            v = xb[n, at, :].astype(F32)
            v = v - jnp.mean(v, axis=1, keepdims=True)
            inverse = lax.rsqrt(jnp.mean(v * v, axis=1, keepdims=True) + EPSILON)
            v = v * inverse
            a, b = one[at, :], two[at, :]
            for i, w in enumerate((a * v, b * v, a, b)):
                no_own[i] += jnp.sum(w.reshape(4, 8, 1024), axis=0)
            one[at, :] = gain[0:1, :] * a + gain[1:2, :] * b
            std[at, :] = v
            inv[at, :] = inverse
            return carry

        lax.fori_loop(0, 8, norms, 0)

        @pl.when(j < 4)
        def _():
            sends[k] = one[...].astype(BF)
            give(k).start()

        @pl.when(j >= 4)
        def _():
            give(k).wait_recv()

            def finish(r, carry):
                at = aligned(r, 32)
                v, own = one[at, :] + gets[k, at, :].astype(F32), std[at, :]
                v = v - jnp.mean(v, axis=1, keepdims=True) - own * jnp.mean(v * own, axis=1, keepdims=True)
                rows[k, at, :] = (gb[n, at, :].astype(F32) + v * inv[at, :]).astype(BF)
                return carry

            lax.fori_loop(0, 8, finish, 0)
            here = (k == 0) & local_row

            @pl.when(here)
            def _():
                own_row().start()

            @pl.when(jnp.logical_not(here))
            def _():
                row(k).start()

        @pl.when(j == 0)
        def _():
            share().wait_recv()
            for i in range(6):
                sh[i] = (dsh[i, :, aligned(c, 512)].astype(F32) + sh_in[i].astype(F32)).astype(BF)
            for i in range(5):
                for p in (1, 2, 3):
                    cross(p, i).start()

        @pl.when(j == 3)
        def _():
            for i in range(5):
                for p in (1, 2, 3):
                    cross(p, i).wait_recv()
                total = parts(t)[i][...].astype(F32)
                for p in (0, 1, 2):
                    total = total + got[i][p].astype(F32)
                sums[i][0] = total.astype(BF)
                along(0, i).start()

        for step, when in ((0, 4), (1, 6)):
            @pl.when(j == when)
            def _():
                for i in range(5):
                    arrived(step, i).wait_recv()
                    mine, other = half(sums[i].at[step], i, low), half(halves[i].at[step], i, low)
                    half(sums[i].at[step + 1], i, low)[...] = (mine[...].astype(F32) + other[...].astype(F32)).astype(BF)
                    along(step + 1, i).start()

        return carry

    lax.fori_loop(0, 8, block, 0)

    plane = [(h, k) for h in (0, 1) for k in range(4) if h or k]

    def norm(n):
        h, k = plane[n]
        return remote(no_mid.at[0], no_plane.at[2 * t + c], norm_sems.at[0, n], norm_sems.at[1, n], (2 * z + (c ^ h), t ^ k))

    def norm_from(n):
        h, k = plane[n]
        spot = no_plane.at[2 * (t ^ k) + (c ^ h)]
        return remote(spot, spot, norm_sems.at[0, n], norm_sems.at[1, n], sibling)

    def norm_z(k):
        return remote(no_mid.at[1], no_z.at[z], norm_sems.at[0, 6 + k], norm_sems.at[1, 6 + k], (d ^ (2 * k), t))

    def norm_z_from(k):
        return remote(no_z.at[z ^ k], no_z.at[z ^ k], norm_sems.at[0, 6 + k], norm_sems.at[1, 6 + k], sibling)

    own = jnp.sum(no_own[...], axis=1)
    no_mid[0] = own
    for n in range(7):
        norm(n).start()
    no_plane[2 * t + c] = own
    for i in range(5):
        arrived(2, i).wait_recv()
        result[i][...] = sums[i][2].astype(F32)
        last(i).start()
    for n in range(7):
        norm_from(n).wait_recv()
    own = no_plane[0]
    for n in range(1, 8):
        own = own + no_plane[n]
    no_mid[1] = own
    for k in (1, 2, 3):
        norm_z(k).start()
    no_z[z] = own
    for i in range(5):
        remote(theirs[i], theirs[i], last_sems.at[0, i], last_sems.at[1, i], sibling).wait_recv()
        last(i).wait_send()
        for step in (0, 1, 2):
            along(step, i).wait_send()
        for k in (1, 2, 3):
            cross(k, i).wait_send()
    share().wait_send()
    for k in (1, 2, 3):
        norm_z_from(k).wait_recv()
    ono[...] = ((no_z[0] + no_z[1]) + no_z[2]) + no_z[3]
    for n in range(7):
        norm(n).wait_send()
    for k in (1, 2, 3):
        norm_z(k).wait_send()
        row(k).wait_send()
        y_row(k).wait_send()
    for k in range(4):
        give(k).wait_send()

    @pl.when(jnp.logical_not(local_row))
    def _():
        row(0).wait_send()
        y_row(0).wait_send()

    for m in (0, 1):
        for h in (0, 1):
            pltpu.make_async_copy(rows.at[0], out.at[m, pl.ds(256 * h, 256)], row_sems.at[4 + 2 * m + h]).wait()
            pltpu.make_async_copy(y.at[0], yout.at[m, pl.ds(256 * h, 256)], row_sems.at[20 + 2 * m + h]).wait()


def back(dl, dp, mq, mu, xf, gf, gain, y, dbq, dbu, dao, dad, dsh):
    vmem = pl.BlockSpec(memory_space=pltpu.VMEM)
    anywhere = pl.BlockSpec(memory_space=pl.ANY)
    part = [(3, 128, 128), (128, 512), (128, 128), (128, 512), (6, 32, 512)]
    outs = [((2, 512, 1024), BF), ((2, 512, 1024), BF), ((3, 128, 256), F32), ((128, 1024), F32), ((256, 128), F32), ((128, 1024), F32),
            ((6, 32, 1024), F32), ((4, 1024), F32)]
    return pl.pallas_call(
        back_kernel,
        in_specs=[anywhere] * 6 + [vmem] * 7,
        out_specs=[anywhere] * 2 + [vmem] * 6,
        out_shape=[jax.ShapeDtypeStruct(s, d) for s, d in outs],
        scratch_shapes=[
            pltpu.SemaphoreType.DMA((24,)),
            pltpu.SemaphoreType.DMA((2,)),
            pltpu.SemaphoreType.DMA((2, 3, 5)),
            pltpu.SemaphoreType.DMA((2, 3, 5)),
            pltpu.SemaphoreType.DMA((2, 5)),
            pltpu.SemaphoreType.DMA((2, 10)),
            pltpu.SemaphoreType.DMA((4, 2)),
            pltpu.SemaphoreType.DMA((2,)),
            pltpu.VMEM((6, 128, 512), BF),
            pltpu.VMEM((6, 128, 512), BF),
        ] + [pltpu.VMEM((3,) + s, BF) for s in part + part] + [pltpu.VMEM((2,) + s, BF) for s in part] + [
            pltpu.VMEM((8, 4, 1024), F32),
            pltpu.VMEM((4, 4, 1024), F32),
            pltpu.VMEM((4, 8, 1024), F32),
            pltpu.VMEM((2, 4, 1024), F32),
            pltpu.VMEM((3, 1024, 512), BF),
            pltpu.VMEM((1024, 2048), BF),
            pltpu.VMEM((2, 3, 512, 256), BF),
            pltpu.VMEM((2, 256, 2048), BF),
            pltpu.VMEM((2, 256, 1024), BF),
            pltpu.VMEM((2, 256, 1024), BF),
            pltpu.VMEM((3, 256, 512), BF),
            pltpu.VMEM((256, 1024), F32),
            pltpu.VMEM((256, 1024), F32),
            pltpu.VMEM((256, 1024), F32),
            pltpu.VMEM((256, 1), F32),
            pltpu.VMEM((4, 256, 1024), BF),
            pltpu.VMEM((4, 256, 1024), BF),
            pltpu.VMEM((4, 256, 1024), BF),
        ],
        compiler_params=pltpu.CompilerParams(collective_id=1, has_side_effects=True, vmem_limit_bytes=56 << 20),
        name="back",
    )(dl, dp, mq, mu, xf, gf, gain, y, dbq, dbu, dao, dad, dsh)


def swap(v, k=1):
    return lax.ppermute(v, "dp", [(i, i ^ k) for i in range(lax.axis_size("dp"))])


def pick(v, axis, index, size):
    return lax.dynamic_slice_in_dim(v, index * size, size, axis)


def half_rows(v, c):
    return pick(v.reshape(4, 2, 256, -1), 1, c, 1)[:, 0]


def by_groups(x, gy, segment, keep, gain, bias, w_qkv, w_out, w_up, w_down,
              a_in, b_qkv, b_up, a_out, a_down, b_out):
    z, c, t = place()
    tables = jnp.stack([segment[:, 0], keep[:, 0]], 1)
    pair = jnp.where(t % 2 == c, tables, swap(tables))
    seg, kept = jnp.where(t // 2 == 0, pair[0], pair[1])

    x_full, g_full, _, out, a_full, b_qkv_all, a_out_all, b_full, n1, n2, m_qkv, lin, low3, low1 = front(
        x[:, 0], gy[:, 0], w_qkv, w_out, jnp.swapaxes(a_in, 1, 2), b_qkv, a_out, b_out, gain, bias)
    up, down = lax.optimization_barrier((
        jnp.concatenate([pick(w_up, 1, c, 512), pick(b_up, 1, c, 512)], axis=0),
        jnp.concatenate([pick(w_down, 0, c, 512), pick(a_down, 0, c, 512)], axis=1), x_full))[:2]
    up = lax.all_gather(up, "tensor", axis=0)
    down = lax.all_gather(down, "tensor", axis=0, tiled=True)
    w_up_all = jnp.concatenate([up[i, :1024] for i in range(4)], axis=1)
    b_up_all = jnp.concatenate([up[i, 1024:] for i in range(4)], axis=1)
    w_down_all, a_down_all = down[:, :1024], down[:, 1024:]

    m_up = (w_up_all.astype(F32) + SCALE * dot(a_full[3], b_up_all, 0, 0)).astype(BF)
    m_out = (out.astype(F32) + SCALE * dot(a_out_all, b_full[0], 1, 0)).astype(BF)
    m_down = (w_down_all.astype(F32) + SCALE * dot(a_down_all, b_full[1], 1, 0)).astype(BF)
    b_both = b_full.reshape(2 * RANK, 1024)

    g_ctx = dot(m_out, g_full, 1, 1).astype(BF)
    low_grad = (SCALE * dot(b_both, g_full, 1, 1)).astype(BF)
    cos, sin = rotary_tables(seg)
    ctx, d_lin = attention(lin, g_ctx, cos, sin, seg, kept)

    pre = dot(n2, m_up, 1, 0)
    cdf = 0.5 * (1.0 + lax.erf(pre * math.sqrt(0.5)))
    hidden = (pre * cdf).astype(BF)
    slope = cdf + pre * (math.sqrt(0.5 / math.pi) * jnp.exp(-0.5 * pre * pre))
    d_pre = (dot(g_full, m_down, 1, 1) * slope).astype(BF)

    part = dot(ctx, m_out, 0, 0) + dot(hidden, m_down, 1, 0)
    theirs = swap(half_rows(part, 1 - c).astype(BF))
    y = half_rows(x_full, c).astype(F32) + half_rows(part, c) + theirs.astype(F32)

    lo = jnp.concatenate([dot(a_out_all, ctx, 0, 0), dot(a_down_all, hidden, 0, 1)], axis=0).astype(BF)
    d_a_out = dot(ctx, low_grad[:RANK], 1, 1).astype(BF)
    d_a_down = dot(low_grad[RANK:], hidden, 1, 0).astype(BF)
    d_b_qkv = (SCALE * jnp.einsum("nrs,ncs->nrc", low3, d_lin, preferred_element_type=F32)).astype(BF)
    d_b_up = (SCALE * dot(low1, d_pre, 1, 0)).astype(BF)
    back3 = (SCALE * jnp.einsum("nrc,ncs->nrs", b_qkv_all, d_lin, preferred_element_type=F32)).astype(BF)
    back1 = (SCALE * dot(b_up_all, d_pre, 1, 1)).astype(BF)
    shared = jnp.concatenate([dot(back3.reshape(3 * RANK, 2048), n1, 1, 0).astype(BF), dot(back1, n2, 1, 0).astype(BF),
                              (SCALE * dot(lo, g_full, 1, 0)).astype(BF)], axis=0).reshape(6, RANK, 1024)
    grad, y, r_b_qkv, r_b_up, r_a_out, r_a_down, rest, norms = back(
        d_lin, d_pre, m_qkv, m_up, x_full, g_full, gain, y.astype(BF), d_b_qkv, d_b_up, d_a_out, d_a_down, shared)
    r_a_in = jnp.swapaxes(rest[:4], 1, 2)
    return (y[:, None], grad[:, None], norms[:2], norms[2:], r_a_in, r_b_qkv, r_b_up, r_a_out, jnp.transpose(r_a_down), rest[4:])


def solution(mesh):
    in_specs = (
        P(None, "dp", "tensor", None),
        P(None, "dp", "tensor", None),
        P(None, "dp", None),
        P(None, "dp", None),
        P(),
        P(),
        P(None, None, "tensor"),
        P("tensor", None),
        P(None, "tensor"),
        P("tensor", None),
        P(None, None, "tensor"),
        P(None, None, "tensor"),
        P(None, "tensor"),
        P("tensor", None),
        P("tensor", None),
        P(None, "tensor", None),
    )
    out_specs = (
        P(None, "dp", "tensor", None),
        P(None, "dp", "tensor", None),
        P(),
        P(),
        P(None, None, "tensor"),
        P(None, None, "tensor"),
        P(None, "tensor"),
        P("tensor", None),
        P("tensor", None),
        P(None, "tensor", None),
    )
    small = mesh.shape["tensor"] == 4 and mesh.shape["dp"] == 8
    return jax.shard_map(
        by_groups if small else by_features, mesh=mesh, in_specs=in_specs, out_specs=out_specs, check_vma=False
    )
```

```python
import functools
import math

import jax
import jax.numpy as jnp
from jax import lax
from jax.experimental import pallas as pl
from jax.experimental.pallas import tpu as pltpu
from jax.sharding import PartitionSpec as P

HEAD = 64
HALF = 8
N_DOCS = 5
TILE = 256
SLOTS = 5
EPSILON = 1e-05
SCALE = 0.25
F32 = jnp.float32
BF = jnp.bfloat16


def dot(a, b, ca, cb):
    return lax.dot_general(a, b, (((ca,), (cb,)), ((), ())), preferred_element_type=F32)


def attention_kernel(heads, lo_ref, lin_ref, g_ref, cos_ref, sin_ref, segq_ref, segk_ref,
                     ctx_ref, dlin_ref, qt, kt, vt, kn, vn, acc, s_scr, e_scr, p_scr, row):
    length = lin_ref.shape[2]
    blocks = length // TILE

    def rotate(z, cos, sin):
        a, b = z[:HALF], z[HALF:2 * HALF]
        return jnp.concatenate([a * cos - b * sin, b * cos + a * sin, z[2 * HALF:]], axis=0)

    def prepare(c, carry):
        cols = pl.ds(pl.multiple_of(c * TILE, TILE), TILE)
        cos, sin = cos_ref[:, cols], sin_ref[:, cols]
        for h in range(heads):
            rows = pl.ds(h * HEAD, HEAD)
            q = rotate(lin_ref[0, pl.ds(h * HEAD, HEAD), cols], cos, sin).astype(BF).astype(F32) * 0.125
            k = rotate(lin_ref[1, pl.ds(h * HEAD, HEAD), cols], cos, sin)
            v = lin_ref[2, pl.ds(h * HEAD, HEAD), cols]
            qt[rows, cols] = q.astype(BF)
            kt[rows, cols] = k.astype(BF)
            vt[rows, cols] = v.astype(BF)
            kn[h, cols, :] = jnp.transpose(k).astype(BF)
            vn[h, cols, :] = jnp.transpose(v).astype(BF)
            acc[h, :, cols] = jnp.zeros((2 * HEAD, TILE), F32)
        return carry

    lax.fori_loop(0, blocks, prepare, 0)

    def query_block(qb, carry):
        lo = lo_ref[qb]
        qcols = pl.ds(pl.multiple_of(qb * TILE, TILE), TILE)
        segq = segq_ref[:, qcols]

        def scores(kb, tops, last=False):
            krows = pl.ds(pl.multiple_of(kb * TILE, TILE), TILE)
            allowed = segk_ref[krows, :] == segq
            if last:
                k, q = (lax.broadcasted_iota(jnp.int32, (TILE, TILE), i) for i in (0, 1))
                allowed = (allowed & (k < q)) | (k == q)
            out = []
            for h in range(heads):
                rows = pl.ds(h * HEAD, HEAD)
                s = dot(kn[h, krows, :], qt[rows, qcols], 1, 0)
                s = jnp.where(allowed, s, -1e30)
                s_scr[h, kb - lo] = s
                p_scr[h, kb - lo] = dot(vn[h, krows, :], g_ref[rows, qcols], 1, 0)
                out.append(jnp.maximum(tops[h], jnp.max(s, axis=0, keepdims=True)))
            return tuple(out)

        tops = lax.fori_loop(lo, qb, scores, tuple(jnp.full((1, TILE), -1e30, F32) for _ in range(heads)))
        tops = scores(qb, tops, True)

        def weights(kb, sums):
            kcols = pl.ds(pl.multiple_of(kb * TILE, TILE), TILE)
            out = []
            for h in range(heads):
                e = jnp.exp(s_scr[h, kb - lo] - tops[h])
                low = e.astype(BF)
                e_scr[h, kb - lo] = low
                out.append(sums[h] + jnp.sum(e, axis=0, keepdims=True))
                row[h] += dot(vt[pl.ds(h * HEAD, HEAD), kcols], low, 1, 0)
            return tuple(out)

        row[...] = jnp.zeros_like(row)
        sums = lax.fori_loop(lo, qb + 1, weights, tuple(jnp.zeros((1, TILE), F32) for _ in range(heads)))
        gts, terms, scales = [], [], []
        for h in range(heads):
            rows = pl.ds(h * HEAD, HEAD)
            inverse = 1.0 / sums[h]
            ctx = row[h] * inverse
            ctx_ref[rows, qcols] = ctx.astype(BF)
            g = g_ref[rows, qcols].astype(F32)
            terms.append(jnp.sum(g * ctx, axis=0, keepdims=True))
            scales.append(inverse)
            gts.append((g * inverse).astype(BF))

        row[...] = jnp.zeros_like(row)

        def backward(kb, carry):
            krows = pl.ds(pl.multiple_of(kb * TILE, TILE), TILE)
            for h in range(heads):
                low = e_scr[h, kb - lo]
                ds = (low.astype(F32) * ((p_scr[h, kb - lo] - terms[h]) * scales[h])).astype(BF)
                acc[h, :HEAD, krows] += dot(gts[h], low, 1, 1)
                acc[h, HEAD:, krows] += dot(qt[pl.ds(h * HEAD, HEAD), qcols], ds, 1, 1)
                row[h] += dot(kt[pl.ds(h * HEAD, HEAD), krows], ds, 1, 0)
            return carry

        lax.fori_loop(lo, qb + 1, backward, 0)
        cos, sin = cos_ref[:, qcols], sin_ref[:, qcols]
        for h in range(heads):
            dlin_ref[0, pl.ds(h * HEAD, HEAD), qcols] = rotate(row[h] * 0.125, cos, -sin).astype(BF)
        return carry

    lax.fori_loop(0, blocks, query_block, 0)

    def finish(c, carry):
        cols = pl.ds(pl.multiple_of(c * TILE, TILE), TILE)
        cos, sin = cos_ref[:, cols], sin_ref[:, cols]
        for h in range(heads):
            both = acc[h, :, cols]
            dlin_ref[1, pl.ds(h * HEAD, HEAD), cols] = rotate(both[HEAD:], cos, -sin).astype(BF)
            dlin_ref[2, pl.ds(h * HEAD, HEAD), cols] = both[:HEAD].astype(BF)
        return carry

    lax.fori_loop(0, blocks, finish, 0)


def attention(lin, g, cos, sin, segment, keep):
    width, length = g.shape
    heads = min(4, width // HEAD)
    wide = heads * HEAD
    starts = jnp.sum(segment[None, :] < jnp.arange(N_DOCS, dtype=jnp.int32)[:, None], axis=1)
    firsts = segment[::TILE]
    lo = jnp.sum(jnp.where(firsts[:, None] == jnp.arange(N_DOCS)[None, :], starts[None, :], 0), axis=1)
    lo = (lo // TILE).astype(jnp.int32)
    segk = jnp.where(keep == 1, segment, -1)[:, None]
    vmem = pl.BlockSpec(memory_space=pltpu.VMEM)
    three = pl.BlockSpec((3, wide, length), lambda i, lo: (0, i, 0))
    single = pl.BlockSpec((wide, length), lambda i, lo: (i, 0))
    return pl.pallas_call(
        functools.partial(attention_kernel, heads),
        grid_spec=pltpu.PrefetchScalarGridSpec(
            num_scalar_prefetch=1,
            grid=(width // wide,),
            in_specs=[three, single] + [vmem] * 4,
            out_specs=[single, three],
            scratch_shapes=[
                pltpu.VMEM((wide, length), BF),
                pltpu.VMEM((wide, length), BF),
                pltpu.VMEM((wide, length), BF),
                pltpu.VMEM((heads, length, HEAD), BF),
                pltpu.VMEM((heads, length, HEAD), BF),
                pltpu.VMEM((heads, 2 * HEAD, length), F32),
                pltpu.VMEM((heads, SLOTS, TILE, TILE), F32),
                pltpu.VMEM((heads, SLOTS, TILE, TILE), BF),
                pltpu.VMEM((heads, SLOTS, TILE, TILE), F32),
                pltpu.VMEM((heads, HEAD, TILE), F32),
            ]),
        out_shape=[jax.ShapeDtypeStruct((width, length), BF), jax.ShapeDtypeStruct((3, width, length), BF)],
        compiler_params=pltpu.CompilerParams(vmem_limit_bytes=60 << 20),
        name="attention",
        cost_estimate=pl.CostEstimate(flops=10 * width * length * 768, transcendentals=width * length * 12,
                                      bytes_accessed=26 * width * length),
    )(lo, lin, g, cos, sin, segment[None, :], segk)


def rotary_tables(segment):
    length = segment.shape[0]
    starts = jnp.sum(segment[None, :] < jnp.arange(N_DOCS, dtype=jnp.int32)[:, None], axis=1)
    begin = jnp.sum(jnp.where(segment[None, :] == jnp.arange(N_DOCS)[:, None], starts[:, None], 0), axis=0)
    position = (jnp.arange(length, dtype=jnp.int32) - begin).astype(F32)
    exponent = jnp.arange(HALF, dtype=F32) / HALF
    frequency = jnp.exp(-math.log(10000.0) * exponent)
    angles = frequency[:, None] * position[None, :]
    return jnp.cos(angles), jnp.sin(angles)


def normalized(values):
    average = jnp.mean(values, axis=-1, keepdims=True)
    centered = values - average
    variance = jnp.mean(centered * centered, axis=-1, keepdims=True)
    inverse = lax.rsqrt(variance + EPSILON)
    return centered * inverse, inverse


def by_features(x, gy, segment, keep, gain, bias, w_qkv, w_out, w_up, w_down,
              a_in, b_qkv, b_up, a_out, a_down, b_out):
    width = w_qkv.shape[2]
    micro = x.shape[0]
    a_full = lax.all_gather(a_in, "tensor", axis=2, tiled=True)
    b_full = lax.all_gather(b_out, "tensor", axis=1, tiled=True)

    m_qkv = jnp.concatenate([
        (w_qkv[i].astype(F32) + SCALE * dot(a_full[i], b_qkv[i], 1, 0)).astype(BF) for i in range(3)
    ], axis=1)
    m_up = (w_up.astype(F32) + SCALE * dot(a_full[3], b_up, 1, 0)).astype(BF)
    m_out = (w_out.astype(F32) + SCALE * dot(a_out, b_full[0], 1, 0)).astype(BF)
    m_down = (w_down.astype(F32) + SCALE * dot(a_down, b_full[1], 1, 0)).astype(BF)
    a_three = jnp.concatenate([a_full[0], a_full[1], a_full[2]], axis=1)
    b_both = jnp.concatenate([b_full[0], b_full[1]], axis=0)

    outs, grads, sums = [], [], None
    for m in range(micro):
        rows, seg = x[m, 0], segment[m, 0]
        xg = lax.all_gather(rows, "tensor", axis=0, tiled=True)
        gg = lax.all_gather(gy[m, 0], "tensor", axis=0, tiled=True)
        standard, _ = normalized(xg.astype(F32))
        n1 = (standard * gain[0] + bias[0]).astype(BF)
        n2 = (standard * gain[1] + bias[1]).astype(BF)
        lin = dot(m_qkv, n1, 0, 1)
        low3 = dot(n1, a_three, 1, 0).astype(BF)
        low1 = dot(n2, a_full[3], 1, 0).astype(BF)
        g_ctx = dot(m_out, gg, 1, 1).astype(BF)
        low_grad = (SCALE * dot(gg, b_both, 1, 1)).astype(BF)
        cos, sin = rotary_tables(seg)
        ctx, d_lin = attention(lin.reshape(3, width, -1), g_ctx, cos, sin, seg, keep[m, 0])
        d_lin = d_lin.reshape(3 * width, -1)

        pre = dot(n2, m_up, 1, 0)
        cdf = 0.5 * (1.0 + lax.erf(pre * math.sqrt(0.5)))
        hidden = (pre * cdf).astype(BF)
        slope = cdf + pre * (math.sqrt(0.5 / math.pi) * jnp.exp(-0.5 * pre * pre))
        d_pre = (dot(gg, m_down, 1, 1) * slope).astype(BF)

        part = dot(ctx, m_out, 0, 0) + dot(hidden, m_down, 1, 0)
        branch = lax.psum_scatter(part.astype(BF), "tensor", scatter_dimension=0, tiled=True)
        outs.append((rows.astype(F32) + branch.astype(F32)).astype(BF))

        one = dot(d_lin, m_qkv, 0, 1)
        two = dot(d_pre, m_up, 1, 1)
        total = (gain[0] * one + gain[1] * two).astype(BF)
        total = lax.psum_scatter(total, "tensor", scatter_dimension=0, tiled=True).astype(F32)
        own, inverse = normalized(rows.astype(F32))
        grad = total - jnp.mean(total, axis=-1, keepdims=True)
        grad = grad - own * jnp.mean(total * own, axis=-1, keepdims=True)
        grads.append((gy[m, 0].astype(F32) + grad * inverse).astype(BF))

        norms = jnp.stack([jnp.sum(one * standard, axis=0), jnp.sum(two * standard, axis=0),
                           jnp.sum(one, axis=0), jnp.sum(two, axis=0)])
        lo_ctx = dot(ctx, a_out, 0, 0).astype(BF)
        lo_hid = dot(hidden, a_down, 1, 0).astype(BF)
        d_b_out = SCALE * jnp.stack([dot(lo_ctx, gg, 0, 0), dot(lo_hid, gg, 0, 0)], axis=1)
        d_a_out = dot(ctx, low_grad[:, :128], 1, 0)
        d_a_down = dot(hidden, low_grad[:, 128:], 0, 0)
        d_b_qkv = SCALE * jnp.stack([
            dot(low3[:, 128 * i:128 * (i + 1)], d_lin[width * i:width * (i + 1)], 0, 1) for i in range(3)])
        d_b_up = SCALE * dot(low1, d_pre, 0, 0)
        back = [(SCALE * dot(d_lin[width * i:width * (i + 1)], b_qkv[i], 0, 1)).astype(BF) for i in range(3)]
        back.append((SCALE * dot(d_pre, b_up, 1, 1)).astype(BF))
        d_a_in = jnp.stack([dot(back[i], n1 if i < 3 else n2, 0, 0) for i in range(4)], axis=1)
        terms = (d_a_in, d_b_qkv, d_b_up, d_a_out, d_a_down, d_b_out, norms)
        sums = terms if sums is None else tuple(p + q for p, q in zip(sums, terms))

    d_a_in, d_b_qkv, d_b_up, d_a_out, d_a_down, d_b_out, norms = sums
    d_a_in = lax.psum_scatter(d_a_in, "tensor", scatter_dimension=0, tiled=True)
    d_b_out = lax.psum_scatter(d_b_out, "tensor", scatter_dimension=0, tiled=True)
    d_a_in, d_b_qkv, d_b_up, d_a_out, d_a_down, d_b_out = lax.psum(
        (d_a_in, d_b_qkv, d_b_up, d_a_out, d_a_down, d_b_out), "dp")
    norms = lax.psum(norms, ("dp", "tensor"))
    return (jnp.stack(outs)[:, None], jnp.stack(grads)[:, None], norms[:2], norms[2:],
            jnp.transpose(d_a_in, (1, 2, 0)), d_b_qkv, d_b_up, d_a_out, d_a_down,
            jnp.transpose(d_b_out, (1, 0, 2)))


RANK = 128


MESH = pl.DeviceIdType.MESH


def place():
    d = lax.axis_index("dp")
    return d // 2, d % 2, lax.axis_index("tensor")


def meet(z, c, t, planes):
    barrier = pltpu.get_barrier_semaphore()
    for h in (0, 1):
        for k in range(4):
            if h or k:
                pl.semaphore_signal(barrier, 1, device_id=(2 * z + (c ^ h), t ^ k), device_id_type=MESH)
    for k in planes:
        pl.semaphore_signal(barrier, 1, device_id=(2 * (z ^ k) + c, t), device_id_type=MESH)
    pl.semaphore_wait(barrier, 7 + len(planes))


def remote(src, dst, send_sem, recv_sem, device):
    return pltpu.make_async_remote_copy(src_ref=src, dst_ref=dst, send_sem=send_sem, recv_sem=recv_sem,
                                        device_id=device, device_id_type=MESH)


class Rows:
    def __init__(self, v, full, sems, stage, local, z, c, t):
        self.v, self.full, self.sems, self.stage, self.local = v, full, sems, stage, local
        self.z, self.c, self.t = z, c, t

    def rows(self, s, h):
        return self.full.at[pl.ds(pl.multiple_of(s * 512 + h * 256, 256), 256)]

    def block(self, m, h):
        return self.v.at[m, pl.ds(pl.multiple_of(h * 256, 256), 256)]

    def copy(self, m, other):
        h = self.c ^ other
        return remote(self.block(m, h), self.rows(self.t, h), self.sems.at[2 * m + other], self.sems.at[4 + self.t],
                      (2 * self.z + h, 2 * m + self.c))

    def forward(self, s):
        part = self.rows(s, self.c)
        return remote(part, part, self.sems.at[8 + s], self.sems.at[12 + s], (2 * self.z + (self.c ^ 1), self.t))

    def start(self):
        for m in (0, 1):
            away = 2 * m + self.c != self.t

            @pl.when(away)
            def _():
                self.copy(m, 0).start()

            self.copy(m, 1).start()

            @pl.when(jnp.logical_not(away))
            def _():
                pltpu.make_async_copy(self.block(m, self.c), self.stage, self.local.at[0]).start()

    def relay(self):
        mine = self.t % 2 == self.c

        @pl.when(mine)
        def _():
            pltpu.make_async_copy(self.block(0, self.c), self.stage, self.local.at[0]).wait()
            pltpu.make_async_copy(self.stage, self.rows(self.t, self.c), self.sems.at[4 + self.t]).start()

        for k in (0, 1, 2, 3):
            s = self.t ^ k
            pltpu.make_async_copy(self.stage, self.rows(s, self.c), self.sems.at[4 + s]).wait()
            self.forward(s).start()

    def finish(self):
        for s in range(4):
            part = self.rows(s, self.c ^ 1)
            remote(part, part, self.sems.at[8 + s], self.sems.at[12 + s], (2 * self.z + (self.c ^ 1), self.t)).wait_recv()
            self.forward(s).wait_send()
        for m in (0, 1):
            @pl.when(2 * m + self.c != self.t)
            def _():
                self.copy(m, 0).wait_send()

            self.copy(m, 1).wait_send()


class Blocks:
    def __init__(self, own, where, sems, stage, local, cut, quarter, z, c, t):
        self.own, self.where, self.sems, self.stage, self.local = own, where, sems, stage, local
        self.cut, self.quarter, self.t, self.d, self.half = cut, quarter, t, 2 * z + c, z % 2

    def spot(self, k, other=0):
        return self.cut(self.where(self.t ^ k), self.half ^ other)

    def first(self, k):
        return remote(self.cut(self.own, self.half), self.spot(0), self.sems.at[k - 1], self.sems.at[2 + k],
                      (self.d, self.t ^ k))

    def arrival(self, k):
        return remote(self.spot(k), self.spot(k), self.sems.at[k - 1], self.sems.at[2 + k], (self.d, self.t ^ k))

    def second(self, k):
        part = self.quarter(self.spot(3 - k), k - 1)
        return remote(part, part, self.sems.at[5 + k], self.sems.at[7 + k], (self.d, self.t ^ k))

    def last(self, k):
        part = self.quarter(self.spot(3), k - 1)
        return remote(part, part, self.sems.at[5 + k], self.sems.at[7 + k], (self.d, self.t ^ k))

    def across(self, k, other=0):
        return remote(self.spot(k, other), self.spot(k, other), self.sems.at[9 + k], self.sems.at[12 + k],
                      (self.d ^ 2, self.t))

    def start(self):
        for k in ((1, 2) if self.quarter else (1, 2, 3)):
            self.first(k).start()
        pltpu.make_async_copy(self.own, self.stage, self.local.at[0]).start()

    def store(self):
        pltpu.make_async_copy(self.own, self.stage, self.local.at[0]).wait()
        pltpu.make_async_copy(self.stage, self.where(self.t), self.local.at[1]).start()

    def relay(self):
        for k in (1, 2):
            self.arrival(3 - k).wait_recv()
            if self.quarter:
                self.second(k).start()
            self.across(3 - k).start()

    def pass_on(self):
        if self.quarter:
            for k in (1, 2):
                self.last(k).wait_recv()
        else:
            self.arrival(3).wait_recv()
        self.across(3).start()

    def finish(self):
        pltpu.make_async_copy(self.stage, self.where(self.t), self.local.at[1]).wait()
        for k in (1, 2, 3):
            self.across(k, 1).wait_recv()
            self.across(k).wait_send()
            if k < 3 or not self.quarter:
                self.first(k).wait_send()
            if k < 3 and self.quarter:
                self.second(k).wait_send()


def aligned(i, n):
    return pl.ds(pl.multiple_of(i * n, n), n)


def front_kernel(x, g, wq, wo, ain, bq, ao, bo,
                 xf, gf, wqf, wof, ainf, bqf, aof, bof,
                 row_sems, sems, local, xs, gs, wqs, wos, ains, bqs, aos, bos):
    z, c, t = place()
    meet(z, c, t, (1,))
    at = dict(z=z, c=c, t=t)
    x_rows = Rows(x, xf, row_sems.at[0], xs, local.at[0], **at)
    g_rows = Rows(g, gf, row_sems.at[1], gs, local.at[1], **at)
    qkv = Blocks(wq.at[:, :, aligned(c, 128)], lambda i: wqf.at[:, :, aligned(i, 128)], sems.at[0], wqs, local.at[2],
                 lambda v, h: v.at[:, aligned(h, 512)], lambda v, h: v.at[:, pl.ds(h * 256, 256)], **at)
    into = Blocks(ain, lambda i: ainf.at[:, aligned(i, 32)], sems.at[1], ains, local.at[3],
                  lambda v, h: v.at[pl.ds(2 * h, 2)], None, **at)
    second = Blocks(bq.at[:, :, aligned(c, 128)], lambda i: bqf.at[:, :, aligned(i, 128)], sems.at[2], bqs, local.at[4],
                    lambda v, h: v.at[:, aligned(h, 64)], None, **at)
    out = Blocks(wo.at[aligned(c, 128)], lambda i: wof.at[aligned(i, 128)], sems.at[3], wos, local.at[5],
                 lambda v, h: v.at[aligned(h, 64)], lambda v, h: v.at[pl.ds(h * 32, 32)], **at)
    a_out = Blocks(ao.at[aligned(c, 128)], lambda i: aof.at[aligned(i, 128)], sems.at[4], aos, local.at[6],
                   lambda v, h: v.at[aligned(h, 64)], None, **at)
    b_out = Blocks(bo, lambda i: bof.at[:, aligned(i, 32)], sems.at[5], bos, local.at[7],
                   lambda v, h: v.at[pl.ds(h, 1)], None, **at)
    x_rows.start()
    for v in (into, second, qkv, b_out, a_out, out):
        v.start()
    g_rows.start()
    x_rows.relay()
    for v in (into, second, qkv, b_out, a_out, out):
        v.store()
    for v in (into, second, qkv, b_out, a_out, out):
        v.relay()
    for v in (into, second, qkv, b_out, a_out, out):
        v.pass_on()
    g_rows.relay()
    for v in (x_rows, into, second, qkv, b_out, a_out, out, g_rows):
        v.finish()


def front(x, g, wq, wo, ain, bq, ao, bo):
    shapes = [(2048, 1024), (2048, 1024), (3, 1024, 512), (512, 1024), (4, 128, 1024), (3, 128, 512), (512, 128),
              (2, 128, 1024)]
    anywhere = pl.BlockSpec(memory_space=pl.ANY)
    return pl.pallas_call(
        front_kernel,
        in_specs=[anywhere] * 8,
        out_specs=[anywhere] * 8,
        out_shape=[jax.ShapeDtypeStruct(s, BF) for s in shapes],
        scratch_shapes=[
            pltpu.SemaphoreType.DMA((2, 16)),
            pltpu.SemaphoreType.DMA((6, 16)),
            pltpu.SemaphoreType.DMA((8, 2)),
            pltpu.VMEM((256, 1024), BF),
            pltpu.VMEM((256, 1024), BF),
            pltpu.VMEM((3, 1024, 128), BF),
            pltpu.VMEM((128, 1024), BF),
            pltpu.VMEM((4, 32, 1024), BF),
            pltpu.VMEM((3, 128, 128), BF),
            pltpu.VMEM((128, 128), BF),
            pltpu.VMEM((2, 32, 1024), BF),
        ],
        compiler_params=pltpu.CompilerParams(collective_id=0, has_side_effects=True),
        name="front",
    )(x, g, wq, wo, ain, bq, ao, bo)


def back_kernel(dl, dp, mq, mu, xf, gf, gain, y, dbq, dbu, dao, dad, dsh,
                out, yout, obq, obu, oao, oad, osh, ono,
                row_sems, share_sems, cross_sems, z_sems, last_sems, norm_sems, local, weight_sems,
                sh_in, sh, rbq, rbu, rao, rad, rsh, pbq, pbu, pao, pad, psh, qbq, qbu, qao, qad, qsh,
                no_plane, no_z, no_own, no_mid, wq, wu, dlb, dpb, xb, gb, dlt, one, two, std, inv, sends, gets, rows):
    z, c, t = place()
    d = 2 * z + c
    sibling = (2 * z + (c ^ 1), t)

    def first_row(j):
        return (t ^ (j % 4)) * 512 + ((c + 1 + j // 4) % 2) * 256

    def loads(j):
        n = j % 2
        at = pl.ds(pl.multiple_of(first_row(j), 256), 256)
        return [pltpu.make_async_copy(v, w.at[n], local.at[i, n]) for i, (v, w) in enumerate((
            (dl.at[:, :, at], dlb), (dp.at[at], dpb), (xf.at[at], xb), (gf.at[at], gb)))]

    weights = (pltpu.make_async_copy(mq, wq, weight_sems.at[0]), pltpu.make_async_copy(mu, wu, weight_sems.at[1]))
    for v in loads(0):
        v.start()
    for v in weights:
        v.start()
    meet(z, c, t, (1, 2, 3))

    home = t % 2
    local_row = home == c
    slot = (t // 2) * 2 + c

    def row(k):
        return remote(rows.at[k], out.at[t // 2, aligned(c, 256)], row_sems.at[k], row_sems.at[4 + slot],
                      (2 * z + home, t ^ k))

    def own_row():
        return pltpu.make_async_copy(rows.at[0], out.at[t // 2, aligned(c, 256)], row_sems.at[4 + slot])

    def y_row(k):
        return remote(y.at[t ^ k], yout.at[t // 2, aligned(c, 256)], row_sems.at[16 + k], row_sems.at[20 + slot],
                      (2 * z + home, t ^ k))

    def own_y():
        return pltpu.make_async_copy(y.at[t], yout.at[t // 2, aligned(c, 256)], row_sems.at[20 + slot])

    def give(k):
        return remote(sends.at[k], gets.at[k], row_sems.at[8 + k], row_sems.at[12 + k], sibling)

    def share():
        return remote(dsh.at[:, :, aligned(c ^ 1, 512)], sh_in, share_sems.at[0], share_sems.at[1], sibling)

    def parts(j):
        return (dbq.at[:, :, aligned(j, 128)], dbu.at[:, aligned(j, 512)], dao.at[aligned(j, 128)],
                dad.at[:, aligned(j, 512)], sh.at[:, aligned(j, 32)])

    got = (rbq, rbu, rao, rad, rsh)

    def cross(k, i):
        return remote(parts(t ^ k)[i], got[i].at[k - 1], cross_sems.at[0, k - 1, i], cross_sems.at[1, k - 1, i], (d, t ^ k))

    sums = (pbq, pbu, pao, pad, psh)
    halves = (qbq, qbu, qao, qad, qsh)
    low = z % 2

    def half(v, i, j):
        if i == 0:
            return v.at[:, aligned(j, 64)]
        if i == 4:
            return v.at[:, aligned(j, 16)]
        return v.at[aligned(j, 64)]

    def along(step, i):
        j = low ^ 1 if step == 0 else low
        dst = sums[i].at[2] if step == 2 else halves[i].at[step]
        return remote(half(sums[i].at[step], i, j), half(dst, i, j), z_sems.at[0, step, i], z_sems.at[1, step, i],
                      (d ^ (4 if step == 1 else 2), t))

    def arrived(step, i):
        j = low ^ 1 if step == 2 else low
        dst = sums[i].at[2] if step == 2 else halves[i].at[step]
        return remote(half(dst, i, j), half(dst, i, j), z_sems.at[0, step, i], z_sems.at[1, step, i], (d, t ^ 1))

    result = (obq.at[:, :, aligned(c, 128)], obu.at[:, aligned(c, 512)], oao.at[aligned(c, 128)],
              oad.at[:, aligned(c, 512)], osh.at[:, :, aligned(c, 512)])
    theirs = (obq.at[:, :, aligned(c ^ 1, 128)], obu.at[:, aligned(c ^ 1, 512)], oao.at[aligned(c ^ 1, 128)],
              oad.at[:, aligned(c ^ 1, 512)], osh.at[:, :, aligned(c ^ 1, 512)])

    def last(i):
        return remote(result[i], result[i], last_sems.at[0, i], last_sems.at[1, i], sibling)

    share().start()
    for v in weights:
        v.wait()
    no_own[...] = jnp.zeros_like(no_own)

    def block(j, carry):
        n, k = j % 2, j % 4
        for v in loads(j):
            v.wait()

        @pl.when(j < 7)
        def _():
            for v in loads(j + 1):
                v.start()

        for i in range(3):
            dlt[i] = jnp.transpose(dlb[n, i])

        def columns(m, carry):
            at = aligned(m, 256)
            one[:, at] = (dot(dlt[0], wq[0, at, :], 1, 1) + dot(dlt[1], wq[1, at, :], 1, 1)
                          + dot(dlt[2], wq[2, at, :], 1, 1))
            two[:, at] = dot(dpb[n], wu[at, :], 1, 1)
            return carry

        lax.fori_loop(0, 4, columns, 0)

        def norms(r, carry):
            at = aligned(r, 32)
            v = xb[n, at, :].astype(F32)
            v = v - jnp.mean(v, axis=1, keepdims=True)
            inverse = lax.rsqrt(jnp.mean(v * v, axis=1, keepdims=True) + EPSILON)
            v = v * inverse
            a, b = one[at, :], two[at, :]
            for i, w in enumerate((a * v, b * v, a, b)):
                no_own[i] += jnp.sum(w.reshape(4, 8, 1024), axis=0)
            one[at, :] = gain[0:1, :] * a + gain[1:2, :] * b
            std[at, :] = v
            inv[at, :] = inverse
            return carry

        lax.fori_loop(0, 8, norms, 0)

        @pl.when(j < 4)
        def _():
            sends[k] = one[...].astype(BF)
            give(k).start()

        @pl.when(j >= 4)
        def _():
            give(k).wait_recv()

            def finish(r, carry):
                at = aligned(r, 32)
                v, own = one[at, :] + gets[k, at, :].astype(F32), std[at, :]
                v = v - jnp.mean(v, axis=1, keepdims=True) - own * jnp.mean(v * own, axis=1, keepdims=True)
                rows[k, at, :] = (gb[n, at, :].astype(F32) + v * inv[at, :]).astype(BF)
                return carry

            lax.fori_loop(0, 8, finish, 0)
            here = (k == 0) & local_row

            @pl.when(here)
            def _():
                own_row().start()

            @pl.when(jnp.logical_not(here))
            def _():
                row(k).start()

        @pl.when(j == 0)
        def _():
            share().wait_recv()
            for i in range(6):
                sh[i] = (dsh[i, :, aligned(c, 512)].astype(F32) + sh_in[i].astype(F32)).astype(BF)
            for i in range(5):
                for p in (1, 2, 3):
                    cross(p, i).start()

        @pl.when(j == 3)
        def _():
            for i in range(5):
                for p in (1, 2, 3):
                    cross(p, i).wait_recv()
                total = parts(t)[i][...].astype(F32)
                for p in (0, 1, 2):
                    total = total + got[i][p].astype(F32)
                sums[i][0] = total.astype(BF)
                along(0, i).start()
            for p in (1, 2, 3):
                y_row(p).start()

            @pl.when(local_row)
            def _():
                own_y().start()

            @pl.when(jnp.logical_not(local_row))
            def _():
                y_row(0).start()

        for step, when in ((0, 4), (1, 6)):
            @pl.when(j == when)
            def _():
                for i in range(5):
                    arrived(step, i).wait_recv()
                    mine, other = half(sums[i].at[step], i, low), half(halves[i].at[step], i, low)
                    half(sums[i].at[step + 1], i, low)[...] = (mine[...].astype(F32) + other[...].astype(F32)).astype(BF)
                    along(step + 1, i).start()

        return carry

    lax.fori_loop(0, 8, block, 0)

    plane = [(h, k) for h in (0, 1) for k in range(4) if h or k]

    def norm(n):
        h, k = plane[n]
        return remote(no_mid.at[0], no_plane.at[2 * t + c], norm_sems.at[0, n], norm_sems.at[1, n], (2 * z + (c ^ h), t ^ k))

    def norm_from(n):
        h, k = plane[n]
        spot = no_plane.at[2 * (t ^ k) + (c ^ h)]
        return remote(spot, spot, norm_sems.at[0, n], norm_sems.at[1, n], sibling)

    def norm_z(k):
        return remote(no_mid.at[1], no_z.at[z], norm_sems.at[0, 6 + k], norm_sems.at[1, 6 + k], (d ^ (2 * k), t))

    def norm_z_from(k):
        return remote(no_z.at[z ^ k], no_z.at[z ^ k], norm_sems.at[0, 6 + k], norm_sems.at[1, 6 + k], sibling)

    own = jnp.sum(no_own[...], axis=1)
    no_mid[0] = own
    for n in range(7):
        norm(n).start()
    no_plane[2 * t + c] = own
    for i in range(5):
        arrived(2, i).wait_recv()
        result[i][...] = sums[i][2].astype(F32)
        last(i).start()
    for n in range(7):
        norm_from(n).wait_recv()
    own = no_plane[0]
    for n in range(1, 8):
        own = own + no_plane[n]
    no_mid[1] = own
    for k in (1, 2, 3):
        norm_z(k).start()
    no_z[z] = own
    for i in range(5):
        remote(theirs[i], theirs[i], last_sems.at[0, i], last_sems.at[1, i], sibling).wait_recv()
        last(i).wait_send()
        for step in (0, 1, 2):
            along(step, i).wait_send()
        for k in (1, 2, 3):
            cross(k, i).wait_send()
    share().wait_send()
    for k in (1, 2, 3):
        norm_z_from(k).wait_recv()
    ono[...] = ((no_z[0] + no_z[1]) + no_z[2]) + no_z[3]
    for n in range(7):
        norm(n).wait_send()
    for k in (1, 2, 3):
        norm_z(k).wait_send()
        row(k).wait_send()
        y_row(k).wait_send()
    for k in range(4):
        give(k).wait_send()

    @pl.when(jnp.logical_not(local_row))
    def _():
        row(0).wait_send()
        y_row(0).wait_send()

    for m in (0, 1):
        for h in (0, 1):
            pltpu.make_async_copy(rows.at[0], out.at[m, pl.ds(256 * h, 256)], row_sems.at[4 + 2 * m + h]).wait()
            pltpu.make_async_copy(y.at[0], yout.at[m, pl.ds(256 * h, 256)], row_sems.at[20 + 2 * m + h]).wait()


def back(dl, dp, mq, mu, xf, gf, gain, y, dbq, dbu, dao, dad, dsh):
    vmem = pl.BlockSpec(memory_space=pltpu.VMEM)
    anywhere = pl.BlockSpec(memory_space=pl.ANY)
    part = [(3, 128, 128), (128, 512), (128, 128), (128, 512), (6, 32, 512)]
    outs = [((2, 512, 1024), BF), ((2, 512, 1024), BF), ((3, 128, 256), F32), ((128, 1024), F32), ((256, 128), F32), ((128, 1024), F32),
            ((6, 32, 1024), F32), ((4, 1024), F32)]
    return pl.pallas_call(
        back_kernel,
        in_specs=[anywhere] * 6 + [vmem] * 7,
        out_specs=[anywhere] * 2 + [vmem] * 6,
        out_shape=[jax.ShapeDtypeStruct(s, d) for s, d in outs],
        scratch_shapes=[
            pltpu.SemaphoreType.DMA((24,)),
            pltpu.SemaphoreType.DMA((2,)),
            pltpu.SemaphoreType.DMA((2, 3, 5)),
            pltpu.SemaphoreType.DMA((2, 3, 5)),
            pltpu.SemaphoreType.DMA((2, 5)),
            pltpu.SemaphoreType.DMA((2, 10)),
            pltpu.SemaphoreType.DMA((4, 2)),
            pltpu.SemaphoreType.DMA((2,)),
            pltpu.VMEM((6, 128, 512), BF),
            pltpu.VMEM((6, 128, 512), BF),
        ] + [pltpu.VMEM((3,) + s, BF) for s in part + part] + [pltpu.VMEM((2,) + s, BF) for s in part] + [
            pltpu.VMEM((8, 4, 1024), F32),
            pltpu.VMEM((4, 4, 1024), F32),
            pltpu.VMEM((4, 8, 1024), F32),
            pltpu.VMEM((2, 4, 1024), F32),
            pltpu.VMEM((3, 1024, 512), BF),
            pltpu.VMEM((1024, 2048), BF),
            pltpu.VMEM((2, 3, 512, 256), BF),
            pltpu.VMEM((2, 256, 2048), BF),
            pltpu.VMEM((2, 256, 1024), BF),
            pltpu.VMEM((2, 256, 1024), BF),
            pltpu.VMEM((3, 256, 512), BF),
            pltpu.VMEM((256, 1024), F32),
            pltpu.VMEM((256, 1024), F32),
            pltpu.VMEM((256, 1024), F32),
            pltpu.VMEM((256, 1), F32),
            pltpu.VMEM((4, 256, 1024), BF),
            pltpu.VMEM((4, 256, 1024), BF),
            pltpu.VMEM((4, 256, 1024), BF),
        ],
        compiler_params=pltpu.CompilerParams(collective_id=1, has_side_effects=True, vmem_limit_bytes=56 << 20),
        name="back",
    )(dl, dp, mq, mu, xf, gf, gain, y, dbq, dbu, dao, dad, dsh)


def swap(v, k=1):
    return lax.ppermute(v, "dp", [(i, i ^ k) for i in range(lax.axis_size("dp"))])


def pick(v, axis, index, size):
    return lax.dynamic_slice_in_dim(v, index * size, size, axis)


def half_rows(v, c):
    return pick(v.reshape(4, 2, 256, -1), 1, c, 1)[:, 0]


def by_groups(x, gy, segment, keep, gain, bias, w_qkv, w_out, w_up, w_down,
              a_in, b_qkv, b_up, a_out, a_down, b_out):
    z, c, t = place()
    tables = jnp.stack([segment[:, 0], keep[:, 0]], 1)
    pair = jnp.where(t % 2 == c, tables, swap(tables))
    seg, kept = jnp.where(t // 2 == 0, pair[0], pair[1])

    x_full, g_full, qkv, out, a_full, b_qkv_all, a_out_all, b_full = front(
        x[:, 0], gy[:, 0], w_qkv, w_out, jnp.swapaxes(a_in, 1, 2), b_qkv, a_out, b_out)
    up, down = lax.optimization_barrier((
        jnp.concatenate([pick(w_up, 1, c, 512), pick(b_up, 1, c, 512)], axis=0),
        jnp.concatenate([pick(w_down, 0, c, 512), pick(a_down, 0, c, 512)], axis=1), x_full))[:2]
    up = lax.all_gather(up, "tensor", axis=0)
    down = lax.all_gather(down, "tensor", axis=0, tiled=True)
    w_up_all = jnp.concatenate([up[i, :1024] for i in range(4)], axis=1)
    b_up_all = jnp.concatenate([up[i, 1024:] for i in range(4)], axis=1)
    w_down_all, a_down_all = down[:, :1024], down[:, 1024:]

    m_qkv = (qkv.astype(F32) + SCALE * jnp.einsum("nrk,nrc->nkc", a_full[:3], b_qkv_all,
                                                  preferred_element_type=F32)).astype(BF)
    m_up = (w_up_all.astype(F32) + SCALE * dot(a_full[3], b_up_all, 0, 0)).astype(BF)
    m_out = (out.astype(F32) + SCALE * dot(a_out_all, b_full[0], 1, 0)).astype(BF)
    m_down = (w_down_all.astype(F32) + SCALE * dot(a_down_all, b_full[1], 1, 0)).astype(BF)
    a_three = a_full[:3].reshape(3 * RANK, 1024)
    b_both = b_full.reshape(2 * RANK, 1024)

    standard, _ = normalized(x_full.astype(F32))
    n1 = (standard * gain[0] + bias[0]).astype(BF)
    n2 = (standard * gain[1] + bias[1]).astype(BF)
    lin = jnp.einsum("nkc,sk->ncs", m_qkv, n1, preferred_element_type=F32)
    low3 = dot(a_three, n1, 1, 1).astype(BF).reshape(3, RANK, 2048)
    low1 = dot(a_full[3], n2, 1, 1).astype(BF)
    g_ctx = dot(m_out, g_full, 1, 1).astype(BF)
    low_grad = (SCALE * dot(b_both, g_full, 1, 1)).astype(BF)
    cos, sin = rotary_tables(seg)
    ctx, d_lin = attention(lin, g_ctx, cos, sin, seg, kept)

    pre = dot(n2, m_up, 1, 0)
    cdf = 0.5 * (1.0 + lax.erf(pre * math.sqrt(0.5)))
    hidden = (pre * cdf).astype(BF)
    slope = cdf + pre * (math.sqrt(0.5 / math.pi) * jnp.exp(-0.5 * pre * pre))
    d_pre = (dot(g_full, m_down, 1, 1) * slope).astype(BF)

    part = dot(ctx, m_out, 0, 0) + dot(hidden, m_down, 1, 0)
    theirs = swap(half_rows(part, 1 - c).astype(BF))
    y = half_rows(x_full, c).astype(F32) + half_rows(part, c) + theirs.astype(F32)

    lo = jnp.concatenate([dot(a_out_all, ctx, 0, 0), dot(a_down_all, hidden, 0, 1)], axis=0).astype(BF)
    d_a_out = dot(ctx, low_grad[:RANK], 1, 1).astype(BF)
    d_a_down = dot(low_grad[RANK:], hidden, 1, 0).astype(BF)
    d_b_qkv = (SCALE * jnp.einsum("nrs,ncs->nrc", low3, d_lin, preferred_element_type=F32)).astype(BF)
    d_b_up = (SCALE * dot(low1, d_pre, 1, 0)).astype(BF)
    back3 = (SCALE * jnp.einsum("nrc,ncs->nrs", b_qkv_all, d_lin, preferred_element_type=F32)).astype(BF)
    back1 = (SCALE * dot(b_up_all, d_pre, 1, 1)).astype(BF)
    shared = jnp.concatenate([dot(back3.reshape(3 * RANK, 2048), n1, 1, 0).astype(BF), dot(back1, n2, 1, 0).astype(BF),
                              (SCALE * dot(lo, g_full, 1, 0)).astype(BF)], axis=0).reshape(6, RANK, 1024)
    grad, y, r_b_qkv, r_b_up, r_a_out, r_a_down, rest, norms = back(
        d_lin, d_pre, m_qkv, m_up, x_full, g_full, gain, y.astype(BF), d_b_qkv, d_b_up, d_a_out, d_a_down, shared)
    r_a_in = jnp.swapaxes(rest[:4], 1, 2)
    return (y[:, None], grad[:, None], norms[:2], norms[2:], r_a_in, r_b_qkv, r_b_up, r_a_out, jnp.transpose(r_a_down), rest[4:])


def solution(mesh):
    in_specs = (
        P(None, "dp", "tensor", None),
        P(None, "dp", "tensor", None),
        P(None, "dp", None),
        P(None, "dp", None),
        P(),
        P(),
        P(None, None, "tensor"),
        P("tensor", None),
        P(None, "tensor"),
        P("tensor", None),
        P(None, None, "tensor"),
        P(None, None, "tensor"),
        P(None, "tensor"),
        P("tensor", None),
        P("tensor", None),
        P(None, "tensor", None),
    )
    out_specs = (
        P(None, "dp", "tensor", None),
        P(None, "dp", "tensor", None),
        P(),
        P(),
        P(None, None, "tensor"),
        P(None, None, "tensor"),
        P(None, "tensor"),
        P("tensor", None),
        P("tensor", None),
        P(None, "tensor", None),
    )
    small = mesh.shape["tensor"] == 4 and mesh.shape["dp"] == 8
    return jax.shard_map(
        by_groups if small else by_features, mesh=mesh, in_specs=in_specs, out_specs=out_specs, check_vma=False
    )
```

```python
import functools
import math

import jax
import jax.numpy as jnp
from jax import lax
from jax.experimental import pallas as pl
from jax.experimental.pallas import tpu as pltpu
from jax.sharding import PartitionSpec as P

HEAD = 64
HALF = 8
N_DOCS = 5
TILE = 256
SLOTS = 5
EPSILON = 1e-05
SCALE = 0.25
F32 = jnp.float32
BF = jnp.bfloat16


def dot(a, b, ca, cb):
    return lax.dot_general(a, b, (((ca,), (cb,)), ((), ())), preferred_element_type=F32)


def attention_kernel(heads, lo_ref, lin_ref, g_ref, cos_ref, sin_ref, segq_ref, segk_ref,
                     ctx_ref, dlin_ref, qt, kt, vt, kn, vn, acc, s_scr, e_scr, p_scr, row):
    length = lin_ref.shape[2]
    blocks = length // TILE

    def rotate(z, cos, sin):
        a, b = z[:HALF], z[HALF:2 * HALF]
        return jnp.concatenate([a * cos - b * sin, b * cos + a * sin, z[2 * HALF:]], axis=0)

    def prepare(c, carry):
        cols = pl.ds(pl.multiple_of(c * TILE, TILE), TILE)
        cos, sin = cos_ref[:, cols], sin_ref[:, cols]
        for h in range(heads):
            rows = pl.ds(h * HEAD, HEAD)
            q = rotate(lin_ref[0, pl.ds(h * HEAD, HEAD), cols], cos, sin).astype(BF).astype(F32) * 0.125
            k = rotate(lin_ref[1, pl.ds(h * HEAD, HEAD), cols], cos, sin)
            v = lin_ref[2, pl.ds(h * HEAD, HEAD), cols]
            qt[rows, cols] = q.astype(BF)
            kt[rows, cols] = k.astype(BF)
            vt[rows, cols] = v.astype(BF)
            kn[h, cols, :] = jnp.transpose(k).astype(BF)
            vn[h, cols, :] = jnp.transpose(v).astype(BF)
            acc[h, :, cols] = jnp.zeros((2 * HEAD, TILE), F32)
        return carry

    lax.fori_loop(0, blocks, prepare, 0)

    def query_block(qb, carry):
        lo = lo_ref[qb]
        qcols = pl.ds(pl.multiple_of(qb * TILE, TILE), TILE)
        segq = segq_ref[:, qcols]

        def scores(kb, tops, last=False):
            krows = pl.ds(pl.multiple_of(kb * TILE, TILE), TILE)
            allowed = segk_ref[krows, :] == segq
            if last:
                k, q = (lax.broadcasted_iota(jnp.int32, (TILE, TILE), i) for i in (0, 1))
                allowed = (allowed & (k < q)) | (k == q)
            out = []
            for h in range(heads):
                rows = pl.ds(h * HEAD, HEAD)
                s = dot(kn[h, krows, :], qt[rows, qcols], 1, 0)
                s = jnp.where(allowed, s, -1e30)
                s_scr[h, kb - lo] = s
                p_scr[h, kb - lo] = dot(vn[h, krows, :], g_ref[rows, qcols], 1, 0)
                out.append(jnp.maximum(tops[h], jnp.max(s, axis=0, keepdims=True)))
            return tuple(out)

        tops = lax.fori_loop(lo, qb, scores, tuple(jnp.full((1, TILE), -1e30, F32) for _ in range(heads)))
        tops = scores(qb, tops, True)

        def weights(kb, sums):
            kcols = pl.ds(pl.multiple_of(kb * TILE, TILE), TILE)
            out = []
            for h in range(heads):
                e = jnp.exp(s_scr[h, kb - lo] - tops[h])
                low = e.astype(BF)
                e_scr[h, kb - lo] = low
                out.append(sums[h] + jnp.sum(e, axis=0, keepdims=True))
                row[h] += dot(vt[pl.ds(h * HEAD, HEAD), kcols], low, 1, 0)
            return tuple(out)

        row[...] = jnp.zeros_like(row)
        sums = lax.fori_loop(lo, qb + 1, weights, tuple(jnp.zeros((1, TILE), F32) for _ in range(heads)))
        gts, terms, scales = [], [], []
        for h in range(heads):
            rows = pl.ds(h * HEAD, HEAD)
            inverse = 1.0 / sums[h]
            ctx = row[h] * inverse
            ctx_ref[rows, qcols] = ctx.astype(BF)
            g = g_ref[rows, qcols].astype(F32)
            terms.append(jnp.sum(g * ctx, axis=0, keepdims=True))
            scales.append(inverse)
            gts.append((g * inverse).astype(BF))

        row[...] = jnp.zeros_like(row)

        def backward(kb, carry):
            krows = pl.ds(pl.multiple_of(kb * TILE, TILE), TILE)
            for h in range(heads):
                low = e_scr[h, kb - lo]
                ds = (low.astype(F32) * ((p_scr[h, kb - lo] - terms[h]) * scales[h])).astype(BF)
                acc[h, :HEAD, krows] += dot(gts[h], low, 1, 1)
                acc[h, HEAD:, krows] += dot(qt[pl.ds(h * HEAD, HEAD), qcols], ds, 1, 1)
                row[h] += dot(kt[pl.ds(h * HEAD, HEAD), krows], ds, 1, 0)
            return carry

        lax.fori_loop(lo, qb + 1, backward, 0)
        cos, sin = cos_ref[:, qcols], sin_ref[:, qcols]
        for h in range(heads):
            dlin_ref[0, pl.ds(h * HEAD, HEAD), qcols] = rotate(row[h] * 0.125, cos, -sin).astype(BF)
        return carry

    lax.fori_loop(0, blocks, query_block, 0)

    def finish(c, carry):
        cols = pl.ds(pl.multiple_of(c * TILE, TILE), TILE)
        cos, sin = cos_ref[:, cols], sin_ref[:, cols]
        for h in range(heads):
            both = acc[h, :, cols]
            dlin_ref[1, pl.ds(h * HEAD, HEAD), cols] = rotate(both[HEAD:], cos, -sin).astype(BF)
            dlin_ref[2, pl.ds(h * HEAD, HEAD), cols] = both[:HEAD].astype(BF)
        return carry

    lax.fori_loop(0, blocks, finish, 0)


def attention(lin, g, cos, sin, segment, keep):
    width, length = g.shape
    heads = min(4, width // HEAD)
    wide = heads * HEAD
    starts = jnp.sum(segment[None, :] < jnp.arange(N_DOCS, dtype=jnp.int32)[:, None], axis=1)
    firsts = segment[::TILE]
    lo = jnp.sum(jnp.where(firsts[:, None] == jnp.arange(N_DOCS)[None, :], starts[None, :], 0), axis=1)
    lo = (lo // TILE).astype(jnp.int32)
    segk = jnp.where(keep == 1, segment, -1)[:, None]
    vmem = pl.BlockSpec(memory_space=pltpu.VMEM)
    three = pl.BlockSpec((3, wide, length), lambda i, lo: (0, i, 0))
    single = pl.BlockSpec((wide, length), lambda i, lo: (i, 0))
    return pl.pallas_call(
        functools.partial(attention_kernel, heads),
        grid_spec=pltpu.PrefetchScalarGridSpec(
            num_scalar_prefetch=1,
            grid=(width // wide,),
            in_specs=[three, single] + [vmem] * 4,
            out_specs=[single, three],
            scratch_shapes=[
                pltpu.VMEM((wide, length), BF),
                pltpu.VMEM((wide, length), BF),
                pltpu.VMEM((wide, length), BF),
                pltpu.VMEM((heads, length, HEAD), BF),
                pltpu.VMEM((heads, length, HEAD), BF),
                pltpu.VMEM((heads, 2 * HEAD, length), F32),
                pltpu.VMEM((heads, SLOTS, TILE, TILE), F32),
                pltpu.VMEM((heads, SLOTS, TILE, TILE), BF),
                pltpu.VMEM((heads, SLOTS, TILE, TILE), F32),
                pltpu.VMEM((heads, HEAD, TILE), F32),
            ]),
        out_shape=[jax.ShapeDtypeStruct((width, length), BF), jax.ShapeDtypeStruct((3, width, length), BF)],
        compiler_params=pltpu.CompilerParams(vmem_limit_bytes=60 << 20),
        name="attention",
        cost_estimate=pl.CostEstimate(flops=10 * width * length * 768, transcendentals=width * length * 12,
                                      bytes_accessed=26 * width * length),
    )(lo, lin, g, cos, sin, segment[None, :], segk)


def rotary_tables(segment):
    length = segment.shape[0]
    starts = jnp.sum(segment[None, :] < jnp.arange(N_DOCS, dtype=jnp.int32)[:, None], axis=1)
    begin = jnp.sum(jnp.where(segment[None, :] == jnp.arange(N_DOCS)[:, None], starts[:, None], 0), axis=0)
    position = (jnp.arange(length, dtype=jnp.int32) - begin).astype(F32)
    exponent = jnp.arange(HALF, dtype=F32) / HALF
    frequency = jnp.exp(-math.log(10000.0) * exponent)
    angles = frequency[:, None] * position[None, :]
    return jnp.cos(angles), jnp.sin(angles)


def normalized(values):
    average = jnp.mean(values, axis=-1, keepdims=True)
    centered = values - average
    variance = jnp.mean(centered * centered, axis=-1, keepdims=True)
    inverse = lax.rsqrt(variance + EPSILON)
    return centered * inverse, inverse


def by_features(x, gy, segment, keep, gain, bias, w_qkv, w_out, w_up, w_down,
              a_in, b_qkv, b_up, a_out, a_down, b_out):
    width = w_qkv.shape[2]
    micro = x.shape[0]
    a_full = lax.all_gather(a_in, "tensor", axis=2, tiled=True)
    b_full = lax.all_gather(b_out, "tensor", axis=1, tiled=True)

    m_qkv = jnp.concatenate([
        (w_qkv[i].astype(F32) + SCALE * dot(a_full[i], b_qkv[i], 1, 0)).astype(BF) for i in range(3)
    ], axis=1)
    m_up = (w_up.astype(F32) + SCALE * dot(a_full[3], b_up, 1, 0)).astype(BF)
    m_out = (w_out.astype(F32) + SCALE * dot(a_out, b_full[0], 1, 0)).astype(BF)
    m_down = (w_down.astype(F32) + SCALE * dot(a_down, b_full[1], 1, 0)).astype(BF)
    a_three = jnp.concatenate([a_full[0], a_full[1], a_full[2]], axis=1)
    b_both = jnp.concatenate([b_full[0], b_full[1]], axis=0)

    outs, grads, sums = [], [], None
    for m in range(micro):
        rows, seg = x[m, 0], segment[m, 0]
        xg = lax.all_gather(rows, "tensor", axis=0, tiled=True)
        gg = lax.all_gather(gy[m, 0], "tensor", axis=0, tiled=True)
        standard, _ = normalized(xg.astype(F32))
        n1 = (standard * gain[0] + bias[0]).astype(BF)
        n2 = (standard * gain[1] + bias[1]).astype(BF)
        lin = dot(m_qkv, n1, 0, 1)
        low3 = dot(n1, a_three, 1, 0).astype(BF)
        low1 = dot(n2, a_full[3], 1, 0).astype(BF)
        g_ctx = dot(m_out, gg, 1, 1).astype(BF)
        low_grad = (SCALE * dot(gg, b_both, 1, 1)).astype(BF)
        cos, sin = rotary_tables(seg)
        ctx, d_lin = attention(lin.reshape(3, width, -1), g_ctx, cos, sin, seg, keep[m, 0])
        d_lin = d_lin.reshape(3 * width, -1)

        pre = dot(n2, m_up, 1, 0)
        cdf = 0.5 * (1.0 + lax.erf(pre * math.sqrt(0.5)))
        hidden = (pre * cdf).astype(BF)
        slope = cdf + pre * (math.sqrt(0.5 / math.pi) * jnp.exp(-0.5 * pre * pre))
        d_pre = (dot(gg, m_down, 1, 1) * slope).astype(BF)

        part = dot(ctx, m_out, 0, 0) + dot(hidden, m_down, 1, 0)
        branch = lax.psum_scatter(part.astype(BF), "tensor", scatter_dimension=0, tiled=True)
        outs.append((rows.astype(F32) + branch.astype(F32)).astype(BF))

        one = dot(d_lin, m_qkv, 0, 1)
        two = dot(d_pre, m_up, 1, 1)
        total = (gain[0] * one + gain[1] * two).astype(BF)
        total = lax.psum_scatter(total, "tensor", scatter_dimension=0, tiled=True).astype(F32)
        own, inverse = normalized(rows.astype(F32))
        grad = total - jnp.mean(total, axis=-1, keepdims=True)
        grad = grad - own * jnp.mean(total * own, axis=-1, keepdims=True)
        grads.append((gy[m, 0].astype(F32) + grad * inverse).astype(BF))

        norms = jnp.stack([jnp.sum(one * standard, axis=0), jnp.sum(two * standard, axis=0),
                           jnp.sum(one, axis=0), jnp.sum(two, axis=0)])
        lo_ctx = dot(ctx, a_out, 0, 0).astype(BF)
        lo_hid = dot(hidden, a_down, 1, 0).astype(BF)
        d_b_out = SCALE * jnp.stack([dot(lo_ctx, gg, 0, 0), dot(lo_hid, gg, 0, 0)], axis=1)
        d_a_out = dot(ctx, low_grad[:, :128], 1, 0)
        d_a_down = dot(hidden, low_grad[:, 128:], 0, 0)
        d_b_qkv = SCALE * jnp.stack([
            dot(low3[:, 128 * i:128 * (i + 1)], d_lin[width * i:width * (i + 1)], 0, 1) for i in range(3)])
        d_b_up = SCALE * dot(low1, d_pre, 0, 0)
        back = [(SCALE * dot(d_lin[width * i:width * (i + 1)], b_qkv[i], 0, 1)).astype(BF) for i in range(3)]
        back.append((SCALE * dot(d_pre, b_up, 1, 1)).astype(BF))
        d_a_in = jnp.stack([dot(back[i], n1 if i < 3 else n2, 0, 0) for i in range(4)], axis=1)
        terms = (d_a_in, d_b_qkv, d_b_up, d_a_out, d_a_down, d_b_out, norms)
        sums = terms if sums is None else tuple(p + q for p, q in zip(sums, terms))

    d_a_in, d_b_qkv, d_b_up, d_a_out, d_a_down, d_b_out, norms = sums
    d_a_in = lax.psum_scatter(d_a_in, "tensor", scatter_dimension=0, tiled=True)
    d_b_out = lax.psum_scatter(d_b_out, "tensor", scatter_dimension=0, tiled=True)
    d_a_in, d_b_qkv, d_b_up, d_a_out, d_a_down, d_b_out = lax.psum(
        (d_a_in, d_b_qkv, d_b_up, d_a_out, d_a_down, d_b_out), "dp")
    norms = lax.psum(norms, ("dp", "tensor"))
    return (jnp.stack(outs)[:, None], jnp.stack(grads)[:, None], norms[:2], norms[2:],
            jnp.transpose(d_a_in, (1, 2, 0)), d_b_qkv, d_b_up, d_a_out, d_a_down,
            jnp.transpose(d_b_out, (1, 0, 2)))


RANK = 128


MESH = pl.DeviceIdType.MESH


def place():
    d = lax.axis_index("dp")
    return d // 2, d % 2, lax.axis_index("tensor")


def meet(z, c, t, planes):
    barrier = pltpu.get_barrier_semaphore()
    for h in (0, 1):
        for k in range(4):
            if h or k:
                pl.semaphore_signal(barrier, 1, device_id=(2 * z + (c ^ h), t ^ k), device_id_type=MESH)
    for k in planes:
        pl.semaphore_signal(barrier, 1, device_id=(2 * (z ^ k) + c, t), device_id_type=MESH)
    pl.semaphore_wait(barrier, 7 + len(planes))


def remote(src, dst, send_sem, recv_sem, device):
    return pltpu.make_async_remote_copy(src_ref=src, dst_ref=dst, send_sem=send_sem, recv_sem=recv_sem,
                                        device_id=device, device_id_type=MESH)


class Rows:
    def __init__(self, v, full, sems, stage, local, z, c, t):
        self.v, self.full, self.sems, self.stage, self.local = v, full, sems, stage, local
        self.z, self.c, self.t = z, c, t

    def rows(self, s, h):
        return self.full.at[pl.ds(pl.multiple_of(s * 512 + h * 256, 256), 256)]

    def block(self, m, h):
        return self.v.at[m, pl.ds(pl.multiple_of(h * 256, 256), 256)]

    def copy(self, m, other):
        h = self.c ^ other
        return remote(self.block(m, h), self.rows(self.t, h), self.sems.at[2 * m + other], self.sems.at[4 + self.t],
                      (2 * self.z + h, 2 * m + self.c))

    def forward(self, s):
        part = self.rows(s, self.c)
        return remote(part, part, self.sems.at[8 + s], self.sems.at[12 + s], (2 * self.z + (self.c ^ 1), self.t))

    def start(self):
        for m in (0, 1):
            away = 2 * m + self.c != self.t

            @pl.when(away)
            def _():
                self.copy(m, 0).start()

            self.copy(m, 1).start()

            @pl.when(jnp.logical_not(away))
            def _():
                pltpu.make_async_copy(self.block(m, self.c), self.stage, self.local.at[0]).start()

    def relay(self):
        mine = self.t % 2 == self.c

        @pl.when(mine)
        def _():
            pltpu.make_async_copy(self.block(0, self.c), self.stage, self.local.at[0]).wait()
            pltpu.make_async_copy(self.stage, self.rows(self.t, self.c), self.sems.at[4 + self.t]).start()

        for k in (0, 1, 2, 3):
            s = self.t ^ k
            pltpu.make_async_copy(self.stage, self.rows(s, self.c), self.sems.at[4 + s]).wait()
            self.forward(s).start()

    def finish(self):
        for s in range(4):
            part = self.rows(s, self.c ^ 1)
            remote(part, part, self.sems.at[8 + s], self.sems.at[12 + s], (2 * self.z + (self.c ^ 1), self.t)).wait_recv()
            self.forward(s).wait_send()
        for m in (0, 1):
            @pl.when(2 * m + self.c != self.t)
            def _():
                self.copy(m, 0).wait_send()

            self.copy(m, 1).wait_send()


class Blocks:
    def __init__(self, own, where, sems, stage, local, cut, quarter, z, c, t):
        self.own, self.where, self.sems, self.stage, self.local = own, where, sems, stage, local
        self.cut, self.quarter, self.t, self.d, self.half = cut, quarter, t, 2 * z + c, z % 2

    def spot(self, k, other=0):
        return self.cut(self.where(self.t ^ k), self.half ^ other)

    def first(self, k):
        return remote(self.cut(self.own, self.half), self.spot(0), self.sems.at[k - 1], self.sems.at[2 + k],
                      (self.d, self.t ^ k))

    def arrival(self, k):
        return remote(self.spot(k), self.spot(k), self.sems.at[k - 1], self.sems.at[2 + k], (self.d, self.t ^ k))

    def second(self, k):
        part = self.quarter(self.spot(3 - k), k - 1)
        return remote(part, part, self.sems.at[5 + k], self.sems.at[7 + k], (self.d, self.t ^ k))

    def last(self, k):
        part = self.quarter(self.spot(3), k - 1)
        return remote(part, part, self.sems.at[5 + k], self.sems.at[7 + k], (self.d, self.t ^ k))

    def across(self, k, other=0):
        return remote(self.spot(k, other), self.spot(k, other), self.sems.at[9 + k], self.sems.at[12 + k],
                      (self.d ^ 2, self.t))

    def start(self):
        for k in ((1, 2) if self.quarter else (1, 2, 3)):
            self.first(k).start()
        pltpu.make_async_copy(self.own, self.stage, self.local.at[0]).start()

    def store(self):
        pltpu.make_async_copy(self.own, self.stage, self.local.at[0]).wait()
        pltpu.make_async_copy(self.stage, self.where(self.t), self.local.at[1]).start()

    def relay(self):
        for k in (1, 2):
            self.arrival(3 - k).wait_recv()
            if self.quarter:
                self.second(k).start()
            self.across(3 - k).start()

    def pass_on(self):
        if self.quarter:
            for k in (1, 2):
                self.last(k).wait_recv()
        else:
            self.arrival(3).wait_recv()
        self.across(3).start()

    def finish(self):
        pltpu.make_async_copy(self.stage, self.where(self.t), self.local.at[1]).wait()
        for k in (1, 2, 3):
            self.across(k, 1).wait_recv()
            self.across(k).wait_send()
            if k < 3 or not self.quarter:
                self.first(k).wait_send()
            if k < 3 and self.quarter:
                self.second(k).wait_send()


def aligned(i, n):
    return pl.ds(pl.multiple_of(i * n, n), n)


def front_kernel(x, g, wq, wo, ain, bq, ao, bo, gain, bias,
                 xf, gf, wqf, wof, ainf, bqf, aof, bof, n1, n2,
                 row_sems, sems, local, xs, gs, wqs, wos, ains, bqs, aos, bos, norm_sems, xb, n1s, n2s):
    z, c, t = place()
    meet(z, c, t, (1,))
    at = dict(z=z, c=c, t=t)
    x_rows = Rows(x, xf, row_sems.at[0], xs, local.at[0], **at)
    g_rows = Rows(g, gf, row_sems.at[1], gs, local.at[1], **at)
    qkv = Blocks(wq.at[:, :, aligned(c, 128)], lambda i: wqf.at[:, :, aligned(i, 128)], sems.at[0], wqs, local.at[2],
                 lambda v, h: v.at[:, aligned(h, 512)], lambda v, h: v.at[:, pl.ds(h * 256, 256)], **at)
    into = Blocks(ain, lambda i: ainf.at[:, aligned(i, 32)], sems.at[1], ains, local.at[3],
                  lambda v, h: v.at[pl.ds(2 * h, 2)], None, **at)
    second = Blocks(bq.at[:, :, aligned(c, 128)], lambda i: bqf.at[:, :, aligned(i, 128)], sems.at[2], bqs, local.at[4],
                    lambda v, h: v.at[:, aligned(h, 64)], None, **at)
    out = Blocks(wo.at[aligned(c, 128)], lambda i: wof.at[aligned(i, 128)], sems.at[3], wos, local.at[5],
                 lambda v, h: v.at[aligned(h, 64)], lambda v, h: v.at[pl.ds(h * 32, 32)], **at)
    a_out = Blocks(ao.at[aligned(c, 128)], lambda i: aof.at[aligned(i, 128)], sems.at[4], aos, local.at[6],
                   lambda v, h: v.at[aligned(h, 64)], None, **at)
    b_out = Blocks(bo, lambda i: bof.at[:, aligned(i, 32)], sems.at[5], bos, local.at[7],
                   lambda v, h: v.at[pl.ds(h, 1)], None, **at)
    blocks = (into, second, qkv, b_out, a_out, out)
    x_rows.start()
    for v in blocks:
        v.start()
    g_rows.start()
    x_rows.relay()
    for v in blocks:
        v.store()
    for v in blocks:
        v.relay()
    x_rows.finish()

    def load(j):
        return pltpu.make_async_copy(xf.at[aligned(j, 256)], xb.at[j % 2], norm_sems.at[j % 2])

    load(0).start()

    def norms(j, carry):
        load(j).wait()

        @pl.when(j < 7)
        def _():
            load(j + 1).start()

        def some(r, carry):
            v = xb[j % 2, aligned(r, 32), :].astype(F32)
            v = v - jnp.mean(v, axis=1, keepdims=True)
            v = v * lax.rsqrt(jnp.mean(v * v, axis=1, keepdims=True) + EPSILON)
            at = aligned(j * 8 + r, 32)
            n1s[at, :] = (v * gain[0:1, :] + bias[0:1, :]).astype(BF)
            n2s[at, :] = (v * gain[1:2, :] + bias[1:2, :]).astype(BF)
            return carry

        return lax.fori_loop(0, 8, some, carry)

    lax.fori_loop(0, 8, norms, 0)
    saves = (pltpu.make_async_copy(n1s, n1, norm_sems.at[2]), pltpu.make_async_copy(n2s, n2, norm_sems.at[3]))
    for v in saves:
        v.start()
    for v in blocks:
        v.pass_on()
    g_rows.relay()
    for v in blocks + (g_rows,):
        v.finish()
    for v in saves:
        v.wait()


def front(x, g, wq, wo, ain, bq, ao, bo, gain, bias):
    shapes = [(2048, 1024), (2048, 1024), (3, 1024, 512), (512, 1024), (4, 128, 1024), (3, 128, 512), (512, 128),
              (2, 128, 1024), (2048, 1024), (2048, 1024)]
    anywhere, vmem = pl.BlockSpec(memory_space=pl.ANY), pl.BlockSpec(memory_space=pltpu.VMEM)
    return pl.pallas_call(
        front_kernel,
        in_specs=[anywhere] * 8 + [vmem] * 2,
        out_specs=[anywhere] * 10,
        out_shape=[jax.ShapeDtypeStruct(s, BF) for s in shapes],
        scratch_shapes=[
            pltpu.SemaphoreType.DMA((2, 16)),
            pltpu.SemaphoreType.DMA((6, 16)),
            pltpu.SemaphoreType.DMA((8, 2)),
            pltpu.VMEM((256, 1024), BF),
            pltpu.VMEM((256, 1024), BF),
            pltpu.VMEM((3, 1024, 128), BF),
            pltpu.VMEM((128, 1024), BF),
            pltpu.VMEM((4, 32, 1024), BF),
            pltpu.VMEM((3, 128, 128), BF),
            pltpu.VMEM((128, 128), BF),
            pltpu.VMEM((2, 32, 1024), BF),
            pltpu.SemaphoreType.DMA((4,)),
            pltpu.VMEM((2, 256, 1024), BF),
            pltpu.VMEM((2048, 1024), BF),
            pltpu.VMEM((2048, 1024), BF),
        ],
        compiler_params=pltpu.CompilerParams(collective_id=0, has_side_effects=True),
        name="front",
    )(x, g, wq, wo, ain, bq, ao, bo, gain, bias)


def back_kernel(dl, dp, mq, mu, xf, gf, gain, y, dbq, dbu, dao, dad, dsh,
                out, yout, obq, obu, oao, oad, oai, obo, ono,
                row_sems, share_sems, cross_sems, z_sems, last_sems, norm_sems, local, weight_sems,
                sh_in, sh, rbq, rbu, rao, rad, rsh, pbq, pbu, pao, pad, psh, qbq, qbu, qao, qad, qsh,
                no_plane, no_z, no_own, no_mid, wq, wu, dlb, dpb, xb, gb, dlt, one, two, std, inv, sends, gets, rows):
    z, c, t = place()
    d = 2 * z + c
    sibling = (2 * z + (c ^ 1), t)

    def first_row(j):
        return (t ^ (j % 4)) * 512 + ((c + 1 + j // 4) % 2) * 256

    def loads(j):
        n = j % 2
        at = pl.ds(pl.multiple_of(first_row(j), 256), 256)
        return [pltpu.make_async_copy(v, w.at[n], local.at[i, n]) for i, (v, w) in enumerate((
            (dl.at[:, :, at], dlb), (dp.at[at], dpb), (xf.at[at], xb), (gf.at[at], gb)))]

    weights = (pltpu.make_async_copy(mq, wq, weight_sems.at[0]), pltpu.make_async_copy(mu, wu, weight_sems.at[1]))
    for v in loads(0):
        v.start()
    for v in weights:
        v.start()
    meet(z, c, t, (1, 2, 3))

    home = t % 2
    local_row = home == c
    slot = (t // 2) * 2 + c

    def row(k):
        return remote(rows.at[k], out.at[t // 2, aligned(c, 256)], row_sems.at[k], row_sems.at[4 + slot],
                      (2 * z + home, t ^ k))

    def own_row():
        return pltpu.make_async_copy(rows.at[0], out.at[t // 2, aligned(c, 256)], row_sems.at[4 + slot])

    def y_row(k):
        return remote(y.at[t ^ k], yout.at[t // 2, aligned(c, 256)], row_sems.at[16 + k], row_sems.at[20 + slot],
                      (2 * z + home, t ^ k))

    def own_y():
        return pltpu.make_async_copy(y.at[t], yout.at[t // 2, aligned(c, 256)], row_sems.at[20 + slot])

    def give(k):
        return remote(sends.at[k], gets.at[k], row_sems.at[8 + k], row_sems.at[12 + k], sibling)

    def share():
        return remote(dsh.at[:, :, aligned(c ^ 1, 512)], sh_in, share_sems.at[0], share_sems.at[1], sibling)

    def parts(j):
        return (dbq.at[:, :, aligned(j, 128)], dbu.at[:, aligned(j, 512)], dao.at[aligned(j, 128)],
                dad.at[:, aligned(j, 512)], sh.at[:, aligned(j, 32)])

    got = (rbq, rbu, rao, rad, rsh)

    def cross(k, i):
        return remote(parts(t ^ k)[i], got[i].at[k - 1], cross_sems.at[0, k - 1, i], cross_sems.at[1, k - 1, i], (d, t ^ k))

    sums = (pbq, pbu, pao, pad, psh)
    halves = (qbq, qbu, qao, qad, qsh)
    low = z % 2

    def half(v, i, j):
        if i == 0:
            return v.at[:, aligned(j, 64)]
        if i == 4:
            return v.at[:, aligned(j, 16)]
        return v.at[aligned(j, 64)]

    def along(step, i):
        j = low ^ 1 if step == 0 else low
        dst = sums[i].at[2] if step == 2 else halves[i].at[step]
        return remote(half(sums[i].at[step], i, j), half(dst, i, j), z_sems.at[0, step, i], z_sems.at[1, step, i],
                      (d ^ (4 if step == 1 else 2), t))

    def arrived(step, i):
        j = low ^ 1 if step == 2 else low
        dst = sums[i].at[2] if step == 2 else halves[i].at[step]
        return remote(half(dst, i, j), half(dst, i, j), z_sems.at[0, step, i], z_sems.at[1, step, i], (d, t ^ 1))

    result = (obq.at[:, :, aligned(c, 128)], obu.at[:, aligned(c, 512)], oao.at[aligned(c, 128)],
              oad.at[:, aligned(c, 512)], oai.at[:, :, aligned(c, 512)], obo.at[:, :, aligned(c, 512)])
    theirs = (obq.at[:, :, aligned(c ^ 1, 128)], obu.at[:, aligned(c ^ 1, 512)], oao.at[aligned(c ^ 1, 128)],
              oad.at[:, aligned(c ^ 1, 512)], oai.at[:, :, aligned(c ^ 1, 512)], obo.at[:, :, aligned(c ^ 1, 512)])

    def last(i):
        return remote(result[i], result[i], last_sems.at[0, i], last_sems.at[1, i], sibling)

    share().start()
    for v in weights:
        v.wait()
    no_own[...] = jnp.zeros_like(no_own)

    def block(j, carry):
        n, k = j % 2, j % 4
        for v in loads(j):
            v.wait()

        @pl.when(j < 7)
        def _():
            for v in loads(j + 1):
                v.start()

        for i in range(3):
            dlt[i] = jnp.transpose(dlb[n, i])

        def columns(m, carry):
            at = aligned(m, 256)
            one[:, at] = (dot(dlt[0], wq[0, at, :], 1, 1) + dot(dlt[1], wq[1, at, :], 1, 1)
                          + dot(dlt[2], wq[2, at, :], 1, 1))
            two[:, at] = dot(dpb[n], wu[at, :], 1, 1)
            return carry

        lax.fori_loop(0, 4, columns, 0)

        def norms(r, carry):
            at = aligned(r, 32)
            v = xb[n, at, :].astype(F32)
            v = v - jnp.mean(v, axis=1, keepdims=True)
            inverse = lax.rsqrt(jnp.mean(v * v, axis=1, keepdims=True) + EPSILON)
            v = v * inverse
            a, b = one[at, :], two[at, :]
            for i, w in enumerate((a * v, b * v, a, b)):
                no_own[i] += jnp.sum(w.reshape(4, 8, 1024), axis=0)
            one[at, :] = gain[0:1, :] * a + gain[1:2, :] * b
            std[at, :] = v
            inv[at, :] = inverse
            return carry

        lax.fori_loop(0, 8, norms, 0)

        @pl.when(j < 4)
        def _():
            sends[k] = one[...].astype(BF)
            give(k).start()

        @pl.when(j >= 4)
        def _():
            give(k).wait_recv()

            def finish(r, carry):
                at = aligned(r, 32)
                v, own = one[at, :] + gets[k, at, :].astype(F32), std[at, :]
                v = v - jnp.mean(v, axis=1, keepdims=True) - own * jnp.mean(v * own, axis=1, keepdims=True)
                rows[k, at, :] = (gb[n, at, :].astype(F32) + v * inv[at, :]).astype(BF)
                return carry

            lax.fori_loop(0, 8, finish, 0)
            here = (k == 0) & local_row

            @pl.when(here)
            def _():
                own_row().start()

            @pl.when(jnp.logical_not(here))
            def _():
                row(k).start()

        @pl.when(j == 0)
        def _():
            share().wait_recv()
            for i in range(6):
                sh[i] = (dsh[i, :, aligned(c, 512)].astype(F32) + sh_in[i].astype(F32)).astype(BF)
            for i in range(5):
                for p in (1, 2, 3):
                    cross(p, i).start()

        @pl.when(j == 3)
        def _():
            for i in range(5):
                for p in (1, 2, 3):
                    cross(p, i).wait_recv()
                total = parts(t)[i][...].astype(F32)
                for p in (0, 1, 2):
                    total = total + got[i][p].astype(F32)
                sums[i][0] = total.astype(BF)
                along(0, i).start()
            for p in (1, 2, 3):
                y_row(p).start()

            @pl.when(local_row)
            def _():
                own_y().start()

            @pl.when(jnp.logical_not(local_row))
            def _():
                y_row(0).start()

        for step, when in ((0, 4), (1, 6)):
            @pl.when(j == when)
            def _():
                for i in range(5):
                    arrived(step, i).wait_recv()
                    mine, other = half(sums[i].at[step], i, low), half(halves[i].at[step], i, low)
                    half(sums[i].at[step + 1], i, low)[...] = (mine[...].astype(F32) + other[...].astype(F32)).astype(BF)
                    along(step + 1, i).start()

        return carry

    lax.fori_loop(0, 8, block, 0)

    plane = [(h, k) for h in (0, 1) for k in range(4) if h or k]

    def norm(n):
        h, k = plane[n]
        return remote(no_mid.at[0], no_plane.at[2 * t + c], norm_sems.at[0, n], norm_sems.at[1, n], (2 * z + (c ^ h), t ^ k))

    def norm_from(n):
        h, k = plane[n]
        spot = no_plane.at[2 * (t ^ k) + (c ^ h)]
        return remote(spot, spot, norm_sems.at[0, n], norm_sems.at[1, n], sibling)

    def norm_z(k):
        return remote(no_mid.at[1], no_z.at[z], norm_sems.at[0, 6 + k], norm_sems.at[1, 6 + k], (d ^ (2 * k), t))

    def norm_z_from(k):
        return remote(no_z.at[z ^ k], no_z.at[z ^ k], norm_sems.at[0, 6 + k], norm_sems.at[1, 6 + k], sibling)

    own = jnp.sum(no_own[...], axis=1)
    no_mid[0] = own
    for n in range(7):
        norm(n).start()
    no_plane[2 * t + c] = own
    for i in range(5):
        arrived(2, i).wait_recv()
        if i < 4:
            result[i][...] = sums[i][2].astype(F32)
        else:
            result[4][...] = sums[4][2, :4].astype(F32)
            result[5][...] = sums[4][2, 4:].astype(F32)
            last(5).start()
        last(i).start()
    for n in range(7):
        norm_from(n).wait_recv()
    own = no_plane[0]
    for n in range(1, 8):
        own = own + no_plane[n]
    no_mid[1] = own
    for k in (1, 2, 3):
        norm_z(k).start()
    no_z[z] = own
    for i in range(6):
        remote(theirs[i], theirs[i], last_sems.at[0, i], last_sems.at[1, i], sibling).wait_recv()
        last(i).wait_send()
    for i in range(5):
        for step in (0, 1, 2):
            along(step, i).wait_send()
        for k in (1, 2, 3):
            cross(k, i).wait_send()
    share().wait_send()
    for k in (1, 2, 3):
        norm_z_from(k).wait_recv()
    ono[...] = ((no_z[0] + no_z[1]) + no_z[2]) + no_z[3]
    for n in range(7):
        norm(n).wait_send()
    for k in (1, 2, 3):
        norm_z(k).wait_send()
        row(k).wait_send()
        y_row(k).wait_send()
    for k in range(4):
        give(k).wait_send()

    @pl.when(jnp.logical_not(local_row))
    def _():
        row(0).wait_send()
        y_row(0).wait_send()

    for m in (0, 1):
        for h in (0, 1):
            pltpu.make_async_copy(rows.at[0], out.at[m, pl.ds(256 * h, 256)], row_sems.at[4 + 2 * m + h]).wait()
            pltpu.make_async_copy(y.at[0], yout.at[m, pl.ds(256 * h, 256)], row_sems.at[20 + 2 * m + h]).wait()


def back(dl, dp, mq, mu, xf, gf, gain, y, dbq, dbu, dao, dad, dsh):
    vmem = pl.BlockSpec(memory_space=pltpu.VMEM)
    anywhere = pl.BlockSpec(memory_space=pl.ANY)
    part = [(3, 128, 128), (128, 512), (128, 128), (128, 512), (6, 32, 512)]
    outs = [((2, 512, 1024), BF), ((2, 512, 1024), BF), ((3, 128, 256), F32), ((128, 1024), F32), ((256, 128), F32), ((128, 1024), F32),
            ((4, 32, 1024), F32), ((2, 32, 1024), F32), ((4, 1024), F32)]
    return pl.pallas_call(
        back_kernel,
        in_specs=[anywhere] * 6 + [vmem] * 7,
        out_specs=[anywhere] * 2 + [vmem] * 7,
        out_shape=[jax.ShapeDtypeStruct(s, d) for s, d in outs],
        scratch_shapes=[
            pltpu.SemaphoreType.DMA((24,)),
            pltpu.SemaphoreType.DMA((2,)),
            pltpu.SemaphoreType.DMA((2, 3, 5)),
            pltpu.SemaphoreType.DMA((2, 3, 5)),
            pltpu.SemaphoreType.DMA((2, 6)),
            pltpu.SemaphoreType.DMA((2, 10)),
            pltpu.SemaphoreType.DMA((4, 2)),
            pltpu.SemaphoreType.DMA((2,)),
            pltpu.VMEM((6, 128, 512), BF),
            pltpu.VMEM((6, 128, 512), BF),
        ] + [pltpu.VMEM((3,) + s, BF) for s in part + part] + [pltpu.VMEM((2,) + s, BF) for s in part] + [
            pltpu.VMEM((8, 4, 1024), F32),
            pltpu.VMEM((4, 4, 1024), F32),
            pltpu.VMEM((4, 8, 1024), F32),
            pltpu.VMEM((2, 4, 1024), F32),
            pltpu.VMEM((3, 1024, 512), BF),
            pltpu.VMEM((1024, 2048), BF),
            pltpu.VMEM((2, 3, 512, 256), BF),
            pltpu.VMEM((2, 256, 2048), BF),
            pltpu.VMEM((2, 256, 1024), BF),
            pltpu.VMEM((2, 256, 1024), BF),
            pltpu.VMEM((3, 256, 512), BF),
            pltpu.VMEM((256, 1024), F32),
            pltpu.VMEM((256, 1024), F32),
            pltpu.VMEM((256, 1024), F32),
            pltpu.VMEM((256, 1), F32),
            pltpu.VMEM((4, 256, 1024), BF),
            pltpu.VMEM((4, 256, 1024), BF),
            pltpu.VMEM((4, 256, 1024), BF),
        ],
        compiler_params=pltpu.CompilerParams(collective_id=1, has_side_effects=True, vmem_limit_bytes=56 << 20),
        name="back",
    )(dl, dp, mq, mu, xf, gf, gain, y, dbq, dbu, dao, dad, dsh)


def swap(v, k=1):
    return lax.ppermute(v, "dp", [(i, i ^ k) for i in range(lax.axis_size("dp"))])


def pick(v, axis, index, size):
    return lax.dynamic_slice_in_dim(v, index * size, size, axis)


def half_rows(v, c):
    return pick(v.reshape(4, 2, 256, -1), 1, c, 1)[:, 0]


def by_groups(x, gy, segment, keep, gain, bias, w_qkv, w_out, w_up, w_down,
              a_in, b_qkv, b_up, a_out, a_down, b_out):
    z, c, t = place()
    tables = jnp.stack([segment[:, 0], keep[:, 0]], 1)
    pair = jnp.where(t % 2 == c, tables, swap(tables))
    seg, kept = jnp.where(t // 2 == 0, pair[0], pair[1])

    x_full, g_full, qkv, out, a_full, b_qkv_all, a_out_all, b_full, n1, n2 = front(
        x[:, 0], gy[:, 0], w_qkv, w_out, jnp.swapaxes(a_in, 1, 2), b_qkv, a_out, b_out, gain, bias)
    up, down = lax.optimization_barrier((
        jnp.concatenate([pick(w_up, 1, c, 512), pick(b_up, 1, c, 512)], axis=0),
        jnp.concatenate([pick(w_down, 0, c, 512), pick(a_down, 0, c, 512)], axis=1), x_full))[:2]
    up = lax.all_gather(up, "tensor", axis=0)
    down = lax.all_gather(down, "tensor", axis=0, tiled=True)
    w_up_all = jnp.concatenate([up[i, :1024] for i in range(4)], axis=1)
    b_up_all = jnp.concatenate([up[i, 1024:] for i in range(4)], axis=1)
    w_down_all, a_down_all = down[:, :1024], down[:, 1024:]

    m_qkv = (qkv.astype(F32) + SCALE * jnp.einsum("nrk,nrc->nkc", a_full[:3], b_qkv_all,
                                                  preferred_element_type=F32)).astype(BF)
    m_up = (w_up_all.astype(F32) + SCALE * dot(a_full[3], b_up_all, 0, 0)).astype(BF)
    m_out = (out.astype(F32) + SCALE * dot(a_out_all, b_full[0], 1, 0)).astype(BF)
    m_down = (w_down_all.astype(F32) + SCALE * dot(a_down_all, b_full[1], 1, 0)).astype(BF)
    a_three = a_full[:3].reshape(3 * RANK, 1024)
    b_both = b_full.reshape(2 * RANK, 1024)

    lin = jnp.einsum("nkc,sk->ncs", m_qkv, n1, preferred_element_type=F32)
    low3 = dot(a_three, n1, 1, 1).astype(BF).reshape(3, RANK, 2048)
    low1 = dot(a_full[3], n2, 1, 1).astype(BF)
    g_ctx = dot(m_out, g_full, 1, 1).astype(BF)
    low_grad = (SCALE * dot(b_both, g_full, 1, 1)).astype(BF)
    cos, sin = rotary_tables(seg)
    ctx, d_lin = attention(lin, g_ctx, cos, sin, seg, kept)

    pre = dot(n2, m_up, 1, 0)
    cdf = 0.5 * (1.0 + lax.erf(pre * math.sqrt(0.5)))
    hidden = (pre * cdf).astype(BF)
    slope = cdf + pre * (math.sqrt(0.5 / math.pi) * jnp.exp(-0.5 * pre * pre))
    d_pre = (dot(g_full, m_down, 1, 1) * slope).astype(BF)

    part = dot(ctx, m_out, 0, 0) + dot(hidden, m_down, 1, 0)
    theirs = swap(half_rows(part, 1 - c).astype(BF))
    y = half_rows(x_full, c).astype(F32) + half_rows(part, c) + theirs.astype(F32)

    lo = jnp.concatenate([dot(a_out_all, ctx, 0, 0), dot(a_down_all, hidden, 0, 1)], axis=0).astype(BF)
    d_a_out = dot(ctx, low_grad[:RANK], 1, 1).astype(BF)
    d_a_down = dot(low_grad[RANK:], hidden, 1, 0).astype(BF)
    d_b_qkv = (SCALE * jnp.einsum("nrs,ncs->nrc", low3, d_lin, preferred_element_type=F32)).astype(BF)
    d_b_up = (SCALE * dot(low1, d_pre, 1, 0)).astype(BF)
    back3 = (SCALE * jnp.einsum("nrc,ncs->nrs", b_qkv_all, d_lin, preferred_element_type=F32)).astype(BF)
    back1 = (SCALE * dot(b_up_all, d_pre, 1, 1)).astype(BF)
    shared = jnp.concatenate([dot(back3.reshape(3 * RANK, 2048), n1, 1, 0).astype(BF), dot(back1, n2, 1, 0).astype(BF),
                              (SCALE * dot(lo, g_full, 1, 0)).astype(BF)], axis=0).reshape(6, RANK, 1024)
    grad, y, r_b_qkv, r_b_up, r_a_out, r_a_down, r_a_in, r_b_out, norms = back(
        d_lin, d_pre, m_qkv, m_up, x_full, g_full, gain, y.astype(BF), d_b_qkv, d_b_up, d_a_out, d_a_down, shared)
    r_a_in = jnp.swapaxes(r_a_in, 1, 2)
    return (y[:, None], grad[:, None], norms[:2], norms[2:], r_a_in, r_b_qkv, r_b_up, r_a_out, jnp.transpose(r_a_down), r_b_out)


def solution(mesh):
    in_specs = (
        P(None, "dp", "tensor", None),
        P(None, "dp", "tensor", None),
        P(None, "dp", None),
        P(None, "dp", None),
        P(),
        P(),
        P(None, None, "tensor"),
        P("tensor", None),
        P(None, "tensor"),
        P("tensor", None),
        P(None, None, "tensor"),
        P(None, None, "tensor"),
        P(None, "tensor"),
        P("tensor", None),
        P("tensor", None),
        P(None, "tensor", None),
    )
    out_specs = (
        P(None, "dp", "tensor", None),
        P(None, "dp", "tensor", None),
        P(),
        P(),
        P(None, None, "tensor"),
        P(None, None, "tensor"),
        P(None, "tensor"),
        P("tensor", None),
        P("tensor", None),
        P(None, "tensor", None),
    )
    small = mesh.shape["tensor"] == 4 and mesh.shape["dp"] == 8
    return jax.shard_map(
        by_groups if small else by_features, mesh=mesh, in_specs=in_specs, out_specs=out_specs, check_vma=False
    )
```
